32 devices in a mesh: section: 2 (over core), shard: 2 (over x), replica: 8 (over z, y).
Axes of the slice: x: 2, y: 2, z: 4, core: 2. Of those that a mesh axis runs over, the one named last changes fastest.
Arguments:
- inputs: bfloat16 [32, 512, 1024], P(('shard', 'replica')), may hold values from -6 to 6
- cotangent: bfloat16 [32, 512, 1024], P(('shard', 'replica')), may hold values from -6 to 6
- lengths: int32 [32], replicated, may hold values from 128 to 512, as said below
- permutation: int32 [32], replicated, may hold values from 0 to 31, as said below
- query_weight: bfloat16 [2, 1024, 1024], P('section', 'shard'), may hold values from -0.1875 to 0.1875
- query_bias: bfloat16 [2, 1024], P('section', 'shard'), may hold values from -3 to 3
- key_weight: bfloat16 [2, 1024, 1024], P('section', 'shard'), may hold values from -0.1875 to 0.1875
- value_weight: bfloat16 [2, 1024, 1024], P('section', 'shard'), may hold values from -0.1875 to 0.1875
- value_bias: bfloat16 [2, 1024], P('section', 'shard'), may hold values from -3 to 3
- output_weight: bfloat16 [2, 1024, 1024], P('section', 'shard'), may hold values from -3 to 3
- output_bias: bfloat16 [2, 1024], P('section', 'shard'), may hold values from -3 to 3
- first_gain: bfloat16 [2, 1024], P('section', 'shard'), may hold values from 0.5 to 1.5
- first_bias: bfloat16 [2, 1024], P('section', 'shard'), may hold values from -3 to 3
- inner_weight: bfloat16 [2, 1024, 4096], P('section', 'shard'), may hold values from -0.1875 to 0.1875
- inner_bias: bfloat16 [2, 4096], P('section', 'shard'), may hold values from -3 to 3
- outer_weight: bfloat16 [2, 4096, 1024], P('section', 'shard'), may hold values from -0.09375 to 0.09375
- outer_bias: bfloat16 [2, 1024], P('section', 'shard'), may hold values from -3 to 3
- second_gain: bfloat16 [2, 1024], P('section', 'shard'), may hold values from 0.5 to 1.5
- second_bias: bfloat16 [2, 1024], P('section', 'shard'), may hold values from -3 to 3
Outputs:
- activations: bfloat16 [2, 32, 512, 1024], P('section', ('shard', 'replica'))
- input_grads: bfloat16 [2, 32, 512, 1024], P('section', ('shard', 'replica'))
- grad_query_weight: float32 [2, 1024, 1024], P('section', 'shard')
- grad_query_bias: float32 [2, 1024], P('section', 'shard')
- grad_key_weight: float32 [2, 1024, 1024], P('section', 'shard')
- grad_value_weight: float32 [2, 1024, 1024], P('section', 'shard')
- grad_value_bias: float32 [2, 1024], P('section', 'shard')
- grad_output_weight: float32 [2, 1024, 1024], P('section', 'shard')
- grad_output_bias: float32 [2, 1024], P('section', 'shard')
- grad_first_gain: float32 [2, 1024], P('section', 'shard')
- grad_first_bias: float32 [2, 1024], P('section', 'shard')
- grad_inner_weight: float32 [2, 1024, 4096], P('section', 'shard')
- grad_inner_bias: float32 [2, 4096], P('section', 'shard')
- grad_outer_weight: float32 [2, 4096, 1024], P('section', 'shard')
- grad_outer_bias: float32 [2, 1024], P('section', 'shard')
- grad_second_gain: float32 [2, 1024], P('section', 'shard')
- grad_second_bias: float32 [2, 1024], P('section', 'shard')
The draws below stay inside these ranges and needn't reach their ends.
Inputs may be any that keep to these rules, and one draw needn't show every extreme that they name: `lengths`: live tokens of each sequence; slots from it up to 512 are padding; some sequence has exactly 512. `permutation`: each of 0 to 31 once.
All inputs are finite; a program needn't handle non-finite values.
Results may differ from the reference program's by a relative error of at most 0.029.
Values may be sent and summed in bfloat16 or wider, within the bound.
A program may use at most 448 MiB of HBM per device.

```python
import jax
import jax.numpy as jnp
from jax import lax

D = 1024
HEADS = 16
HEAD_DIM = 64
FF = 4096
LMAX = 512
SEQ_DEV = 2
SEQS = 32
SECTIONS = 2


def common_lengths(key):
    inner_key = jax.random.fold_in(key, 11)
    drawn = jax.random.randint(inner_key, (SEQS,), LMAX // 4, LMAX + 1, dtype=jnp.int32)
    return drawn.at[0].set(LMAX)


def draw_lengths(key, part):
    return common_lengths(key)


def draw_permutation(key, part):
    sizes_drawn = common_lengths(key)
    ranking = jnp.arange(SEQS, dtype=jnp.int32)
    scores = sizes_drawn * SEQS + ranking
    order = jnp.argsort(scores, stable=True).astype(jnp.int32)
    groups = SEQS // SEQ_DEV
    rounds = ranking // groups
    position = ranking % groups
    device = jnp.where(rounds % 2 == 0, position, groups - 1 - position)
    dealt = device * SEQ_DEV + rounds
    return jnp.zeros((SEQS,), jnp.int32).at[dealt].set(order)


def steps_of(key, extent, cuts, smallest, largest):
    def one(axis_at, shards_of):
        draws = jax.random.uniform(jax.random.fold_in(jax.random.fold_in(key, 6), axis_at), (shards_of,), jnp.float32, smallest / len(cuts), largest / len(cuts))
        return jnp.repeat(jnp.exp(draws), extent[axis_at] // shards_of).reshape((-1,) + (1,) * (len(extent) - axis_at - 1))

    loudness = one(*cuts[0])
    for cut in cuts[1:]:
        loudness = loudness * one(*cut)
    return loudness


def noise(key, dims, scale, limit, cuts=(), kind=jnp.bfloat16):
    values = jax.random.normal(key, dims, jnp.float32) * scale
    if len(cuts) > 0:
        values = steps_of(key, dims, cuts, -0.22, 0.18) * values
    return jnp.clip(values, min=-limit, max=limit).astype(kind)


def setup_inputs(seed: int = 0) -> dict:
    splits = jax.random.split(jax.random.key(seed), 20)
    inputs = noise(splits[0], (SEQS, LMAX, D), 1.0, 6.0, ((0, 16),))
    cotangent = noise(splits[1], (SEQS, LMAX, D), 1.0, 6.0, ((0, 16),))
    lengths = draw_lengths(jax.random.fold_in(splits[19], 71), 0)
    permutation = draw_permutation(jax.random.fold_in(splits[19], 71), 0)
    query_weight = noise(splits[4], (SECTIONS, D, D), D ** -0.5, 0.1875, ((0, 2), (1, 2)))
    query_bias = noise(splits[5], (SECTIONS, D), 0.5, 3.0, ((0, 2), (1, 2)))
    key_weight = noise(splits[6], (SECTIONS, D, D), D ** -0.5, 0.1875, ((0, 2), (1, 2)))
    value_weight = noise(splits[7], (SECTIONS, D, D), D ** -0.5, 0.1875, ((0, 2), (1, 2)))
    value_bias = noise(splits[8], (SECTIONS, D), 0.5, 3.0, ((0, 2), (1, 2)))
    output_weight = noise(splits[9], (SECTIONS, D, D), (max(1, 2 * D // LMAX)) ** -0.5, 3.0, ((0, 2), (1, 2)))
    output_bias = noise(splits[10], (SECTIONS, D), 0.5, 3.0, ((0, 2), (1, 2)))
    first_gain = jnp.clip(1.0 + 0.1 * jax.random.normal(splits[11], (SECTIONS, D), jnp.float32), 0.5, 1.5).astype(jnp.bfloat16)
    first_bias = noise(splits[12], (SECTIONS, D), 0.5, 3.0, ((0, 2), (1, 2)))
    inner_weight = noise(splits[13], (SECTIONS, D, FF), D ** -0.5, 0.1875, ((0, 2), (1, 2)))
    inner_bias = noise(splits[14], (SECTIONS, FF), 0.5, 3.0, ((0, 2), (1, 2)))
    outer_weight = noise(splits[15], (SECTIONS, FF, D), FF ** -0.5, 0.09375, ((0, 2), (1, 2)))
    outer_bias = noise(splits[16], (SECTIONS, D), 0.5, 3.0, ((0, 2), (1, 2)))
    second_gain = jnp.clip(1.0 + 0.1 * jax.random.normal(splits[17], (SECTIONS, D), jnp.float32), 0.5, 1.5).astype(jnp.bfloat16)
    second_bias = noise(splits[18], (SECTIONS, D), 0.5, 3.0, ((0, 2), (1, 2)))
    return dict(inputs=inputs, cotangent=cotangent, lengths=lengths, permutation=permutation, query_weight=query_weight, query_bias=query_bias, key_weight=key_weight, value_weight=value_weight, value_bias=value_bias, output_weight=output_weight, output_bias=output_bias, first_gain=first_gain, first_bias=first_bias, inner_weight=inner_weight, inner_bias=inner_bias, outer_weight=outer_weight, outer_bias=outer_bias, second_gain=second_gain, second_bias=second_bias)


@jax.custom_vjp
def low(v):
    return lax.optimization_barrier(v.astype(jnp.bfloat16)).astype(jnp.float32)

@jax.custom_vjp
def low_back(v):
    return v

def low_keep(v):
    return (low(v), None)

def low_pass(kept, grad):
    return (grad,)

def back_keep(v):
    return (v, None)

def back_low(kept, grad):
    return (low(grad),)
low.defvjp(low_keep, low_pass)
low_back.defvjp(back_keep, back_low)
EPSILON = 1e-12
MASKED = -1000000000.0
PRECISE = lax.Precision.HIGHEST

def normalize(values, scaling, offset):
    average = lax.optimization_barrier(jnp.mean(values, axis=-1, keepdims=True))
    centred = values - average
    variance = lax.optimization_barrier(jnp.mean(centred * centred, axis=-1, keepdims=True))
    return centred * lax.rsqrt(variance + EPSILON) * scaling + offset

def matmul(left_side, right_side):
    return jnp.dot(left_side, right_side, precision=PRECISE, preferred_element_type=jnp.float32)

def layer_sequence(row_block, length, params):
    query_weight, query_bias, key_weight, value_weight, value_bias, output_weight, output_bias, first_gain, first_bias, inner_weight, inner_bias, outer_weight, outer_bias, second_gain, second_bias = params
    live = jnp.arange(LMAX) < length
    split_heads = (LMAX, HEADS, HEAD_DIM)
    queries = low_back(low(matmul(row_block, query_weight) + query_bias)).reshape(split_heads)
    key_rows = low_back(low(matmul(row_block, key_weight))).reshape(split_heads)
    values = low_back(low(matmul(row_block, value_weight) + value_bias)).reshape(split_heads)
    scores = low_back(jnp.einsum('qhd,khd->hqk', queries, key_rows, precision=PRECISE) * HEAD_DIM ** (-0.5))
    scores = jnp.where(live[None, None, :], scores, MASKED)
    highest = lax.optimization_barrier(jnp.max(scores, axis=-1, keepdims=True))
    exponent = jnp.exp(scores - highest)
    attention_weights = low(exponent / lax.optimization_barrier(jnp.sum(exponent, axis=-1, keepdims=True)))
    context = low_back(low(jnp.einsum('hqk,khd->qhd', attention_weights, values, precision=PRECISE).reshape(LMAX, D)))
    first_sum = row_block + low_back(matmul(context, output_weight) + output_bias)
    middle = normalize(first_sum, first_gain, first_bias)
    inner = low_back(matmul(low(middle), inner_weight) + inner_bias)
    activated = low(jax.nn.gelu(inner, approximate=False))
    second_sum = middle + low_back(matmul(activated, outer_weight) + outer_bias)
    return normalize(second_sum, second_gain, second_bias) * live.astype(jnp.float32)[:, None]

def segment_forward(row_blocks, lengths, params):

    def one_sequence(element):
        return layer_sequence(element[0], element[1], params)
    return lax.map(jax.checkpoint(one_sequence), (row_blocks, lengths))

def reference(inputs, cotangent, lengths, permutation, query_weight, query_bias, key_weight, value_weight, value_bias, output_weight, output_bias, first_gain, first_bias, inner_weight, inner_bias, outer_weight, outer_bias, second_gain, second_bias):
    weights = (query_weight, query_bias, key_weight, value_weight, value_bias, output_weight, output_bias, first_gain, first_bias, inner_weight, inner_bias, outer_weight, outer_bias, second_gain, second_bias)
    lower_params = tuple((weight[0].astype(jnp.float32) for weight in weights))
    upper_params = tuple((weight[1].astype(jnp.float32) for weight in weights))
    order = permutation.astype(jnp.int32)
    inverse = jnp.zeros(order.shape, jnp.int32).at[order].set(jnp.arange(order.shape[0], dtype=jnp.int32))
    own_cotangent = jnp.take(cotangent, inverse, axis=0)

    def apply_segment(row_blocks, params):
        return segment_forward(row_blocks, lengths, params)
    lower_out, lower_back = jax.vjp(apply_segment, inputs.astype(jnp.float32), lower_params)
    lower_act = lower_out.astype(jnp.bfloat16)
    upper_out, upper_back = jax.vjp(apply_segment, lower_act.astype(jnp.float32), upper_params)
    upper_act = upper_out.astype(jnp.bfloat16)
    upper_grad, upper_weights = upper_back(own_cotangent.astype(jnp.float32))
    upper_low = upper_grad.astype(jnp.bfloat16)
    lower_grad, lower_weights = lower_back(upper_low.astype(jnp.float32))
    stacked = [jnp.stack([lower_one, upper_one]) for lower_one, upper_one in zip(lower_weights, upper_weights)]
    grads_dealt = jnp.take(jnp.stack([lower_grad.astype(jnp.bfloat16), upper_low]), order, axis=1)
    return (jnp.stack([lower_act, upper_act]), grads_dealt, stacked[0], stacked[1], stacked[2], stacked[3], stacked[4], stacked[5], stacked[6], stacked[7], stacked[8], stacked[9], stacked[10], stacked[11], stacked[12], stacked[13], stacked[14])
```

```python
import jax
import jax.numpy as jnp
from jax import lax
from jax.experimental import pallas as pl
from jax.experimental.pallas import tpu as pltpu

ALL = ("section", "shard", "replica")
GROUP = ("shard", "replica")
UNITS = 12
DIRECT = (0, 1, 2)
DOUBLED = (3, 4, 5, 6, 7, 8, 9, 10, 11)
VMEM_LIMIT = 64000000


def my_bits(count):
    replica = lax.axis_index("replica")
    return tuple((lax.rem(replica // (1 << (count - 1 - p)), 2) for p in range(count)))


def across(p, count, bits):
    replica = lax.axis_index("replica")
    weight = 1 << (count - 1 - p)
    return {"replica": replica + weight * (1 - 2 * bits[p])}


def greet(partners):
    barrier = pltpu.get_barrier_semaphore()
    for partner in partners:
        pl.semaphore_signal(barrier, inc=1, device_id=partner, device_id_type=pl.DeviceIdType.MESH)
    pl.semaphore_wait(barrier, len(partners))


def remote(src, dst, send_sem, recv_sem, partner):
    return pltpu.make_async_remote_copy(
        src_ref=src,
        dst_ref=dst,
        send_sem=send_sem,
        recv_sem=recv_sem,
        device_id=partner,
        device_id_type=pl.DeviceIdType.MESH,
    )


def gather_kernel(
    count, wq, wk, wv, wo, w1, w2, small,
    oq, ok, ov, oo, o1, o2, osmall,
    stage, send_sem, recv_sem, load_sem, store_sem,
):
    core = lax.axis_index("section")
    side = lax.axis_index("shard")
    bits = my_bits(count)
    sibling = {"section": 1 - core}
    facing = {"shard": 1 - side}
    corner = {"section": 1 - core, "shard": 1 - side}
    everything = (slice(None),) * count

    def source(unit, index):
        if unit < 4:
            return (wq, wk, wv, wo)[unit].at[index]
        if unit < 8:
            return w1.at[index + (slice(None), pl.ds(1024 * (unit - 4), 1024))]
        return w2.at[(unit - 8,) + index]

    def target(unit, layer, half, index):
        if unit < 4:
            return (oq, ok, ov, oo)[unit].at[(layer, half) + index]
        if unit < 8:
            return o1.at[(layer, half) + index + (slice(None), pl.ds(1024 * (unit - 4), 1024))]
        return o2.at[(layer, half, unit - 8) + index]

    greet([sibling, facing, corner] + [across(p, count, bits) for p in range(count)])
    number = [0]
    sends = []

    def start(src, dst, partner):
        at = number[0]
        number[0] += 1
        copy = remote(src, dst, send_sem.at[at], recv_sem.at[at], partner)
        copy.start()
        sends.append(copy)
        return at

    def arrive(at, dst, partner):
        remote(dst, dst, send_sem.at[at], recv_sem.at[at], partner).wait_recv()

    first = {}
    for unit in DOUBLED:
        first[unit] = start(source(unit, bits), target(unit, core, side, bits), facing)
    small_at = [
        start(small, osmall.at[core, side], partner) for partner in (sibling, facing, corner)
    ]
    for unit in DIRECT:
        first[unit] = start(source(unit, everything), target(unit, core, side, everything), facing)
    loads = []
    for unit in range(UNITS):
        copy = pltpu.make_async_copy(source(unit, everything), stage.at[unit], load_sem.at[unit])
        copy.start()
        loads.append(copy)
    small_copy = pltpu.make_async_copy(small, osmall.at[core, side], store_sem.at[UNITS])
    small_copy.start()
    own = {}
    for unit in DOUBLED + DIRECT:
        own[unit] = start(source(unit, everything), target(unit, core, side, everything), sibling)
    stores = []
    for unit in range(UNITS):
        loads[unit].wait()
        copy = pltpu.make_async_copy(
            stage.at[unit], target(unit, core, side, everything), store_sem.at[unit]
        )
        copy.start()
        stores.append(copy)
    inflight = {unit: first[unit] for unit in range(UNITS)}
    passed = {}
    waiting = list(DIRECT)

    def finish_direct(unit):
        landed = target(unit, core, 1 - side, everything)
        arrive(inflight[unit], landed, facing)
        passed[unit] = start(landed, landed, sibling)

    for tick in range(len(DOUBLED) + count + 1):
        for step in reversed(range(count + 1)):
            j = tick - step
            if not 0 <= j < len(DOUBLED):
                continue
            unit = DOUBLED[j]
            if step == 0:
                arrive(inflight[unit], target(unit, core, 1 - side, bits), facing)
            else:
                p = step - 1
                landed = everything[:p] + (1 - bits[p],) + bits[p + 1 :]
                arrive(
                    inflight[unit], target(unit, core, 1 - side, landed), across(p, count, bits)
                )
            if step < count:
                held = target(unit, core, 1 - side, everything[:step] + bits[step:])
                inflight[unit] = start(held, held, across(step, count, bits))
            else:
                held = target(unit, core, 1 - side, everything)
                passed[unit] = start(held, held, sibling)
        if tick >= count + 2 and tick % 2 == 1 and waiting:
            finish_direct(waiting.pop(0))
    for unit in waiting:
        finish_direct(unit)
    for unit in range(UNITS):
        arrive(own[unit], target(unit, 1 - core, side, everything), sibling)
        arrive(passed[unit], target(unit, 1 - core, 1 - side, everything), sibling)
        stores[unit].wait()
    small_copy.wait()
    arrive(small_at[0], osmall.at[1 - core, side], sibling)
    arrive(small_at[1], osmall.at[core, 1 - side], facing)
    arrive(small_at[2], osmall.at[1 - core, 1 - side], corner)
    for copy in sends:
        copy.wait_send()


def gather_weights(shards, small, count):
    cut = (2,) * count
    rows = 512 // (1 << count)
    wq, wk, wv, wo, w1, w2 = shards
    narrow = cut + (rows, 1024)
    args = (
        [w.reshape(narrow) for w in (wq, wk, wv, wo)]
        + [w1.reshape(cut + (rows, 4096)), w2.reshape((4,) + narrow), small]
    )
    outs = (
        [jax.ShapeDtypeStruct((2, 2) + narrow, jnp.bfloat16)] * 4
        + [
            jax.ShapeDtypeStruct((2, 2) + cut + (rows, 4096), jnp.bfloat16),
            jax.ShapeDtypeStruct((2, 2, 4) + narrow, jnp.bfloat16),
            jax.ShapeDtypeStruct((2, 2) + small.shape, small.dtype),
        ]
    )
    copies = len(DOUBLED) * (count + 3) + len(DIRECT) * 3 + 3

    def kernel(*refs):
        args, outs, scratch = refs[:7], refs[7:14], refs[14:]
        flat = (scratch[0],) + scratch[1:]
        gather_kernel(count, *args, *outs, *flat)

    result = pl.pallas_call(
        kernel,
        out_shape=outs,
        in_specs=[pl.BlockSpec(memory_space=pl.ANY)] * 7,
        out_specs=[pl.BlockSpec(memory_space=pl.ANY)] * 7,
        scratch_shapes=[
            pltpu.VMEM((UNITS,) + narrow, jnp.bfloat16),
            pltpu.SemaphoreType.DMA((copies,)),
            pltpu.SemaphoreType.DMA((copies,)),
            pltpu.SemaphoreType.DMA((UNITS,)),
            pltpu.SemaphoreType.DMA((UNITS + 1,)),
        ],
        compiler_params=pltpu.CompilerParams(
            collective_id=0, has_side_effects=True, vmem_limit_bytes=VMEM_LIMIT
        ),
        name="gather_weights",
    )(*args)
    full = [w.reshape(2, 1024, 1024) for w in result[:4]]
    full += [result[4].reshape(2, 1024, 4096), result[5].reshape(2, 4096, 1024), result[6]]
    return full


def reduce_kernel(
    count, grads, small,
    total, small_total, landing,
    own, came, across_half, kept, from_x, *rest
):
    halves, rest = rest[:count], rest[count:]
    (small_own, small_recv, send0, recv0, send_x, recv_x, send_rs, recv_rs, send_ag, recv_ag,
     load_sem, came_sem, piece_sem, small_send, small_arrive) = rest
    core = lax.axis_index("section")
    side = lax.axis_index("shard")
    bits = my_bits(count)
    sibling = {"section": 1 - core}
    facing = {"shard": 1 - side}
    everything = (slice(None),) * count
    rows = kept.shape[-2]
    greet([sibling, facing] + [across(p, count, bits) for p in range(count)])

    def core_copy(unit):
        return remote(
            grads.at[1 - core, :, unit], landing.at[unit], send0.at[unit], recv0.at[unit], sibling
        )

    def x_copy(unit):
        return remote(
            across_half.at[unit], from_x.at[unit], send_x.at[unit], recv_x.at[unit], facing
        )

    def rs_copy(unit, p):
        return remote(
            kept.at[(unit,) + everything[:p] + (1 - bits[p],) + bits[p + 1 :]],
            halves[p].at[unit],
            send_rs.at[p, unit],
            recv_rs.at[p, unit],
            across(p, count, bits),
        )

    def ag_copy(unit, p):
        where = (unit,) + everything[:p] + bits[p:]
        source = kept.at[(unit,) + bits] if p == 0 else total.at[where]
        return remote(
            source, total.at[where], send_ag.at[p, unit], recv_ag.at[p, unit],
            across(p, count, bits),
        )

    def ag_arrive(unit, p):
        where = total.at[(unit,) + everything[:p] + (1 - bits[p],) + bits[p + 1 :]]
        remote(
            where, where, send_ag.at[p, unit], recv_ag.at[p, unit], across(p, count, bits)
        ).wait_recv()

    def piece_copy(unit):
        return pltpu.make_async_copy(
            kept.at[(unit,) + bits], total.at[(unit,) + bits], piece_sem.at[unit]
        )

    def own_load(unit):
        slot = lax.rem(unit, 2)
        return pltpu.make_async_copy(grads.at[core, :, unit], own.at[slot], load_sem.at[slot])

    def small_copy(step):
        partner = [sibling, facing] + [across(p, count, bits) for p in range(count)]
        source = small.at[1 - core] if step == 0 else small_own.at[step - 1]
        return remote(
            source, small_recv.at[step], small_send.at[step], small_arrive.at[step], partner[step]
        )

    small_copy(0).start()

    def first(unit, carry):
        core_copy(unit).start()
        return carry

    lax.fori_loop(0, UNITS, first, 0)
    own_load(0).start()
    small_steps = count + 2

    def tick(now, carry):
        for step in range(small_steps):
            @pl.when(now == step + 1)
            def _():
                small_copy(step).wait_recv()
                before = small[core] if step == 0 else small_own[step - 1]
                small_own[step] = before + small_recv[step]
                if step + 1 < small_steps:
                    small_copy(step + 1).start()

        @pl.when(now < UNITS)
        def _():
            unit = now
            slot = lax.rem(unit, 2)

            @pl.when(unit + 1 < UNITS)
            def _():
                own_load(unit + 1).start()

            core_copy(unit).wait_recv()
            arrived = pltpu.make_async_copy(landing.at[unit], came, came_sem)
            arrived.start()
            own_load(unit).wait()
            arrived.wait()
            def add(block, c):
                where = pl.ds(pl.multiple_of(block * 32, 32), 32)
                across_half[unit, where] = own[slot, 1 - side, where] + came[1 - side, where]
                return c

            lax.fori_loop(0, 16, add, 0)
            x_copy(unit).start()

            def add_kept(index, c):
                where = pl.ds(pl.multiple_of(index * rows, rows), rows)
                places = tuple(
                    (lax.rem(index // (1 << (count - 1 - p)), 2) for p in range(count))
                )
                kept[(unit,) + places] = own[slot, side, where] + came[side, where]
                return c

            lax.fori_loop(0, 1 << count, add_kept, 0)

        @pl.when(jnp.logical_and(now >= 1, now < UNITS + 1))
        def _():
            unit = now - 1
            x_copy(unit).wait_recv()

            def add(index, c):
                where = pl.ds(pl.multiple_of(index * rows, rows), rows)
                places = tuple(
                    (lax.rem(index // (1 << (count - 1 - p)), 2) for p in range(count))
                )
                kept[(unit,) + places] = kept[(unit,) + places] + from_x[unit, where]
                return c

            lax.fori_loop(0, 1 << count, add, 0)
            rs_copy(unit, count - 1).start()

        for step in range(count):
            p = count - 1 - step

            @pl.when(jnp.logical_and(now >= 2 + step, now < UNITS + 2 + step))
            def _():
                unit = now - (2 + step)
                rs_copy(unit, p).wait_recv()

                def add(index, c):
                    places = tuple((lax.rem(index // (1 << (p - 1 - q)), 2) for q in range(p)))
                    mine = (unit,) + places + bits[p:]
                    kept[mine] = kept[mine] + halves[p][(unit,) + places]
                    return c

                if p == 0:
                    add(0, 0)
                    piece_copy(unit).start()
                    ag_copy(unit, 0).start()
                else:
                    lax.fori_loop(0, 1 << p, add, 0)
                    rs_copy(unit, p - 1).start()

        for p in range(count):
            lag = 2 + count + p

            @pl.when(jnp.logical_and(now >= lag, now < UNITS + lag))
            def _():
                unit = now - lag
                ag_arrive(unit, p)
                if p == 0:
                    piece_copy(unit).wait()
                if p + 1 < count:
                    ag_copy(unit, p + 1).start()

        return carry

    lax.fori_loop(0, UNITS + 2 + 2 * count, tick, 0)
    out = pltpu.make_async_copy(small_own.at[small_steps - 1], small_total, piece_sem.at[UNITS])
    out.start()

    def last(unit, carry):
        core_copy(unit).wait_send()
        x_copy(unit).wait_send()
        for p in range(count):
            rs_copy(unit, p).wait_send()
            ag_copy(unit, p).wait_send()
        return carry

    lax.fori_loop(0, UNITS, last, 0)
    for step in range(small_steps):
        small_copy(step).wait_send()
    out.wait()


def reduce_grads(grads, small, count):
    cut = (2,) * count
    rows = 512 // (1 << count)
    narrow = cut + (rows, 1024)
    dma = pltpu.SemaphoreType.DMA

    def kernel(*refs):
        reduce_kernel(count, *refs)

    vectors = small.shape[1:]
    total, small_total, _ = pl.pallas_call(
        kernel,
        out_shape=[
            jax.ShapeDtypeStruct((UNITS,) + narrow, jnp.bfloat16),
            jax.ShapeDtypeStruct(vectors, jnp.float32),
            jax.ShapeDtypeStruct((UNITS, 2, 512, 1024), jnp.bfloat16),
        ],
        in_specs=[
            pl.BlockSpec(memory_space=pl.ANY),
            pl.BlockSpec(memory_space=pltpu.VMEM),
        ],
        out_specs=[pl.BlockSpec(memory_space=pl.ANY)] * 3,
        scratch_shapes=[
            pltpu.VMEM((2, 2, 512, 1024), jnp.bfloat16),
            pltpu.VMEM((2, 512, 1024), jnp.bfloat16),
            pltpu.VMEM((UNITS, 512, 1024), jnp.bfloat16),
            pltpu.VMEM((UNITS,) + narrow, jnp.bfloat16),
            pltpu.VMEM((UNITS, 512, 1024), jnp.bfloat16),
        ]
        + [pltpu.VMEM((UNITS,) + (2,) * p + (rows, 1024), jnp.bfloat16) for p in range(count)]
        + [
            pltpu.VMEM((count + 2,) + vectors, jnp.float32),
            pltpu.VMEM((count + 2,) + vectors, jnp.float32),
            dma((UNITS,)),
            dma((UNITS,)),
            dma((UNITS,)),
            dma((UNITS,)),
            dma((count, UNITS)),
            dma((count, UNITS)),
            dma((count, UNITS)),
            dma((count, UNITS)),
            dma((2,)),
            dma,
            dma((UNITS + 1,)),
            dma((count + 2,)),
            dma((count + 2,)),
        ],
        compiler_params=pltpu.CompilerParams(
            collective_id=1, has_side_effects=True, vmem_limit_bytes=VMEM_LIMIT
        ),
        name="reduce_grads",
    )(grads, small)
    return total.reshape(UNITS, 512, 1024), small_total
from jax.sharding import PartitionSpec as P

HEAD_DIM = 64
EPSILON = 1e-12
MASKED = -1000000000.0
VECTORS = (1, 1, 1, 1, 1, 4, 1, 1, 1)


def dense(left_side, right_side):
    return jnp.dot(left_side, right_side, preferred_element_type=jnp.float32)


def dense_left(left_side, right_side):
    return jnp.einsum("ra,rb->ab", left_side, right_side, preferred_element_type=jnp.float32)


def dense_right(left_side, right_side):
    return jnp.einsum("rb,ab->ra", left_side, right_side, preferred_element_type=jnp.float32)


def normalized(values):
    average = jnp.mean(values, axis=-1, keepdims=True)
    centred = values - average
    variance = jnp.mean(centred * centred, axis=-1, keepdims=True)
    scale = lax.rsqrt(variance + EPSILON)
    return centred * scale, scale


def normalize_back(grad, unit, scale, gain):
    gs = grad * gain
    mean_gs = jnp.mean(gs, axis=-1, keepdims=True)
    mean_gn = jnp.mean(gs * unit, axis=-1, keepdims=True)
    return (gs - mean_gs - unit * mean_gn) * scale


def layer_forward(x, live, params):
    wq, wk, wv, wo, w1, w2, (bq, bv, bo, g1, b1, bi, b2, g2, bb2) = params
    slots = x.shape[0]
    heads = (slots, 16, HEAD_DIM)
    q = (dense(x, wq) + bq).astype(jnp.bfloat16).reshape(heads)
    k = dense(x, wk).astype(jnp.bfloat16).reshape(heads)
    v = (dense(x, wv) + bv).astype(jnp.bfloat16).reshape(heads)
    scores = jnp.einsum("qhd,khd->hqk", q, k, preferred_element_type=jnp.float32) * 0.125
    scores = jnp.where(live[None, None, :], scores, MASKED)
    highest = jnp.max(scores, axis=-1, keepdims=True)
    exponent = jnp.exp(scores - highest)
    totals = jnp.sum(exponent, axis=-1, keepdims=True)
    probs = (exponent / totals).astype(jnp.bfloat16)
    log_total = highest + jnp.log(totals)
    context = jnp.einsum("hqk,khd->qhd", probs, v, preferred_element_type=jnp.float32)
    context = context.astype(jnp.bfloat16).reshape(slots, -1)
    first_sum = x.astype(jnp.float32) + (dense(context, wo) + bo)
    unit1, scale1 = normalized(first_sum)
    middle = unit1 * g1 + b1
    middle_low = middle.astype(jnp.bfloat16)
    inner = dense(middle_low, w1) + bi
    cdf = 0.5 * (1.0 + lax.erf(inner * 0.7071067811865476))
    activated = (inner * cdf).astype(jnp.bfloat16)
    slope = (cdf + inner * (jnp.exp(-0.5 * inner * inner) * 0.3989422804014327)).astype(
        jnp.bfloat16
    )
    second_sum = middle + (dense(activated, w2) + b2)
    unit2, scale2 = normalized(second_sum)
    row_mask = live[:, None].astype(jnp.float32)
    result = ((unit2 * g2 + bb2) * row_mask).astype(jnp.bfloat16)
    return result, (q, k, v, log_total, context, unit1, scale1, middle_low, activated, slope, unit2, scale2)


def layer_backward(grad, x, live, params, stored):
    wq, wk, wv, wo, w1, w2, (bq, bv, bo, g1, b1, bi, b2, g2, bb2) = params
    q, k, v, log_total, context, unit1, scale1, middle_low, activated, slope, unit2, scale2 = stored
    slots = x.shape[0]
    heads = (slots, 16, HEAD_DIM)
    g = grad.astype(jnp.float32) * live[:, None].astype(jnp.float32)
    d_second = normalize_back(g, unit2, scale2, g2)
    d_g2, d_bb2 = jnp.sum(g * unit2, axis=0), jnp.sum(g, axis=0)
    d_outer = d_second.astype(jnp.bfloat16)
    d_inner = (dense_right(d_outer, w2) * slope.astype(jnp.float32)).astype(jnp.bfloat16)
    d_middle = d_second + dense_right(d_inner, w1)
    d_first = normalize_back(d_middle, unit1, scale1, g1)
    d_g1, d_b1 = jnp.sum(d_middle * unit1, axis=0), jnp.sum(d_middle, axis=0)
    d_att = d_first.astype(jnp.bfloat16)
    d_context = dense_right(d_att, wo).astype(jnp.bfloat16).reshape(heads)
    scores = jnp.einsum("qhd,khd->hqk", q, k, preferred_element_type=jnp.float32) * 0.125
    scores = jnp.where(live[None, None, :], scores, MASKED)
    probs = jnp.exp(scores - log_total)
    d_v = jnp.einsum(
        "hqk,qhd->khd", probs.astype(jnp.bfloat16), d_context, preferred_element_type=jnp.float32
    )
    d_v = d_v.astype(jnp.bfloat16).reshape(slots, -1)
    d_probs = jnp.einsum("qhd,khd->hqk", d_context, v, preferred_element_type=jnp.float32)
    dots = jnp.sum(probs * d_probs, axis=-1, keepdims=True)
    d_scores = (probs * (d_probs - dots)).astype(jnp.bfloat16)
    d_q = jnp.einsum("hqk,khd->qhd", d_scores, k, preferred_element_type=jnp.float32) * 0.125
    d_k = jnp.einsum("hqk,qhd->khd", d_scores, q, preferred_element_type=jnp.float32) * 0.125
    d_q = d_q.astype(jnp.bfloat16).reshape(slots, -1)
    d_k = d_k.astype(jnp.bfloat16).reshape(slots, -1)
    d_x = d_first + dense_right(d_q, wq) + dense_right(d_k, wk) + dense_right(d_v, wv)

    def sums(values):
        return jnp.sum(values, axis=0, dtype=jnp.float32)

    vectors = (
        sums(d_q), sums(d_v), sums(d_att), d_g1, d_b1, sums(d_inner), sums(d_outer), d_g2, d_bb2
    )
    matrices = [
        dense_left(x, d_q), dense_left(x, d_k), dense_left(x, d_v), dense_left(context, d_att),
        dense_left(middle_low, d_inner), dense_left(activated, d_outer),
    ]
    low = [m.astype(jnp.bfloat16) for m in matrices]
    packed = [m.reshape(2, 1, 512, 1024) for m in low[:4]]
    packed += [low[4].reshape(2, 512, 4, 1024).transpose(0, 2, 1, 3), low[5].reshape(2, 4, 512, 1024)]
    return (
        d_x.astype(jnp.bfloat16),
        jnp.concatenate(packed, axis=1),
        jnp.concatenate([v.reshape(2, -1) for v in vectors], axis=1).reshape(96, 128),
    )


def split_vectors(packed):
    halves = packed.reshape(2, -1)
    out, at = [], 0
    for width in VECTORS:
        out.append(halves[:, at : at + 512 * width].reshape(-1).astype(jnp.float32))
        at += 512 * width
    return tuple(out)


def device_of(number, groups):
    return lax.rem(number, 2) * groups + number // 2


def own_cotangent(cotangent, permutation, groups):
    core = lax.axis_index("section")
    total = permutation.shape[0]
    mine = lax.dynamic_index_in_dim(cotangent, core, 0, keepdims=False)
    shape = mine.shape
    chunks = mine.reshape(2 * groups, shape[0] // (2 * groups), shape[1])
    spread = lax.all_to_all(chunks, ALL, 0, 0, tiled=True)
    device = jnp.arange(total, dtype=jnp.int32)
    number = 2 * lax.rem(device, groups) + device // groups
    slot = jnp.sum(
        jnp.where(permutation[None, :] == number[:, None], device[None, :], 0), axis=1
    )
    ordered = jnp.take(spread, device_of(slot, groups), axis=0)
    return lax.all_to_all(ordered, ALL, 0, 0, tiled=True).reshape(shape)


def dealt_grads(both, permutation, groups):
    slots, width = both.shape[1:]
    rows = slots // groups
    spread = lax.all_to_all(both.reshape(2 * groups, rows, width), ALL, 0, 0, tiled=True)
    ordered = jnp.take(spread, device_of(permutation, groups), axis=0)
    ordered = ordered.reshape(groups, 2, rows, width)
    home = lax.all_to_all(ordered, GROUP, 0, 0, tiled=True)
    return home.transpose(1, 0, 2, 3).reshape(2, slots, width)


def on_device(
    inputs, cotangent, lengths, permutation, query_weight, query_bias, key_weight, value_weight,
    value_bias, output_weight, output_bias, first_gain, first_bias, inner_weight, inner_bias,
    outer_weight, outer_bias, second_gain, second_bias,
):
    core = lax.axis_index("section")
    group = lax.axis_index(GROUP)
    groups = lax.axis_size(GROUP)
    count = lax.axis_size("replica").bit_length() - 1
    slots = inputs.shape[1]
    shards = [
        w[0] for w in (query_weight, key_weight, value_weight, output_weight, inner_weight, outer_weight)
    ]
    vectors = [
        v[0] for v in (query_bias, value_bias, output_bias, first_gain, first_bias, inner_bias,
                       outer_bias, second_gain, second_bias)
    ]
    full = gather_weights(shards, jnp.concatenate(vectors).reshape(48, 128), count)
    layers = [tuple(w[s] for w in full[:6]) + (split_vectors(full[6][s]),) for s in range(2)]
    length = lax.dynamic_index_in_dim(lengths, 2 * group + core, 0, keepdims=False)
    live = jnp.arange(slots, dtype=jnp.int32) < length
    x = lax.dynamic_index_in_dim(inputs, core, 0, keepdims=False)
    grad = own_cotangent(cotangent, permutation, groups)
    lower, lower_stored = layer_forward(x, live, layers[0])
    upper, upper_stored = layer_forward(lower, live, layers[1])
    upper_grad, upper_packed, upper_small = layer_backward(grad, lower, live, layers[1], upper_stored)
    lower_grad, lower_packed, lower_small = layer_backward(
        upper_grad, x, live, layers[0], lower_stored
    )
    total, small = reduce_grads(
        jnp.stack([lower_packed, upper_packed]), jnp.stack([lower_small, upper_small]), count
    )
    sent = jnp.where(core == 0, upper, lower)
    kept = jnp.where(core == 0, lower, upper)
    came = lax.ppermute(sent, "section", [(0, 1), (1, 0)])
    activations = jnp.where(core == 0, jnp.stack([kept, came]), jnp.stack([came, kept]))[None]
    input_grads = dealt_grads(jnp.stack([lower_grad, upper_grad]), permutation, groups)[None]
    wide = total.astype(jnp.float32)
    side = lax.axis_index("shard")
    own = lax.dynamic_index_in_dim(small.reshape(2, -1), side, 0, keepdims=False)
    pieces, at = [], 0
    for width in VECTORS:
        pieces.append(own[None, at : at + 512 * width])
        at += 512 * width
    dq, dk, dv, do = (wide[i][None] for i in range(4))
    d1 = wide[4:8].transpose(1, 0, 2).reshape(1, 512, 4096)
    d2 = wide[8:12].reshape(1, 2048, 1024)
    return (
        activations, input_grads, dq, pieces[0], dk, dv, pieces[1], do, pieces[2], pieces[3],
        pieces[4], d1, pieces[5], d2, pieces[6], pieces[7], pieces[8],
    )


def solution(mesh):
    matrix, vector = P("section", "shard", None), P("section", "shard")
    rows = P(("shard", "replica"), None, None)
    in_specs = (
        rows, rows, P(), P(), matrix, vector, matrix, matrix, vector, matrix, vector, vector,
        vector, matrix, vector, matrix, vector, vector, vector,
    )
    both = P("section", ("shard", "replica"), None, None)
    out_specs = (
        both, both, matrix, vector, matrix, matrix, vector, matrix, vector, vector, vector,
        matrix, vector, matrix, vector, vector, vector,
    )
    return jax.shard_map(
        on_device, mesh=mesh, in_specs=in_specs, out_specs=out_specs, check_vma=False
    )
```

```python
import jax
import jax.numpy as jnp
from jax import lax
from jax.experimental import pallas as pl
from jax.experimental.pallas import tpu as pltpu

ALL = ("section", "shard", "replica")
GROUP = ("shard", "replica")
UNITS = 12
DIRECT = (0, 1, 2)
DOUBLED = (3, 4, 5, 6, 7, 8, 9, 10, 11)
VMEM_LIMIT = 64000000


def my_bits(count):
    replica = lax.axis_index("replica")
    return tuple((lax.rem(replica // (1 << (count - 1 - p)), 2) for p in range(count)))


def across(p, count, bits):
    replica = lax.axis_index("replica")
    weight = 1 << (count - 1 - p)
    return {"replica": replica + weight * (1 - 2 * bits[p])}


def greet(partners):
    barrier = pltpu.get_barrier_semaphore()
    for partner in partners:
        pl.semaphore_signal(barrier, inc=1, device_id=partner, device_id_type=pl.DeviceIdType.MESH)
    pl.semaphore_wait(barrier, len(partners))


def remote(src, dst, send_sem, recv_sem, partner):
    return pltpu.make_async_remote_copy(
        src_ref=src,
        dst_ref=dst,
        send_sem=send_sem,
        recv_sem=recv_sem,
        device_id=partner,
        device_id_type=pl.DeviceIdType.MESH,
    )


def gather_kernel(
    count, wq, wk, wv, wo, w1, w2, small,
    oq, ok, ov, oo, o1, o2, osmall,
    stage, send_sem, recv_sem, load_sem, store_sem,
):
    core = lax.axis_index("section")
    side = lax.axis_index("shard")
    bits = my_bits(count)
    sibling = {"section": 1 - core}
    facing = {"shard": 1 - side}
    corner = {"section": 1 - core, "shard": 1 - side}
    everything = (slice(None),) * count

    def source(unit, index):
        if unit < 4:
            return (wq, wk, wv, wo)[unit].at[index]
        if unit < 8:
            return w1.at[index + (slice(None), pl.ds(1024 * (unit - 4), 1024))]
        return w2.at[(unit - 8,) + index]

    def target(unit, layer, half, index):
        if unit < 4:
            return (oq, ok, ov, oo)[unit].at[(layer, half) + index]
        if unit < 8:
            return o1.at[(layer, half) + index + (slice(None), pl.ds(1024 * (unit - 4), 1024))]
        return o2.at[(layer, half, unit - 8) + index]

    greet([sibling, facing, corner] + [across(p, count, bits) for p in range(count)])
    number = [0]
    sends = []

    def start(src, dst, partner):
        at = number[0]
        number[0] += 1
        copy = remote(src, dst, send_sem.at[at], recv_sem.at[at], partner)
        copy.start()
        sends.append(copy)
        return at

    def arrive(at, dst, partner):
        remote(dst, dst, send_sem.at[at], recv_sem.at[at], partner).wait_recv()

    first = {}
    for unit in DOUBLED:
        first[unit] = start(source(unit, bits), target(unit, core, side, bits), facing)
    small_at = [
        start(small, osmall.at[core, side], partner) for partner in (sibling, facing, corner)
    ]
    for unit in DIRECT:
        first[unit] = start(source(unit, everything), target(unit, core, side, everything), facing)
    loads = []
    for unit in range(UNITS):
        copy = pltpu.make_async_copy(source(unit, everything), stage.at[unit], load_sem.at[unit])
        copy.start()
        loads.append(copy)
    small_copy = pltpu.make_async_copy(small, osmall.at[core, side], store_sem.at[UNITS])
    small_copy.start()
    own = {}
    for unit in DOUBLED + DIRECT:
        own[unit] = start(source(unit, everything), target(unit, core, side, everything), sibling)
    stores = []
    for unit in range(UNITS):
        loads[unit].wait()
        copy = pltpu.make_async_copy(
            stage.at[unit], target(unit, core, side, everything), store_sem.at[unit]
        )
        copy.start()
        stores.append(copy)
    inflight = {unit: first[unit] for unit in range(UNITS)}
    passed = {}
    waiting = list(DIRECT)

    def finish_direct(unit):
        landed = target(unit, core, 1 - side, everything)
        arrive(inflight[unit], landed, facing)
        passed[unit] = start(landed, landed, sibling)

    for tick in range(len(DOUBLED) + count + 1):
        for step in reversed(range(count + 1)):
            j = tick - step
            if not 0 <= j < len(DOUBLED):
                continue
            unit = DOUBLED[j]
            if step == 0:
                arrive(inflight[unit], target(unit, core, 1 - side, bits), facing)
            else:
                p = step - 1
                landed = everything[:p] + (1 - bits[p],) + bits[p + 1 :]
                arrive(
                    inflight[unit], target(unit, core, 1 - side, landed), across(p, count, bits)
                )
            if step < count:
                held = target(unit, core, 1 - side, everything[:step] + bits[step:])
                inflight[unit] = start(held, held, across(step, count, bits))
            else:
                held = target(unit, core, 1 - side, everything)
                passed[unit] = start(held, held, sibling)
        if tick >= count + 2 and tick % 2 == 1 and waiting:
            finish_direct(waiting.pop(0))
    for unit in waiting:
        finish_direct(unit)
    for unit in range(UNITS):
        arrive(own[unit], target(unit, 1 - core, side, everything), sibling)
        arrive(passed[unit], target(unit, 1 - core, 1 - side, everything), sibling)
        stores[unit].wait()
    small_copy.wait()
    arrive(small_at[0], osmall.at[1 - core, side], sibling)
    arrive(small_at[1], osmall.at[core, 1 - side], facing)
    arrive(small_at[2], osmall.at[1 - core, 1 - side], corner)
    for copy in sends:
        copy.wait_send()


def gather_weights(shards, small, count):
    cut = (2,) * count
    rows = 512 // (1 << count)
    wq, wk, wv, wo, w1, w2 = shards
    narrow = cut + (rows, 1024)
    args = (
        [w.reshape(narrow) for w in (wq, wk, wv, wo)]
        + [w1.reshape(cut + (rows, 4096)), w2.reshape((4,) + narrow), small]
    )
    outs = (
        [jax.ShapeDtypeStruct((2, 2) + narrow, jnp.bfloat16)] * 4
        + [
            jax.ShapeDtypeStruct((2, 2) + cut + (rows, 4096), jnp.bfloat16),
            jax.ShapeDtypeStruct((2, 2, 4) + narrow, jnp.bfloat16),
            jax.ShapeDtypeStruct((2, 2) + small.shape, small.dtype),
        ]
    )
    copies = len(DOUBLED) * (count + 3) + len(DIRECT) * 3 + 3

    def kernel(*refs):
        args, outs, scratch = refs[:7], refs[7:14], refs[14:]
        flat = (scratch[0],) + scratch[1:]
        gather_kernel(count, *args, *outs, *flat)

    result = pl.pallas_call(
        kernel,
        out_shape=outs,
        in_specs=[pl.BlockSpec(memory_space=pl.ANY)] * 7,
        out_specs=[pl.BlockSpec(memory_space=pl.ANY)] * 7,
        scratch_shapes=[
            pltpu.VMEM((UNITS,) + narrow, jnp.bfloat16),
            pltpu.SemaphoreType.DMA((copies,)),
            pltpu.SemaphoreType.DMA((copies,)),
            pltpu.SemaphoreType.DMA((UNITS,)),
            pltpu.SemaphoreType.DMA((UNITS + 1,)),
        ],
        compiler_params=pltpu.CompilerParams(
            collective_id=0, has_side_effects=True, vmem_limit_bytes=VMEM_LIMIT
        ),
        name="gather_weights",
    )(*args)
    full = [w.reshape(2, 1024, 1024) for w in result[:4]]
    full += [result[4].reshape(2, 1024, 4096), result[5].reshape(2, 4096, 1024), result[6]]
    return full


def reduce_kernel(
    count, parts, small,
    total, small_total, landing,
    own, came, across_half, kept, from_x, *rest
):
    halves, rest = rest[:count], rest[count:]
    (small_own, small_recv, send0, recv0, send_x, recv_x, send_rs, recv_rs, send_ag, recv_ag,
     load_sem, came_sem, piece_sem, small_send, small_arrive) = rest
    core = lax.axis_index("section")
    side = lax.axis_index("shard")
    bits = my_bits(count)
    sibling = {"section": 1 - core}
    facing = {"shard": 1 - side}
    everything = (slice(None),) * count
    rows = kept.shape[-2]
    greet([sibling, facing] + [across(p, count, bits) for p in range(count)])

    ranges, at = [], 0
    for part in parts:
        ranges.append((part, at, at + part.shape[2]))
        at += part.shape[2]

    def core_copy(unit):
        source = landing.at[unit]
        if isinstance(unit, int):
            part, low, _ = [entry for entry in ranges if entry[1] <= unit < entry[2]][0]
            source = part.at[1 - core, :, unit - low]
        return remote(source, landing.at[unit], send0.at[unit], recv0.at[unit], sibling)

    def x_copy(unit):
        return remote(
            across_half.at[unit], from_x.at[unit], send_x.at[unit], recv_x.at[unit], facing
        )

    def rs_copy(unit, p):
        return remote(
            kept.at[(unit,) + everything[:p] + (1 - bits[p],) + bits[p + 1 :]],
            halves[p].at[unit],
            send_rs.at[p, unit],
            recv_rs.at[p, unit],
            across(p, count, bits),
        )

    def ag_copy(unit, p):
        where = (unit,) + everything[:p] + bits[p:]
        source = kept.at[(unit,) + bits] if p == 0 else total.at[where]
        return remote(
            source, total.at[where], send_ag.at[p, unit], recv_ag.at[p, unit],
            across(p, count, bits),
        )

    def ag_arrive(unit, p):
        where = total.at[(unit,) + everything[:p] + (1 - bits[p],) + bits[p + 1 :]]
        remote(
            where, where, send_ag.at[p, unit], recv_ag.at[p, unit], across(p, count, bits)
        ).wait_recv()

    def piece_copy(unit):
        return pltpu.make_async_copy(
            kept.at[(unit,) + bits], total.at[(unit,) + bits], piece_sem.at[unit]
        )

    def own_load(part, index, slot):
        return pltpu.make_async_copy(part.at[core, :, index], own.at[slot], load_sem.at[slot])

    def start_load(unit):
        for part, low, high in ranges:
            @pl.when(jnp.logical_and(unit >= low, unit < high))
            def _():
                own_load(part, unit - low, lax.rem(unit, 2)).start()

    def small_copy(step):
        partner = [sibling, facing] + [across(p, count, bits) for p in range(count)]
        source = small.at[1 - core] if step == 0 else small_own.at[step - 1]
        return remote(
            source, small_recv.at[step], small_send.at[step], small_arrive.at[step], partner[step]
        )

    small_copy(0).start()

    for unit in range(UNITS):
        core_copy(unit).start()
    own_load(parts[0], 0, 0).start()
    small_steps = count + 2

    def tick(now, carry):
        for step in range(small_steps):
            @pl.when(now == step + 1)
            def _():
                small_copy(step).wait_recv()
                before = small[core] if step == 0 else small_own[step - 1]
                small_own[step] = before + small_recv[step]
                if step + 1 < small_steps:
                    small_copy(step + 1).start()

        @pl.when(now < UNITS)
        def _():
            unit = now
            slot = lax.rem(unit, 2)

            @pl.when(unit + 1 < UNITS)
            def _():
                start_load(unit + 1)

            core_copy(unit).wait_recv()
            arrived = pltpu.make_async_copy(landing.at[unit], came, came_sem)
            arrived.start()
            own_load(parts[0], 0, slot).wait()
            arrived.wait()
            def add(block, c):
                where = pl.ds(pl.multiple_of(block * 32, 32), 32)
                across_half[unit, where] = own[slot, 1 - side, where] + came[1 - side, where]
                return c

            lax.fori_loop(0, 16, add, 0)
            x_copy(unit).start()

            def add_kept(index, c):
                where = pl.ds(pl.multiple_of(index * rows, rows), rows)
                places = tuple(
                    (lax.rem(index // (1 << (count - 1 - p)), 2) for p in range(count))
                )
                kept[(unit,) + places] = own[slot, side, where] + came[side, where]
                return c

            lax.fori_loop(0, 1 << count, add_kept, 0)

        @pl.when(jnp.logical_and(now >= 1, now < UNITS + 1))
        def _():
            unit = now - 1
            x_copy(unit).wait_recv()

            def add(index, c):
                where = pl.ds(pl.multiple_of(index * rows, rows), rows)
                places = tuple(
                    (lax.rem(index // (1 << (count - 1 - p)), 2) for p in range(count))
                )
                kept[(unit,) + places] = kept[(unit,) + places] + from_x[unit, where]
                return c

            lax.fori_loop(0, 1 << count, add, 0)
            rs_copy(unit, count - 1).start()

        for step in range(count):
            p = count - 1 - step

            @pl.when(jnp.logical_and(now >= 2 + step, now < UNITS + 2 + step))
            def _():
                unit = now - (2 + step)
                rs_copy(unit, p).wait_recv()

                def add(index, c):
                    places = tuple((lax.rem(index // (1 << (p - 1 - q)), 2) for q in range(p)))
                    mine = (unit,) + places + bits[p:]
                    kept[mine] = kept[mine] + halves[p][(unit,) + places]
                    return c

                if p == 0:
                    add(0, 0)
                    piece_copy(unit).start()
                    ag_copy(unit, 0).start()
                else:
                    lax.fori_loop(0, 1 << p, add, 0)
                    rs_copy(unit, p - 1).start()

        for p in range(count):
            lag = 2 + count + p

            @pl.when(jnp.logical_and(now >= lag, now < UNITS + lag))
            def _():
                unit = now - lag
                ag_arrive(unit, p)
                if p == 0:
                    piece_copy(unit).wait()
                if p + 1 < count:
                    ag_copy(unit, p + 1).start()

        return carry

    lax.fori_loop(0, UNITS + 2 + 2 * count, tick, 0)
    out = pltpu.make_async_copy(small_own.at[small_steps - 1], small_total, piece_sem.at[UNITS])
    out.start()

    def last(unit, carry):
        core_copy(unit).wait_send()
        x_copy(unit).wait_send()
        for p in range(count):
            rs_copy(unit, p).wait_send()
            ag_copy(unit, p).wait_send()
        return carry

    lax.fori_loop(0, UNITS, last, 0)
    for step in range(small_steps):
        small_copy(step).wait_send()
    out.wait()


def reduce_grads(parts, small, count):
    cut = (2,) * count
    rows = 512 // (1 << count)
    narrow = cut + (rows, 1024)
    dma = pltpu.SemaphoreType.DMA

    held = len(parts)

    def kernel(*refs):
        reduce_kernel(count, refs[:held], *refs[held:])

    vectors = small.shape[1:]
    total, small_total, _ = pl.pallas_call(
        kernel,
        out_shape=[
            jax.ShapeDtypeStruct((UNITS,) + narrow, jnp.bfloat16),
            jax.ShapeDtypeStruct(vectors, jnp.float32),
            jax.ShapeDtypeStruct((UNITS, 2, 512, 1024), jnp.bfloat16),
        ],
        in_specs=[pl.BlockSpec(memory_space=pl.ANY)] * held
        + [pl.BlockSpec(memory_space=pltpu.VMEM)],
        out_specs=[pl.BlockSpec(memory_space=pl.ANY)] * 3,
        scratch_shapes=[
            pltpu.VMEM((2, 2, 512, 1024), jnp.bfloat16),
            pltpu.VMEM((2, 512, 1024), jnp.bfloat16),
            pltpu.VMEM((UNITS, 512, 1024), jnp.bfloat16),
            pltpu.VMEM((UNITS,) + narrow, jnp.bfloat16),
            pltpu.VMEM((UNITS, 512, 1024), jnp.bfloat16),
        ]
        + [pltpu.VMEM((UNITS,) + (2,) * p + (rows, 1024), jnp.bfloat16) for p in range(count)]
        + [
            pltpu.VMEM((count + 2,) + vectors, jnp.float32),
            pltpu.VMEM((count + 2,) + vectors, jnp.float32),
            dma((UNITS,)),
            dma((UNITS,)),
            dma((UNITS,)),
            dma((UNITS,)),
            dma((count, UNITS)),
            dma((count, UNITS)),
            dma((count, UNITS)),
            dma((count, UNITS)),
            dma((2,)),
            dma,
            dma((UNITS + 1,)),
            dma((count + 2,)),
            dma((count + 2,)),
        ],
        compiler_params=pltpu.CompilerParams(
            collective_id=1, has_side_effects=True, vmem_limit_bytes=VMEM_LIMIT
        ),
        name="reduce_grads",
    )(*parts, small)
    return total.reshape(UNITS, 512, 1024), small_total


HEAD_DIM = 64
EPSILON = 1e-12
MASKED = -1000000000.0
HIDDEN_BLOCK = 512
WIDE = 256
BF = jnp.bfloat16
F32 = jnp.float32


def mm(a, b):
    return lax.dot_general(a, b, (((1,), (0,)), ((), ())), preferred_element_type=F32)


def mm_right(a, b):
    return lax.dot_general(a, b, (((1,), (1,)), ((), ())), preferred_element_type=F32)


def mm_left(a, b):
    return lax.dot_general(a, b, (((0,), (0,)), ((), ())), preferred_element_type=F32)


def normalized(values):
    average = jnp.mean(values, axis=-1, keepdims=True)
    centred = values - average
    variance = jnp.mean(centred * centred, axis=-1, keepdims=True)
    scale = lax.rsqrt(variance + EPSILON)
    return centred * scale, scale


def normalize_back(grad, unit, scale, gain):
    gs = grad * gain
    mean_gs = jnp.mean(gs, axis=-1, keepdims=True)
    mean_gn = jnp.mean(gs * unit, axis=-1, keepdims=True)
    return (gs - mean_gs - unit * mean_gn) * scale


def head_lanes(head):
    lane = lax.broadcasted_iota(jnp.int32, (1, WIDE), 1)
    return lane // HEAD_DIM == head


def row_sum(values):
    return jnp.sum(values, axis=0, keepdims=True)


def attend_kernel(
    length, x, wq, wk, wv, wo, bq, bv, bo, q_out, k_out, v_out, log_out, context_out,
    unit_out, scale_out, total,
):
    step = pl.program_id(0)
    slots = x.shape[0]
    rows = x[...]
    q = (mm(rows, wq[...]) + bq[...]).astype(BF)
    k = mm(rows, wk[...]).astype(BF)
    v = (mm(rows, wv[...]) + bv[...]).astype(BF)
    q_out[...] = q
    k_out[...] = k
    v_out[...] = v
    live = lax.broadcasted_iota(jnp.int32, (1, slots), 1) < length[0]
    scaled = (q.astype(F32) * 0.125).astype(BF)
    zero = jnp.zeros_like(scaled)
    context = jnp.zeros((slots, WIDE), F32)
    logs = jnp.zeros((slots, 128), F32)
    column = lax.broadcasted_iota(jnp.int32, (1, 128), 1)
    for head in range(WIDE // HEAD_DIM):
        lanes = head_lanes(head)
        scores = mm_right(jnp.where(lanes, scaled, zero), k)
        scores = jnp.where(live, scores, MASKED)
        highest = jnp.max(scores, axis=-1, keepdims=True)
        exponent = jnp.exp(scores - highest)
        totals = jnp.sum(exponent, axis=-1, keepdims=True)
        probs = (exponent * (1.0 / totals)).astype(BF)
        context = jnp.where(lanes, mm(probs, v), context)
        logs = jnp.where(column == head, highest + jnp.log(totals), logs)
    log_out[...] = jnp.transpose(logs)[:8]
    low = context.astype(BF)
    context_out[...] = low

    @pl.when(step == 0)
    def _():
        total[...] = rows.astype(F32) + bo[...]

    total[...] += mm(low, wo[...])

    @pl.when(step == pl.num_programs(0) - 1)
    def _():
        unit, scale = normalized(total[...])
        unit_out[...] = unit
        scale_out[...] = jnp.broadcast_to(scale, scale_out.shape)


def feed_kernel(
    length, unit1, g1, b1, w1, bi, w2, b2, g2, bb2, act_out, slope_out, unit_out, scale_out,
    result_out, low, total,
):
    step = pl.program_id(0)

    @pl.when(step == 0)
    def _():
        middle = unit1[...] * g1[...] + b1[...]
        low[...] = middle.astype(BF)
        total[...] = middle + b2[...]

    inner = mm(low[...], w1[...]) + bi[...]
    cdf = 0.5 * (1.0 + lax.erf(inner * 0.7071067811865476))
    act = (inner * cdf).astype(BF)
    act_out[...] = act
    slope_out[...] = (cdf + inner * (jnp.exp(-0.5 * inner * inner) * 0.3989422804014327)).astype(BF)
    total[...] += mm(act, w2[...])

    @pl.when(step == pl.num_programs(0) - 1)
    def _():
        unit, scale = normalized(total[...])
        unit_out[...] = unit
        scale_out[...] = jnp.broadcast_to(scale, scale_out.shape)
        live = lax.broadcasted_iota(jnp.int32, (unit.shape[0], 1), 0) < length[0]
        result_out[...] = jnp.where(live, unit * g2[...] + bb2[...], 0.0).astype(BF)


def feed_back_kernel(
    length, grad, unit2, scale2, g2, unit1, scale1, g1, b1, act, slope, w1, w2, *refs
):
    (d1_out, d2_out, first_out, vectors_out, inner_sum_out, second, outer, low, total) = refs[-9:]
    step = pl.program_id(0)

    @pl.when(step == 0)
    def _():
        live = lax.broadcasted_iota(jnp.int32, (grad.shape[0], 1), 0) < length[0]
        g = jnp.where(live, grad[...].astype(F32), 0.0)
        unit = unit2[...]
        d_second = normalize_back(g, unit, scale2[:, :1], g2[...])
        second[...] = d_second
        d_outer = d_second.astype(BF)
        outer[...] = d_outer
        vectors_out[0:1] = row_sum(d_outer.astype(F32))
        vectors_out[1:2] = row_sum(g * unit)
        vectors_out[2:3] = row_sum(g)
        low[...] = (unit1[...] * g1[...] + b1[...]).astype(BF)
        total[...] = jnp.zeros_like(total)

    d_outer = outer[...]
    d_inner = (mm_right(d_outer, w2[...]) * slope[...].astype(F32)).astype(BF)
    inner_sum_out[...] = row_sum(d_inner.astype(F32))
    total[...] += mm_right(d_inner, w1[...])
    d2_out[...] = mm_left(act[...], d_outer).astype(BF).reshape(d2_out.shape)
    d1 = mm_left(low[...], d_inner).astype(BF)
    half = d1.shape[0] // 2
    d1_out[0, 0, 0] = d1[:half]
    d1_out[0, 1, 0] = d1[half:]

    @pl.when(step == pl.num_programs(0) - 1)
    def _():
        d_middle = second[...] + total[...]
        unit = unit1[...]
        d_first = normalize_back(d_middle, unit, scale1[:, :1], g1[...])
        first_out[...] = d_first
        vectors_out[3:4] = row_sum(d_middle * unit)
        vectors_out[4:5] = row_sum(d_middle)
        vectors_out[5:6] = row_sum(d_first.astype(BF).astype(F32))


def attend_back_kernel(
    length, first, x, q, k, v, log, context, wq, wk, wv, wo, *refs
):
    (dqkv_out, do_out, x_out, sums_out, attended, total) = refs[-6:]
    step = pl.program_id(0)
    slots = x.shape[0]

    @pl.when(step == 0)
    def _():
        attended[...] = first[...].astype(BF)
        total[...] = first[...]

    d_att = attended[...]
    d_context = mm_right(d_att, wo[...]).astype(BF)
    queries = q[...]
    keys = k[...]
    values = v[...]
    scaled = (queries.astype(F32) * 0.125).astype(BF)
    zero = jnp.zeros_like(scaled)
    live = lax.broadcasted_iota(jnp.int32, (slots, 1), 0) < length[0]
    d_q = jnp.zeros((slots, WIDE), F32)
    d_k = jnp.zeros((slots, WIDE), F32)
    d_v = jnp.zeros((slots, WIDE), F32)
    for head in range(WIDE // HEAD_DIM):
        lanes = head_lanes(head)
        scores = mm_right(keys, jnp.where(lanes, scaled, zero))
        scores = jnp.where(live, scores, MASKED)
        probs = jnp.exp(scores - log[head : head + 1])
        d_v = jnp.where(lanes, mm(probs.astype(BF), d_context), d_v)
        d_probs = mm_right(values, jnp.where(lanes, d_context, zero))
        dots = row_sum(probs * d_probs)
        d_scores = (probs * (d_probs - dots)).astype(BF)
        d_k = jnp.where(lanes, mm(d_scores, queries), d_k)
        d_q = jnp.where(lanes, mm_left(d_scores, keys), d_q)
    d_q = (d_q * 0.125).astype(BF)
    d_k = (d_k * 0.125).astype(BF)
    d_v = d_v.astype(BF)
    sums_out[0:1] = row_sum(d_q.astype(F32))
    sums_out[1:2] = row_sum(d_v.astype(F32))
    total[...] += mm_right(d_q, wq[...]) + mm_right(d_k, wk[...]) + mm_right(d_v, wv[...])
    rows = x[...]
    for at, value in enumerate((d_q, d_k, d_v)):
        weight = mm_left(rows, value).astype(BF)
        half = weight.shape[0] // 2
        dqkv_out[0, 0, at] = weight[:half]
        dqkv_out[0, 1, at] = weight[half:]
    do_out[...] = mm_left(context[...], d_att).astype(BF).reshape(do_out.shape)

    @pl.when(step == pl.num_programs(0) - 1)
    def _():
        x_out[...] = total[...].astype(BF)


def whole(shape):
    return pl.BlockSpec(shape, lambda j, *_: (0,) * len(shape))


def struct(shape, dtype):
    return jax.ShapeDtypeStruct(shape, dtype)


def grid_call(kernel, steps, in_specs, out_specs, out_shape, scratch, name, flops, aliases=None):
    return pl.pallas_call(
        kernel,
        grid_spec=pltpu.PrefetchScalarGridSpec(
            num_scalar_prefetch=1,
            grid=(steps,),
            in_specs=in_specs,
            out_specs=out_specs,
            scratch_shapes=scratch,
        ),
        out_shape=out_shape,
        input_output_aliases=aliases or {},
        compiler_params=pltpu.CompilerParams(
            dimension_semantics=("arbitrary",), vmem_limit_bytes=VMEM_LIMIT
        ),
        cost_estimate=pl.CostEstimate(
            flops=flops, bytes_accessed=30000000, transcendentals=4000000
        ),
        name=name,
    )


def rank_two(vector):
    return vector.reshape(1, -1)


def layer_of(shape, layer):
    return pl.BlockSpec((None,) + shape, None)


def attend(length, x, layer, weights, vectors):
    wq, wk, wv, wo = weights
    slots, width = x.shape
    steps = width // WIDE
    columns = pl.BlockSpec((None, width, WIDE), lambda j, *_: (layer, 0, j))
    band = pl.BlockSpec((slots, WIDE), lambda j, *_: (0, j))
    line = pl.BlockSpec((1, WIDE), lambda j, *_: (0, j))
    return grid_call(
        attend_kernel,
        steps,
        [
            whole((slots, width)), columns, columns, columns,
            pl.BlockSpec((None, WIDE, width), lambda j, *_: (layer, j, 0)),
            line, line, whole((1, width)),
        ],
        [
            band, band, band,
            pl.BlockSpec((None, 8, slots), lambda j, *_: (j, 0, 0)),
            band, whole((slots, width)), whole((slots, 128)),
        ],
        [
            struct((slots, width), BF), struct((slots, width), BF), struct((slots, width), BF),
            struct((steps, 8, slots), F32), struct((slots, width), BF),
            struct((slots, width), F32), struct((slots, 128), F32),
        ],
        [pltpu.VMEM((slots, width), F32)],
        "attend",
        9000000000,
    )(length, x, wq, wk, wv, wo, *(rank_two(v) for v in vectors))


def feed(length, unit1, layer, w1, w2, vectors):
    slots, width = unit1.shape
    hidden = w1.shape[-1]
    steps = hidden // HIDDEN_BLOCK
    g1, b1, bi, b2, g2, bb2 = (rank_two(v) for v in vectors)
    line = whole((1, width))
    band = pl.BlockSpec((slots, HIDDEN_BLOCK), lambda j, *_: (0, j))
    return grid_call(
        feed_kernel,
        steps,
        [
            whole((slots, width)), line, line,
            pl.BlockSpec((None, width, HIDDEN_BLOCK), lambda j, *_: (layer, 0, j)),
            pl.BlockSpec((1, HIDDEN_BLOCK), lambda j, *_: (0, j)),
            pl.BlockSpec((None, HIDDEN_BLOCK, width), lambda j, *_: (layer, j, 0)),
            line, line, line,
        ],
        [band, band, whole((slots, width)), whole((slots, 128)), whole((slots, width))],
        [
            struct((slots, hidden), BF), struct((slots, hidden), BF), struct((slots, width), F32),
            struct((slots, 128), F32), struct((slots, width), BF),
        ],
        [pltpu.VMEM((slots, width), BF), pltpu.VMEM((slots, width), F32)],
        "feed",
        9000000000,
    )(length, unit1, g1, b1, w1, bi, w2, b2, g2, bb2)


def feed_back(length, grad, unit2, scale2, unit1, scale1, act, slope, layer, w1, w2, vectors, held):
    slots, width = unit1.shape
    hidden = w1.shape[-1]
    steps = hidden // HIDDEN_BLOCK
    per = 1024 // HIDDEN_BLOCK
    g1, b1, g2 = (rank_two(v) for v in vectors)
    line = whole((1, width))
    row = whole((slots, width))
    thin = whole((slots, 128))
    band = pl.BlockSpec((slots, HIDDEN_BLOCK), lambda j, *_: (0, j))
    d1_block = pl.BlockSpec(
        (1, 2, 1, 512, HIDDEN_BLOCK), lambda j, *_: (layer, 0, j // per, 0, j % per)
    )
    pairs = HIDDEN_BLOCK // 512
    d2_block = pl.BlockSpec(
        (1, 1, pairs, 512, width),
        lambda j, *_: (layer, j // (steps // 2), j % (steps // 2), 0, 0),
    )
    extra = () if held is None else tuple(held)
    return grid_call(
        feed_back_kernel,
        steps,
        [
            row, row, thin, line, row, thin, line, line, band, band,
            pl.BlockSpec((None, width, HIDDEN_BLOCK), lambda j, *_: (layer, 0, j)),
            pl.BlockSpec((None, HIDDEN_BLOCK, width), lambda j, *_: (layer, j, 0)),
        ]
        + [pl.BlockSpec(memory_space=pl.ANY)] * len(extra),
        [
            d1_block, d2_block, row, whole((6, width)),
            pl.BlockSpec((1, HIDDEN_BLOCK), lambda j, *_: (0, j)),
        ],
        [
            struct((2, 2, 4, 512, 1024), BF), struct((2, 2, 4, 512, 1024), BF),
            struct((slots, width), F32), struct((6, width), F32), struct((1, hidden), F32),
        ],
        [
            pltpu.VMEM((slots, width), F32), pltpu.VMEM((slots, width), BF),
            pltpu.VMEM((slots, width), BF), pltpu.VMEM((slots, width), F32),
        ],
        "feed_back",
        18000000000,
        {13 + i: i for i in range(len(extra))},
    )(length, grad, unit2, scale2, g2, unit1, scale1, g1, b1, act, slope, w1, w2, *extra)


def attend_back(length, first, x, q, k, v, log, context, layer, weights, held):
    wq, wk, wv, wo = weights
    slots, width = x.shape
    steps = width // WIDE
    columns = pl.BlockSpec((None, width, WIDE), lambda j, *_: (layer, 0, j))
    band = pl.BlockSpec((slots, WIDE), lambda j, *_: (0, j))
    row = whole((slots, width))
    per = 512 // WIDE
    extra = () if held is None else tuple(held)
    return grid_call(
        attend_back_kernel,
        steps,
        [
            row, row, band, band, band,
            pl.BlockSpec((None, 8, slots), lambda j, *_: (j, 0, 0)),
            band, columns, columns, columns,
            pl.BlockSpec((None, WIDE, width), lambda j, *_: (layer, j, 0)),
        ]
        + [pl.BlockSpec(memory_space=pl.ANY)] * len(extra),
        [
            pl.BlockSpec((1, 2, 3, 512, WIDE), lambda j, *_: (layer, 0, 0, 0, j)),
            pl.BlockSpec((1, 1, 1, WIDE, width), lambda j, *_: (layer, j // per, 0, j % per, 0)),
            row,
            pl.BlockSpec((2, WIDE), lambda j, *_: (0, j)),
        ],
        [
            struct((2, 2, 3, 512, 1024), BF), struct((2, 2, 1, 512, 1024), BF),
            struct((slots, width), BF), struct((2, width), F32),
        ],
        [pltpu.VMEM((slots, width), BF), pltpu.VMEM((slots, width), F32)],
        "attend_back",
        20000000000,
        {12 + i: i for i in range(len(extra))},
    )(length, first, x, q, k, v, log, context, wq, wk, wv, wo, *extra)


from jax.sharding import PartitionSpec as P

VECTORS = (1, 1, 1, 1, 1, 4, 1, 1, 1)


def unpack_kernel(narrow, first, second, *outs):
    for at in range(4):
        outs[at][0] = narrow[at].astype(F32)
    for at in range(4):
        outs[4][0, :, pl.ds(1024 * at, 1024)] = first[at].astype(F32)
    outs[5][0] = second[0].astype(F32)


def unpack(total):
    square = pl.BlockSpec((1, 128, 1024), lambda j: (0, j, 0))
    return pl.pallas_call(
        unpack_kernel,
        grid=(4,),
        in_specs=[
            pl.BlockSpec((4, 128, 1024), lambda j: (0, j, 0)),
            pl.BlockSpec((4, 128, 1024), lambda j: (1, j, 0)),
            pl.BlockSpec((1, 512, 1024), lambda j: (8 + j, 0, 0)),
        ],
        out_specs=[square] * 4
        + [
            pl.BlockSpec((1, 128, 4096), lambda j: (0, j, 0)),
            pl.BlockSpec((1, 512, 1024), lambda j: (0, j, 0)),
        ],
        out_shape=[struct((1, 512, 1024), F32)] * 4
        + [struct((1, 512, 4096), F32), struct((1, 2048, 1024), F32)],
        compiler_params=pltpu.CompilerParams(vmem_limit_bytes=VMEM_LIMIT),
        name="unpack",
    )(total, total, total)


def split_vectors(packed):
    halves = packed.reshape(2, -1)
    out, at = [], 0
    for width in VECTORS:
        out.append(halves[:, at : at + 512 * width].reshape(-1).astype(jnp.float32))
        at += 512 * width
    return tuple(out)


def device_of(number, groups):
    return lax.rem(number, 2) * groups + number // 2


def own_cotangent(cotangent, permutation, groups):
    core = lax.axis_index("section")
    total = permutation.shape[0]
    mine = lax.dynamic_index_in_dim(cotangent, core, 0, keepdims=False)
    shape = mine.shape
    chunks = mine.reshape(2 * groups, shape[0] // (2 * groups), shape[1])
    spread = lax.all_to_all(chunks, ALL, 0, 0, tiled=True)
    device = jnp.arange(total, dtype=jnp.int32)
    number = 2 * lax.rem(device, groups) + device // groups
    slot = jnp.sum(
        jnp.where(permutation[None, :] == number[:, None], device[None, :], 0), axis=1
    )
    ordered = jnp.take(spread, device_of(slot, groups), axis=0)
    return lax.all_to_all(ordered, ALL, 0, 0, tiled=True).reshape(shape)


def dealt_grads(both, permutation, groups):
    slots, width = both.shape[1:]
    rows = slots // groups
    spread = lax.all_to_all(both.reshape(2 * groups, rows, width), ALL, 0, 0, tiled=True)
    ordered = jnp.take(spread, device_of(permutation, groups), axis=0)
    ordered = ordered.reshape(groups, 2, rows, width)
    home = lax.all_to_all(ordered, GROUP, 0, 0, tiled=True)
    return home.transpose(1, 0, 2, 3).reshape(2, slots, width)


def layer_forward(length, x, layer, weights, vectors):
    bq, bv, bo, g1, b1, bi, b2, g2, bb2 = vectors
    q, k, v, log, context, unit1, scale1 = attend(length, x, layer, weights[:4], (bq, bv, bo))
    act, slope, unit2, scale2, result = feed(
        length, unit1, layer, weights[4], weights[5], (g1, b1, bi, b2, g2, bb2)
    )
    return result, (q, k, v, log, context, unit1, scale1, act, slope, unit2, scale2)


def layer_backward(length, grad, x, layer, weights, vectors, stored, held):
    q, k, v, log, context, unit1, scale1, act, slope, unit2, scale2 = stored
    g1, b1, g2 = vectors[3], vectors[4], vectors[7]
    d1, d2, first, rows, inner = feed_back(
        length, grad, unit2, scale2, unit1, scale1, act, slope, layer, weights[4], weights[5],
        (g1, b1, g2), None if held is None else held[2:],
    )
    d_qkv, d_o, d_x, sums = attend_back(
        length, first, x, q, k, v, log, context, layer, weights[:4],
        None if held is None else held[:2],
    )
    vectors = (sums[0], sums[1], rows[5], rows[3], rows[4], inner[0], rows[0], rows[1], rows[2])
    small = jnp.concatenate([v.reshape(2, -1) for v in vectors], axis=1).reshape(96, 128)
    return d_x, small, (d_qkv, d_o, d1, d2)


def on_device(
    inputs, cotangent, lengths, permutation, query_weight, query_bias, key_weight, value_weight,
    value_bias, output_weight, output_bias, first_gain, first_bias, inner_weight, inner_bias,
    outer_weight, outer_bias, second_gain, second_bias,
):
    core = lax.axis_index("section")
    group = lax.axis_index(GROUP)
    groups = lax.axis_size(GROUP)
    count = lax.axis_size("replica").bit_length() - 1
    shards = [
        w[0] for w in (query_weight, key_weight, value_weight, output_weight, inner_weight, outer_weight)
    ]
    vectors = [
        v[0] for v in (query_bias, value_bias, output_bias, first_gain, first_bias, inner_bias,
                       outer_bias, second_gain, second_bias)
    ]
    full = gather_weights(shards, jnp.concatenate(vectors).reshape(48, 128), count)
    weights, shared = full[:6], [split_vectors(full[6][s]) for s in range(2)]
    length = lax.dynamic_slice_in_dim(lengths, 2 * group + core, 1)
    x = lax.dynamic_index_in_dim(inputs, core, 0, keepdims=False)
    grad = own_cotangent(cotangent, permutation, groups)
    lower, lower_stored = layer_forward(length, x, 0, weights, shared[0])
    upper, upper_stored = layer_forward(length, lower, 1, weights, shared[1])
    upper_grad, upper_small, parts = layer_backward(
        length, grad, lower, 1, weights, shared[1], upper_stored, None
    )
    lower_grad, lower_small, parts = layer_backward(
        length, upper_grad, x, 0, weights, shared[0], lower_stored, parts
    )
    total, small = reduce_grads(parts, jnp.stack([lower_small, upper_small]), count)
    sent = jnp.where(core == 0, upper, lower)
    kept = jnp.where(core == 0, lower, upper)
    came = lax.ppermute(sent, "section", [(0, 1), (1, 0)])
    activations = jnp.where(core == 0, jnp.stack([kept, came]), jnp.stack([came, kept]))[None]
    input_grads = dealt_grads(jnp.stack([lower_grad, upper_grad]), permutation, groups)[None]
    side = lax.axis_index("shard")
    own = lax.dynamic_index_in_dim(small.reshape(2, -1), side, 0, keepdims=False)
    pieces, at = [], 0
    for width in VECTORS:
        pieces.append(own[None, at : at + 512 * width])
        at += 512 * width
    dq, dk, dv, do, d1, d2 = unpack(total)
    return (
        activations, input_grads, dq, pieces[0], dk, dv, pieces[1], do, pieces[2], pieces[3],
        pieces[4], d1, pieces[5], d2, pieces[6], pieces[7], pieces[8],
    )


def solution(mesh):
    matrix, vector = P("section", "shard", None), P("section", "shard")
    rows = P(("shard", "replica"), None, None)
    in_specs = (
        rows, rows, P(), P(), matrix, vector, matrix, matrix, vector, matrix, vector, vector,
        vector, matrix, vector, matrix, vector, vector, vector,
    )
    both = P("section", ("shard", "replica"), None, None)
    out_specs = (
        both, both, matrix, vector, matrix, matrix, vector, matrix, vector, vector, vector,
        matrix, vector, matrix, vector, vector, vector,
    )
    return jax.shard_map(
        on_device, mesh=mesh, in_specs=in_specs, out_specs=out_specs, check_vma=False
    )
```

```python
import jax
import jax.numpy as jnp
from jax import lax
from jax.experimental import pallas as pl
from jax.experimental.pallas import tpu as pltpu

ALL = ("section", "shard", "replica")
GROUP = ("shard", "replica")
UNITS = 12
DIRECT = (0, 1, 2)
DOUBLED = (3, 4, 5, 6, 7, 8, 9, 10, 11)
VMEM_LIMIT = 64000000


def my_bits(count):
    replica = lax.axis_index("replica")
    return tuple((lax.rem(replica // (1 << (count - 1 - p)), 2) for p in range(count)))


def across(p, count, bits):
    replica = lax.axis_index("replica")
    weight = 1 << (count - 1 - p)
    return {"replica": replica + weight * (1 - 2 * bits[p])}


def greet(partners):
    barrier = pltpu.get_barrier_semaphore()
    for partner in partners:
        pl.semaphore_signal(barrier, inc=1, device_id=partner, device_id_type=pl.DeviceIdType.MESH)
    pl.semaphore_wait(barrier, len(partners))


def remote(src, dst, send_sem, recv_sem, partner):
    return pltpu.make_async_remote_copy(
        src_ref=src,
        dst_ref=dst,
        send_sem=send_sem,
        recv_sem=recv_sem,
        device_id=partner,
        device_id_type=pl.DeviceIdType.MESH,
    )


def gather_kernel(
    count, wq, wk, wv, wo, w1, w2, small,
    oq, ok, ov, oo, o1, o2, osmall,
    stage, send_sem, recv_sem, load_sem, store_sem,
):
    core = lax.axis_index("section")
    side = lax.axis_index("shard")
    bits = my_bits(count)
    sibling = {"section": 1 - core}
    facing = {"shard": 1 - side}
    corner = {"section": 1 - core, "shard": 1 - side}
    everything = (slice(None),) * count

    def source(unit, index):
        if unit < 4:
            return (wq, wk, wv, wo)[unit].at[index]
        if unit < 8:
            return w1.at[index + (slice(None), pl.ds(1024 * (unit - 4), 1024))]
        return w2.at[(unit - 8,) + index]

    def target(unit, layer, half, index):
        if unit < 4:
            return (oq, ok, ov, oo)[unit].at[(layer, half) + index]
        if unit < 8:
            return o1.at[(layer, half) + index + (slice(None), pl.ds(1024 * (unit - 4), 1024))]
        return o2.at[(layer, half, unit - 8) + index]

    greet([sibling, facing, corner] + [across(p, count, bits) for p in range(count)])
    number = [0]
    sends = []

    def start(src, dst, partner):
        at = number[0]
        number[0] += 1
        copy = remote(src, dst, send_sem.at[at], recv_sem.at[at], partner)
        copy.start()
        sends.append(copy)
        return at

    def arrive(at, dst, partner):
        remote(dst, dst, send_sem.at[at], recv_sem.at[at], partner).wait_recv()

    first = {}
    for unit in DOUBLED:
        first[unit] = start(source(unit, bits), target(unit, core, side, bits), facing)
    small_at = [
        start(small, osmall.at[core, side], partner) for partner in (sibling, facing, corner)
    ]
    for unit in DIRECT:
        first[unit] = start(source(unit, everything), target(unit, core, side, everything), facing)
    loads = []
    for unit in range(UNITS):
        copy = pltpu.make_async_copy(source(unit, everything), stage.at[unit], load_sem.at[unit])
        copy.start()
        loads.append(copy)
    small_copy = pltpu.make_async_copy(small, osmall.at[core, side], store_sem.at[UNITS])
    small_copy.start()
    own = {}
    for unit in DOUBLED + DIRECT:
        own[unit] = start(source(unit, everything), target(unit, core, side, everything), sibling)
    stores = []
    for unit in range(UNITS):
        loads[unit].wait()
        copy = pltpu.make_async_copy(
            stage.at[unit], target(unit, core, side, everything), store_sem.at[unit]
        )
        copy.start()
        stores.append(copy)
    inflight = {unit: first[unit] for unit in range(UNITS)}
    passed = {}
    waiting = list(DIRECT)

    def finish_direct(unit):
        landed = target(unit, core, 1 - side, everything)
        arrive(inflight[unit], landed, facing)
        passed[unit] = start(landed, landed, sibling)

    for tick in range(len(DOUBLED) + count + 1):
        for step in reversed(range(count + 1)):
            j = tick - step
            if not 0 <= j < len(DOUBLED):
                continue
            unit = DOUBLED[j]
            if step == 0:
                arrive(inflight[unit], target(unit, core, 1 - side, bits), facing)
            else:
                p = step - 1
                landed = everything[:p] + (1 - bits[p],) + bits[p + 1 :]
                arrive(
                    inflight[unit], target(unit, core, 1 - side, landed), across(p, count, bits)
                )
            if step < count:
                held = target(unit, core, 1 - side, everything[:step] + bits[step:])
                inflight[unit] = start(held, held, across(step, count, bits))
            else:
                held = target(unit, core, 1 - side, everything)
                passed[unit] = start(held, held, sibling)
        if tick >= count + 2 and tick % 2 == 1 and waiting:
            finish_direct(waiting.pop(0))
    for unit in waiting:
        finish_direct(unit)
    for unit in range(UNITS):
        arrive(own[unit], target(unit, 1 - core, side, everything), sibling)
        arrive(passed[unit], target(unit, 1 - core, 1 - side, everything), sibling)
        stores[unit].wait()
    small_copy.wait()
    arrive(small_at[0], osmall.at[1 - core, side], sibling)
    arrive(small_at[1], osmall.at[core, 1 - side], facing)
    arrive(small_at[2], osmall.at[1 - core, 1 - side], corner)
    for copy in sends:
        copy.wait_send()


def gather_weights(shards, small, count):
    cut = (2,) * count
    rows = 512 // (1 << count)
    wq, wk, wv, wo, w1, w2 = shards
    narrow = cut + (rows, 1024)
    args = (
        [w.reshape(narrow) for w in (wq, wk, wv, wo)]
        + [w1.reshape(cut + (rows, 4096)), w2.reshape((4,) + narrow), small]
    )
    outs = (
        [jax.ShapeDtypeStruct((2, 2) + narrow, jnp.bfloat16)] * 4
        + [
            jax.ShapeDtypeStruct((2, 2) + cut + (rows, 4096), jnp.bfloat16),
            jax.ShapeDtypeStruct((2, 2, 4) + narrow, jnp.bfloat16),
            jax.ShapeDtypeStruct((2, 2) + small.shape, small.dtype),
        ]
    )
    copies = len(DOUBLED) * (count + 3) + len(DIRECT) * 3 + 3

    def kernel(*refs):
        args, outs, scratch = refs[:7], refs[7:14], refs[14:]
        flat = (scratch[0],) + scratch[1:]
        gather_kernel(count, *args, *outs, *flat)

    result = pl.pallas_call(
        kernel,
        out_shape=outs,
        in_specs=[pl.BlockSpec(memory_space=pl.ANY)] * 7,
        out_specs=[pl.BlockSpec(memory_space=pl.ANY)] * 7,
        scratch_shapes=[
            pltpu.VMEM((UNITS,) + narrow, jnp.bfloat16),
            pltpu.SemaphoreType.DMA((copies,)),
            pltpu.SemaphoreType.DMA((copies,)),
            pltpu.SemaphoreType.DMA((UNITS,)),
            pltpu.SemaphoreType.DMA((UNITS + 1,)),
        ],
        compiler_params=pltpu.CompilerParams(
            collective_id=0, has_side_effects=True, vmem_limit_bytes=VMEM_LIMIT
        ),
        name="gather_weights",
    )(*args)
    full = [w.reshape(2, 1024, 1024) for w in result[:4]]
    full += [result[4].reshape(2, 1024, 4096), result[5].reshape(2, 4096, 1024), result[6]]
    return full


SENT_RING = 4
LAND_RING = 5


def device_of(number, groups):
    return lax.rem(number, 2) * groups + number // 2


def reduce_kernel(count, layers, small, grads, results, permutation, outs, scratch):
    total, small_total, landing, dealt, acts = outs
    (own, came, across_half, kept, from_x), rest = scratch[:5], scratch[5:]
    halves, rest = rest[:count], rest[count:]
    (spread, ordered, small_own, small_recv, send0, recv0, send_x, recv_x, send_rs, recv_rs,
     send_ag, recv_ag, load_sem, came_sem, piece_sem, small_send, small_arrive, deal_send,
     deal_recv, home_send, home_recv, act_sem, total_sem) = rest
    core = lax.axis_index("section")
    side = lax.axis_index("shard")
    replica = lax.axis_index("replica")
    bits = my_bits(count)
    sibling = {"section": 1 - core}
    facing = {"shard": 1 - side}
    everything = (slice(None),) * count
    rows = kept.shape[-2]
    keep_ring = kept.shape[0]
    replicas = 1 << count
    groups = 2 * replicas
    group = side * replicas + replica
    me = core * groups + group
    chunk = spread.shape[1]

    barrier = pltpu.get_barrier_semaphore()

    def place(device):
        return {
            "section": device // groups,
            "shard": lax.rem(device, groups) // replicas,
            "replica": lax.rem(device, replicas),
        }

    def hello(step, carry):
        pl.semaphore_signal(
            barrier, inc=1, device_id=place(lax.rem(me + step, 2 * groups)),
            device_id_type=pl.DeviceIdType.MESH,
        )
        return carry

    lax.fori_loop(1, 2 * groups, hello, 0)
    pl.semaphore_wait(barrier, 2 * groups - 1)

    ranges, at = [], 0
    for index in range(len(layers[0])):
        ranges.append((index, at, at + layers[0][index].shape[1]))
        at += layers[0][index].shape[1]

    def core_copy(unit, source=None):
        source = landing.at[unit] if source is None else source
        return remote(source, landing.at[unit], send0.at[unit], recv0.at[unit], sibling)

    def send_core(owner):
        for index, low, high in ranges:
            for unit in range(low, high):
                core_copy(unit, layers[owner][index].at[:, unit - low]).start()

    def own_load(source, slot):
        return pltpu.make_async_copy(source, own.at[slot], load_sem.at[slot])

    def start_load(unit):
        for owner in range(2):
            for index, low, high in ranges:
                @pl.when(jnp.logical_and(core == owner, jnp.logical_and(unit >= low, unit < high)))
                def _():
                    own_load(layers[owner][index].at[:, unit - low], lax.rem(unit, 2)).start()

    def x_copy(unit):
        return remote(
            across_half.at[lax.rem(unit, SENT_RING)], from_x.at[lax.rem(unit, LAND_RING)],
            send_x.at[unit], recv_x.at[unit], facing,
        )

    def rs_copy(unit, p):
        slot = lax.rem(unit, keep_ring)
        return remote(
            kept.at[(slot,) + everything[:p] + (1 - bits[p],) + bits[p + 1 :]],
            halves[p].at[lax.rem(unit, LAND_RING)],
            send_rs.at[p, unit],
            recv_rs.at[p, unit],
            across(p, count, bits),
        )

    def ag_copy(unit, p):
        where = (unit,) + everything[:p] + bits[p:]
        source = kept.at[(lax.rem(unit, keep_ring),) + bits] if p == 0 else total.at[where]
        return remote(
            source, total.at[where], send_ag.at[p, unit], recv_ag.at[p, unit],
            across(p, count, bits),
        )

    def ag_arrive(unit, p):
        where = total.at[(unit,) + everything[:p] + (1 - bits[p],) + bits[p + 1 :]]
        remote(
            where, where, send_ag.at[p, unit], recv_ag.at[p, unit], across(p, count, bits)
        ).wait_recv()

    def piece_copy(unit):
        return pltpu.make_async_copy(
            kept.at[(lax.rem(unit, keep_ring),) + bits], total.at[(unit,) + bits],
            piece_sem.at[unit],
        )

    def small_copy(step):
        partner = [sibling, facing] + [across(p, count, bits) for p in range(count)]
        source = small.at[1 - core] if step == 0 else small_own.at[step - 1]
        return remote(
            source, small_recv.at[step], small_send.at[step], small_arrive.at[step], partner[step]
        )

    def spread_copy(target):
        layer_rows = pl.ds(pl.multiple_of(lax.rem(target, groups) * chunk, chunk), chunk)
        return [
            remote(
                grads[layer].at[layer_rows], spread.at[me], deal_send.at[target],
                deal_recv.at[me], place(target),
            )
            for layer in range(2)
        ]

    def spread_own():
        layer_rows = pl.ds(pl.multiple_of(group * chunk, chunk), chunk)
        return [
            pltpu.make_async_copy(grads[layer].at[layer_rows], spread.at[me], deal_recv.at[me])
            for layer in range(2)
        ]

    def spread_start(step, carry):
        target = lax.rem(me + step, 2 * groups)
        for layer in range(2):
            @pl.when(target // groups == layer)
            def _():
                spread_copy(target)[layer].start()
        return carry

    def spread_wait(step, carry):
        source = lax.rem(me + step, 2 * groups)
        remote(
            spread.at[source], spread.at[source], deal_send.at[source], deal_recv.at[source],
            place(source),
        ).wait_recv()
        return carry

    def home_copy(target):
        there = lax.rem(target, groups)
        return remote(
            ordered.at[pl.ds(2 * there, 2)], dealt.at[:, group], home_send.at[there],
            home_recv.at[group], {"shard": there // replicas, "replica": lax.rem(there, replicas)},
        )

    def home_own():
        return pltpu.make_async_copy(
            ordered.at[pl.ds(2 * group, 2)], dealt.at[:, group], home_recv.at[group]
        )

    def home_start(step, carry):
        home_copy(lax.rem(group + step, groups)).start()
        return carry

    def home_wait(step, carry):
        source = lax.rem(group + step, groups)
        remote(
            dealt.at[:, source], dealt.at[:, source], home_send.at[source], home_recv.at[source],
            {"shard": source // replicas, "replica": lax.rem(source, replicas)},
        ).wait_recv()
        return carry

    def act_copies(layer):
        sent = remote(
            results[1 - layer], acts.at[layer], act_sem.at[0], act_sem.at[1], sibling
        )
        held = pltpu.make_async_copy(results[layer], came.at[0], act_sem.at[2])
        return sent, held

    small_copy(0).start()
    for owner in range(2):
        @pl.when(core == 1 - owner)
        def _():
            send_core(owner)
    start_load(0)
    for layer in range(2):
        @pl.when(core == layer)
        def _():
            spread_own()[layer].start()
    lax.fori_loop(1, 2 * groups, spread_start, 0)
    for layer in range(2):
        @pl.when(core == layer)
        def _():
            sent, held = act_copies(layer)
            sent.start()
            held.start()
            held.wait()
    store = pltpu.make_async_copy(came.at[0], acts.at[core], act_sem.at[3])
    store.start()
    store.wait()
    small_steps = count + 2

    def places_of(index, dims):
        return tuple((lax.rem(index // (1 << (dims - 1 - q)), 2) for q in range(dims)))

    def tick(now, carry):
        for step in range(small_steps):
            @pl.when(now == step + 1)
            def _():
                small_copy(step).wait_recv()
                before = small[core] if step == 0 else small_own[step - 1]
                small_own[step] = before + small_recv[step]
                if step + 1 < small_steps:
                    small_copy(step + 1).start()

        @pl.when(now == DEAL_TICK)
        def _():
            spread_own()[0].wait()
            lax.fori_loop(1, 2 * groups, spread_wait, 0)

            def reorder(slot, c):
                ordered[slot] = spread[device_of(permutation[slot], groups)]
                return c

            lax.fori_loop(0, 2 * groups, reorder, 0)
            home_own().start()
            lax.fori_loop(1, groups, home_start, 0)

        @pl.when(jnp.logical_and(now >= SENT_RING, now < UNITS + SENT_RING))
        def _():
            x_copy(now - SENT_RING).wait_send()

        @pl.when(jnp.logical_and(now >= keep_ring, now < UNITS + keep_ring))
        def _():
            for p in range(count):
                rs_copy(now - keep_ring, p).wait_send()
            ag_copy(now - keep_ring, 0).wait_send()

        @pl.when(now < UNITS)
        def _():
            unit = now
            slot = lax.rem(unit, 2)

            @pl.when(unit + 1 < UNITS)
            def _():
                start_load(unit + 1)

            core_copy(unit).wait_recv()
            arrived = pltpu.make_async_copy(landing.at[unit], came, came_sem)
            arrived.start()
            own_load(landing.at[unit], slot).wait()
            arrived.wait()
            out_slot = lax.rem(unit, SENT_RING)
            kept_slot = lax.rem(unit, keep_ring)

            def add(block, c):
                where = pl.ds(pl.multiple_of(block * 32, 32), 32)
                across_half[out_slot, where] = own[slot, 1 - side, where] + came[1 - side, where]
                return c

            lax.fori_loop(0, 16, add, 0)
            x_copy(unit).start()

            def add_kept(index, c):
                where = pl.ds(pl.multiple_of(index * rows, rows), rows)
                mine = (kept_slot,) + places_of(index, count)
                kept[mine] = own[slot, side, where] + came[side, where]
                return c

            lax.fori_loop(0, 1 << count, add_kept, 0)

        @pl.when(jnp.logical_and(now >= 1, now < UNITS + 1))
        def _():
            unit = now - 1
            slot = lax.rem(unit, keep_ring)
            land = lax.rem(unit, LAND_RING)
            x_copy(unit).wait_recv()

            def add(index, c):
                where = pl.ds(pl.multiple_of(index * rows, rows), rows)
                mine = (slot,) + places_of(index, count)
                kept[mine] = kept[mine] + from_x[land, where]
                return c

            lax.fori_loop(0, 1 << count, add, 0)
            rs_copy(unit, count - 1).start()

        for step in range(count):
            p = count - 1 - step

            @pl.when(jnp.logical_and(now >= 2 + step, now < UNITS + 2 + step))
            def _():
                unit = now - (2 + step)
                slot = lax.rem(unit, keep_ring)
                land = lax.rem(unit, LAND_RING)
                rs_copy(unit, p).wait_recv()

                def add(index, c):
                    mine = (slot,) + places_of(index, p) + bits[p:]
                    kept[mine] = kept[mine] + halves[p][(land,) + places_of(index, p)]
                    return c

                if p == 0:
                    add(0, 0)
                    piece_copy(unit).start()
                    ag_copy(unit, 0).start()
                else:
                    lax.fori_loop(0, 1 << p, add, 0)
                    rs_copy(unit, p - 1).start()

        for p in range(count):
            lag = 2 + count + p

            @pl.when(jnp.logical_and(now >= lag, now < UNITS + lag))
            def _():
                unit = now - lag
                ag_arrive(unit, p)
                if p == 0:
                    piece_copy(unit).wait()
                if p + 1 < count:
                    ag_copy(unit, p + 1).start()

        return carry

    lax.fori_loop(0, UNITS + max(keep_ring, 2 + 2 * count), tick, 0)
    out = pltpu.make_async_copy(small_own.at[small_steps - 1], small_total, total_sem)
    out.start()

    def last(unit, carry):
        core_copy(unit).wait_send()
        for p in range(1, count):
            ag_copy(unit, p).wait_send()
        return carry

    lax.fori_loop(0, UNITS, last, 0)
    for step in range(small_steps):
        small_copy(step).wait_send()

    def spread_done(step, carry):
        spread_copy(lax.rem(me + step, 2 * groups))[0].wait_send()
        return carry

    def home_done(step, carry):
        home_copy(lax.rem(group + step, groups)).wait_send()
        return carry

    lax.fori_loop(1, 2 * groups, spread_done, 0)
    home_own().wait()
    lax.fori_loop(1, groups, home_wait, 0)
    lax.fori_loop(1, groups, home_done, 0)
    act = remote(results[0], acts.at[1 - core], act_sem.at[0], act_sem.at[1], sibling)
    act.wait_send()
    act.wait_recv()
    out.wait()


DEAL_TICK = 5


def reduce_grads(layers, small, grads, results, permutation, count):
    cut = (2,) * count
    rows = 512 // (1 << count)
    narrow = cut + (rows, 1024)
    dma = pltpu.SemaphoreType.DMA
    held = len(layers[0])
    groups = 2 << count
    slots, width = grads[0].shape
    chunk = slots // groups
    keep_ring = count + 5

    def kernel(*refs):
        lower, upper, refs = refs[:held], refs[held : 2 * held], refs[2 * held :]
        reduce_kernel(
            count, (lower, upper), refs[0], refs[1:3], refs[3:5], refs[5], refs[6:11], refs[11:]
        )

    vectors = small.shape[1:]
    anywhere = pl.BlockSpec(memory_space=pl.ANY)
    total, small_total, _, dealt, acts = pl.pallas_call(
        kernel,
        out_shape=[
            jax.ShapeDtypeStruct((UNITS,) + narrow, jnp.bfloat16),
            jax.ShapeDtypeStruct(vectors, jnp.float32),
            jax.ShapeDtypeStruct((UNITS, 2, 512, 1024), jnp.bfloat16),
            jax.ShapeDtypeStruct((2, groups, chunk, width), jnp.bfloat16),
            jax.ShapeDtypeStruct((2, slots, width), jnp.bfloat16),
        ],
        in_specs=[anywhere] * (2 * held)
        + [pl.BlockSpec(memory_space=pltpu.VMEM)]
        + [anywhere] * 4
        + [pl.BlockSpec(memory_space=pltpu.SMEM)],
        out_specs=[anywhere] * 5,
        scratch_shapes=[
            pltpu.VMEM((2, 2, 512, 1024), jnp.bfloat16),
            pltpu.VMEM((2, 512, 1024), jnp.bfloat16),
            pltpu.VMEM((SENT_RING, 512, 1024), jnp.bfloat16),
            pltpu.VMEM((keep_ring,) + narrow, jnp.bfloat16),
            pltpu.VMEM((LAND_RING, 512, 1024), jnp.bfloat16),
        ]
        + [pltpu.VMEM((LAND_RING,) + (2,) * p + (rows, 1024), jnp.bfloat16) for p in range(count)]
        + [
            pltpu.VMEM((2 * groups, chunk, width), jnp.bfloat16),
            pltpu.VMEM((2 * groups, chunk, width), jnp.bfloat16),
            pltpu.VMEM((count + 2,) + vectors, jnp.float32),
            pltpu.VMEM((count + 2,) + vectors, jnp.float32),
            dma((UNITS,)),
            dma((UNITS,)),
            dma((UNITS,)),
            dma((UNITS,)),
            dma((count, UNITS)),
            dma((count, UNITS)),
            dma((count, UNITS)),
            dma((count, UNITS)),
            dma((2,)),
            dma,
            dma((UNITS,)),
            dma((count + 2,)),
            dma((count + 2,)),
            dma((2 * groups,)),
            dma((2 * groups,)),
            dma((groups,)),
            dma((groups,)),
            dma((4,)),
            dma,
        ],
        compiler_params=pltpu.CompilerParams(
            collective_id=1, has_side_effects=True, vmem_limit_bytes=VMEM_LIMIT
        ),
        name="reduce_grads",
    )(*layers[0], *layers[1], small, *grads, *results, permutation)
    return (
        total.reshape(UNITS, 512, 1024), small_total, dealt.reshape(2, slots, width), acts
    )


HEAD_DIM = 64
EPSILON = 1e-12
MASKED = -1000000000.0
HIDDEN_BLOCK = 512
WIDE = 256
BF = jnp.bfloat16
F32 = jnp.float32


def mm(a, b):
    return lax.dot_general(a, b, (((1,), (0,)), ((), ())), preferred_element_type=F32)


def mm_right(a, b):
    return lax.dot_general(a, b, (((1,), (1,)), ((), ())), preferred_element_type=F32)


def mm_left(a, b):
    return lax.dot_general(a, b, (((0,), (0,)), ((), ())), preferred_element_type=F32)


def normalized(values):
    average = jnp.mean(values, axis=-1, keepdims=True)
    centred = values - average
    variance = jnp.mean(centred * centred, axis=-1, keepdims=True)
    scale = lax.rsqrt(variance + EPSILON)
    return centred * scale, scale


def normalize_back(grad, unit, scale, gain):
    gs = grad * gain
    mean_gs = jnp.mean(gs, axis=-1, keepdims=True)
    mean_gn = jnp.mean(gs * unit, axis=-1, keepdims=True)
    return (gs - mean_gs - unit * mean_gn) * scale


def head_lanes(head):
    lane = lax.broadcasted_iota(jnp.int32, (1, WIDE), 1)
    return lane // HEAD_DIM == head


def row_sum(values):
    return jnp.sum(values, axis=0, keepdims=True)


def attend_kernel(
    length, x, wq, wk, wv, wo, bq, bv, bo, q_out, k_out, v_out, log_out, context_out,
    unit_out, scale_out, total,
):
    step = pl.program_id(0)
    slots = x.shape[0]
    rows = x[...]
    q = (mm(rows, wq[...]) + bq[...]).astype(BF)
    k = mm(rows, wk[...]).astype(BF)
    v = (mm(rows, wv[...]) + bv[...]).astype(BF)
    q_out[...] = q
    k_out[...] = k
    v_out[...] = v
    live = lax.broadcasted_iota(jnp.int32, (1, slots), 1) < length[0]
    scaled = (q.astype(F32) * 0.125).astype(BF)
    zero = jnp.zeros_like(scaled)
    context = jnp.zeros((slots, WIDE), F32)
    logs = jnp.zeros((slots, 128), F32)
    column = lax.broadcasted_iota(jnp.int32, (1, 128), 1)
    for head in range(WIDE // HEAD_DIM):
        lanes = head_lanes(head)
        scores = mm_right(jnp.where(lanes, scaled, zero), k)
        scores = jnp.where(live, scores, MASKED)
        highest = jnp.max(scores, axis=-1, keepdims=True)
        exponent = jnp.exp(scores - highest)
        totals = jnp.sum(exponent, axis=-1, keepdims=True)
        probs = (exponent * (1.0 / totals)).astype(BF)
        context = jnp.where(lanes, mm(probs, v), context)
        logs = jnp.where(column == head, highest + jnp.log(totals), logs)
    log_out[...] = jnp.transpose(logs)[:8]
    low = context.astype(BF)
    context_out[...] = low

    @pl.when(step == 0)
    def _():
        total[...] = rows.astype(F32) + bo[...]

    total[...] += mm(low, wo[...])

    @pl.when(step == pl.num_programs(0) - 1)
    def _():
        unit, scale = normalized(total[...])
        unit_out[...] = unit
        scale_out[...] = jnp.broadcast_to(scale, scale_out.shape)


def feed_kernel(
    length, unit1, g1, b1, w1, bi, w2, b2, g2, bb2, act_out, slope_out, unit_out, scale_out,
    result_out, low, total,
):
    step = pl.program_id(0)

    @pl.when(step == 0)
    def _():
        middle = unit1[...] * g1[...] + b1[...]
        low[...] = middle.astype(BF)
        total[...] = middle + b2[...]

    inner = mm(low[...], w1[...]) + bi[...]
    cdf = 0.5 * (1.0 + lax.erf(inner * 0.7071067811865476))
    act = (inner * cdf).astype(BF)
    act_out[...] = act
    slope_out[...] = (cdf + inner * (jnp.exp(-0.5 * inner * inner) * 0.3989422804014327)).astype(BF)
    total[...] += mm(act, w2[...])

    @pl.when(step == pl.num_programs(0) - 1)
    def _():
        unit, scale = normalized(total[...])
        unit_out[...] = unit
        scale_out[...] = jnp.broadcast_to(scale, scale_out.shape)
        live = lax.broadcasted_iota(jnp.int32, (unit.shape[0], 1), 0) < length[0]
        result_out[...] = jnp.where(live, unit * g2[...] + bb2[...], 0.0).astype(BF)


def feed_back_kernel(
    length, grad, unit2, scale2, g2, unit1, scale1, g1, b1, act, slope, w1, w2, *refs
):
    (d1_out, d2_out, first_out, vectors_out, inner_sum_out, second, outer, low, total) = refs[-9:]
    step = pl.program_id(0)

    @pl.when(step == 0)
    def _():
        live = lax.broadcasted_iota(jnp.int32, (grad.shape[0], 1), 0) < length[0]
        g = jnp.where(live, grad[...].astype(F32), 0.0)
        unit = unit2[...]
        d_second = normalize_back(g, unit, scale2[:, :1], g2[...])
        second[...] = d_second
        d_outer = d_second.astype(BF)
        outer[...] = d_outer
        vectors_out[0:1] = row_sum(d_outer.astype(F32))
        vectors_out[1:2] = row_sum(g * unit)
        vectors_out[2:3] = row_sum(g)
        low[...] = (unit1[...] * g1[...] + b1[...]).astype(BF)
        total[...] = jnp.zeros_like(total)

    d_outer = outer[...]
    d_inner = (mm_right(d_outer, w2[...]) * slope[...].astype(F32)).astype(BF)
    inner_sum_out[...] = row_sum(d_inner.astype(F32))
    total[...] += mm_right(d_inner, w1[...])
    d2_out[...] = mm_left(act[...], d_outer).astype(BF).reshape(d2_out.shape)
    d1 = mm_left(low[...], d_inner).astype(BF)
    half = d1.shape[0] // 2
    d1_out[0, 0] = d1[:half]
    d1_out[1, 0] = d1[half:]

    @pl.when(step == pl.num_programs(0) - 1)
    def _():
        d_middle = second[...] + total[...]
        unit = unit1[...]
        d_first = normalize_back(d_middle, unit, scale1[:, :1], g1[...])
        first_out[...] = d_first
        vectors_out[3:4] = row_sum(d_middle * unit)
        vectors_out[4:5] = row_sum(d_middle)
        vectors_out[5:6] = row_sum(d_first.astype(BF).astype(F32))


def attend_back_kernel(
    length, first, x, q, k, v, log, context, wq, wk, wv, wo, *refs
):
    (dqkv_out, do_out, x_out, sums_out, attended, total) = refs[-6:]
    step = pl.program_id(0)
    slots = x.shape[0]

    @pl.when(step == 0)
    def _():
        attended[...] = first[...].astype(BF)
        total[...] = first[...]

    d_att = attended[...]
    d_context = mm_right(d_att, wo[...]).astype(BF)
    queries = q[...]
    keys = k[...]
    values = v[...]
    scaled = (queries.astype(F32) * 0.125).astype(BF)
    zero = jnp.zeros_like(scaled)
    live = lax.broadcasted_iota(jnp.int32, (slots, 1), 0) < length[0]
    d_q = jnp.zeros((slots, WIDE), F32)
    d_k = jnp.zeros((slots, WIDE), F32)
    d_v = jnp.zeros((slots, WIDE), F32)
    for head in range(WIDE // HEAD_DIM):
        lanes = head_lanes(head)
        scores = mm_right(keys, jnp.where(lanes, scaled, zero))
        scores = jnp.where(live, scores, MASKED)
        probs = jnp.exp(scores - log[head : head + 1])
        d_v = jnp.where(lanes, mm(probs.astype(BF), d_context), d_v)
        d_probs = mm_right(values, jnp.where(lanes, d_context, zero))
        dots = row_sum(probs * d_probs)
        d_scores = (probs * (d_probs - dots)).astype(BF)
        d_k = jnp.where(lanes, mm(d_scores, queries), d_k)
        d_q = jnp.where(lanes, mm_left(d_scores, keys), d_q)
    d_q = (d_q * 0.125).astype(BF)
    d_k = (d_k * 0.125).astype(BF)
    d_v = d_v.astype(BF)
    sums_out[0:1] = row_sum(d_q.astype(F32))
    sums_out[1:2] = row_sum(d_v.astype(F32))
    total[...] += mm_right(d_q, wq[...]) + mm_right(d_k, wk[...]) + mm_right(d_v, wv[...])
    rows = x[...]
    for at, value in enumerate((d_q, d_k, d_v)):
        weight = mm_left(rows, value).astype(BF)
        half = weight.shape[0] // 2
        dqkv_out[0, at] = weight[:half]
        dqkv_out[1, at] = weight[half:]
    do_out[...] = mm_left(context[...], d_att).astype(BF).reshape(do_out.shape)

    @pl.when(step == pl.num_programs(0) - 1)
    def _():
        x_out[...] = total[...].astype(BF)


def whole(shape):
    return pl.BlockSpec(shape, lambda j, *_: (0,) * len(shape))


def struct(shape, dtype):
    return jax.ShapeDtypeStruct(shape, dtype)


def grid_call(kernel, steps, in_specs, out_specs, out_shape, scratch, name, flops):
    return pl.pallas_call(
        kernel,
        grid_spec=pltpu.PrefetchScalarGridSpec(
            num_scalar_prefetch=1,
            grid=(steps,),
            in_specs=in_specs,
            out_specs=out_specs,
            scratch_shapes=scratch,
        ),
        out_shape=out_shape,
        compiler_params=pltpu.CompilerParams(
            dimension_semantics=("arbitrary",), vmem_limit_bytes=VMEM_LIMIT
        ),
        cost_estimate=pl.CostEstimate(
            flops=flops, bytes_accessed=30000000, transcendentals=4000000
        ),
        name=name,
    )


def rank_two(vector):
    return vector.reshape(1, -1)


def attend(length, x, layer, weights, vectors):
    wq, wk, wv, wo = weights
    slots, width = x.shape
    steps = width // WIDE
    columns = pl.BlockSpec((None, width, WIDE), lambda j, *_: (layer, 0, j))
    band = pl.BlockSpec((slots, WIDE), lambda j, *_: (0, j))
    line = pl.BlockSpec((1, WIDE), lambda j, *_: (0, j))
    return grid_call(
        attend_kernel,
        steps,
        [
            whole((slots, width)), columns, columns, columns,
            pl.BlockSpec((None, WIDE, width), lambda j, *_: (layer, j, 0)),
            line, line, whole((1, width)),
        ],
        [
            band, band, band,
            pl.BlockSpec((None, 8, slots), lambda j, *_: (j, 0, 0)),
            band, whole((slots, width)), whole((slots, 128)),
        ],
        [
            struct((slots, width), BF), struct((slots, width), BF), struct((slots, width), BF),
            struct((steps, 8, slots), F32), struct((slots, width), BF),
            struct((slots, width), F32), struct((slots, 128), F32),
        ],
        [pltpu.VMEM((slots, width), F32)],
        "attend",
        9000000000,
    )(length, x, wq, wk, wv, wo, *(rank_two(v) for v in vectors))


def feed(length, unit1, layer, w1, w2, vectors):
    slots, width = unit1.shape
    hidden = w1.shape[-1]
    steps = hidden // HIDDEN_BLOCK
    g1, b1, bi, b2, g2, bb2 = (rank_two(v) for v in vectors)
    line = whole((1, width))
    band = pl.BlockSpec((slots, HIDDEN_BLOCK), lambda j, *_: (0, j))
    return grid_call(
        feed_kernel,
        steps,
        [
            whole((slots, width)), line, line,
            pl.BlockSpec((None, width, HIDDEN_BLOCK), lambda j, *_: (layer, 0, j)),
            pl.BlockSpec((1, HIDDEN_BLOCK), lambda j, *_: (0, j)),
            pl.BlockSpec((None, HIDDEN_BLOCK, width), lambda j, *_: (layer, j, 0)),
            line, line, line,
        ],
        [band, band, whole((slots, width)), whole((slots, 128)), whole((slots, width))],
        [
            struct((slots, hidden), BF), struct((slots, hidden), BF), struct((slots, width), F32),
            struct((slots, 128), F32), struct((slots, width), BF),
        ],
        [pltpu.VMEM((slots, width), BF), pltpu.VMEM((slots, width), F32)],
        "feed",
        9000000000,
    )(length, unit1, g1, b1, w1, bi, w2, b2, g2, bb2)


def feed_back(length, grad, unit2, scale2, unit1, scale1, act, slope, layer, w1, w2, vectors):
    slots, width = unit1.shape
    hidden = w1.shape[-1]
    steps = hidden // HIDDEN_BLOCK
    per = 1024 // HIDDEN_BLOCK
    g1, b1, g2 = (rank_two(v) for v in vectors)
    line = whole((1, width))
    row = whole((slots, width))
    thin = whole((slots, 128))
    band = pl.BlockSpec((slots, HIDDEN_BLOCK), lambda j, *_: (0, j))
    d1_block = pl.BlockSpec(
        (2, 1, 512, HIDDEN_BLOCK), lambda j, *_: (0, j // per, 0, j % per)
    )
    pairs = HIDDEN_BLOCK // 512
    d2_block = pl.BlockSpec(
        (1, pairs, 512, width),
        lambda j, *_: (j // (steps // 2), j % (steps // 2), 0, 0),
    )
    return grid_call(
        feed_back_kernel,
        steps,
        [
            row, row, thin, line, row, thin, line, line, band, band,
            pl.BlockSpec((None, width, HIDDEN_BLOCK), lambda j, *_: (layer, 0, j)),
            pl.BlockSpec((None, HIDDEN_BLOCK, width), lambda j, *_: (layer, j, 0)),
        ],
        [
            d1_block, d2_block, row, whole((6, width)),
            pl.BlockSpec((1, HIDDEN_BLOCK), lambda j, *_: (0, j)),
        ],
        [
            struct((2, 4, 512, 1024), BF), struct((2, 4, 512, 1024), BF),
            struct((slots, width), F32), struct((6, width), F32), struct((1, hidden), F32),
        ],
        [
            pltpu.VMEM((slots, width), F32), pltpu.VMEM((slots, width), BF),
            pltpu.VMEM((slots, width), BF), pltpu.VMEM((slots, width), F32),
        ],
        "feed_back",
        18000000000,
    )(length, grad, unit2, scale2, g2, unit1, scale1, g1, b1, act, slope, w1, w2)


def attend_back(length, first, x, q, k, v, log, context, layer, weights):
    wq, wk, wv, wo = weights
    slots, width = x.shape
    steps = width // WIDE
    columns = pl.BlockSpec((None, width, WIDE), lambda j, *_: (layer, 0, j))
    band = pl.BlockSpec((slots, WIDE), lambda j, *_: (0, j))
    row = whole((slots, width))
    per = 512 // WIDE
    return grid_call(
        attend_back_kernel,
        steps,
        [
            row, row, band, band, band,
            pl.BlockSpec((None, 8, slots), lambda j, *_: (j, 0, 0)),
            band, columns, columns, columns,
            pl.BlockSpec((None, WIDE, width), lambda j, *_: (layer, j, 0)),
        ],
        [
            pl.BlockSpec((2, 3, 512, WIDE), lambda j, *_: (0, 0, 0, j)),
            pl.BlockSpec((1, 1, WIDE, width), lambda j, *_: (j // per, 0, j % per, 0)),
            row,
            pl.BlockSpec((2, WIDE), lambda j, *_: (0, j)),
        ],
        [
            struct((2, 3, 512, 1024), BF), struct((2, 1, 512, 1024), BF),
            struct((slots, width), BF), struct((2, width), F32),
        ],
        [pltpu.VMEM((slots, width), BF), pltpu.VMEM((slots, width), F32)],
        "attend_back",
        20000000000,
    )(length, first, x, q, k, v, log, context, wq, wk, wv, wo)


from jax.sharding import PartitionSpec as P

VECTORS = (1, 1, 1, 1, 1, 4, 1, 1, 1)


def unpack_kernel(narrow, first, second, *outs):
    for at in range(4):
        outs[at][0] = narrow[at].astype(F32)
    for at in range(4):
        outs[4][0, :, pl.ds(1024 * at, 1024)] = first[at].astype(F32)
    outs[5][0] = second[0].astype(F32)


def unpack(total):
    square = pl.BlockSpec((1, 128, 1024), lambda j: (0, j, 0))
    return pl.pallas_call(
        unpack_kernel,
        grid=(4,),
        in_specs=[
            pl.BlockSpec((4, 128, 1024), lambda j: (0, j, 0)),
            pl.BlockSpec((4, 128, 1024), lambda j: (1, j, 0)),
            pl.BlockSpec((1, 512, 1024), lambda j: (8 + j, 0, 0)),
        ],
        out_specs=[square] * 4
        + [
            pl.BlockSpec((1, 128, 4096), lambda j: (0, j, 0)),
            pl.BlockSpec((1, 512, 1024), lambda j: (0, j, 0)),
        ],
        out_shape=[struct((1, 512, 1024), F32)] * 4
        + [struct((1, 512, 4096), F32), struct((1, 2048, 1024), F32)],
        compiler_params=pltpu.CompilerParams(vmem_limit_bytes=VMEM_LIMIT),
        name="unpack",
    )(total, total, total)


def split_vectors(packed):
    halves = packed.reshape(2, -1)
    out, at = [], 0
    for width in VECTORS:
        out.append(halves[:, at : at + 512 * width].reshape(-1).astype(jnp.float32))
        at += 512 * width
    return tuple(out)


def own_cotangent(cotangent, permutation, groups):
    core = lax.axis_index("section")
    total = permutation.shape[0]
    mine = lax.dynamic_index_in_dim(cotangent, core, 0, keepdims=False)
    shape = mine.shape
    chunks = mine.reshape(2 * groups, shape[0] // (2 * groups), shape[1])
    spread = lax.all_to_all(chunks, ALL, 0, 0, tiled=True)
    device = jnp.arange(total, dtype=jnp.int32)
    number = 2 * lax.rem(device, groups) + device // groups
    slot = jnp.sum(
        jnp.where(permutation[None, :] == number[:, None], device[None, :], 0), axis=1
    )
    ordered = jnp.take(spread, device_of(slot, groups), axis=0)
    return lax.all_to_all(ordered, ALL, 0, 0, tiled=True).reshape(shape)


def layer_forward(length, x, layer, weights, vectors):
    bq, bv, bo, g1, b1, bi, b2, g2, bb2 = vectors
    q, k, v, log, context, unit1, scale1 = attend(length, x, layer, weights[:4], (bq, bv, bo))
    act, slope, unit2, scale2, result = feed(
        length, unit1, layer, weights[4], weights[5], (g1, b1, bi, b2, g2, bb2)
    )
    return result, (q, k, v, log, context, unit1, scale1, act, slope, unit2, scale2)


def layer_backward(length, grad, x, layer, weights, vectors, stored):
    q, k, v, log, context, unit1, scale1, act, slope, unit2, scale2 = stored
    g1, b1, g2 = vectors[3], vectors[4], vectors[7]
    d1, d2, first, rows, inner = feed_back(
        length, grad, unit2, scale2, unit1, scale1, act, slope, layer, weights[4], weights[5],
        (g1, b1, g2),
    )
    d_qkv, d_o, d_x, sums = attend_back(
        length, first, x, q, k, v, log, context, layer, weights[:4]
    )
    vectors = (sums[0], sums[1], rows[5], rows[3], rows[4], inner[0], rows[0], rows[1], rows[2])
    small = jnp.concatenate([v.reshape(2, -1) for v in vectors], axis=1).reshape(96, 128)
    return d_x, small, (d_qkv, d_o, d1, d2)


def on_device(
    inputs, cotangent, lengths, permutation, query_weight, query_bias, key_weight, value_weight,
    value_bias, output_weight, output_bias, first_gain, first_bias, inner_weight, inner_bias,
    outer_weight, outer_bias, second_gain, second_bias,
):
    core = lax.axis_index("section")
    group = lax.axis_index(GROUP)
    groups = lax.axis_size(GROUP)
    count = lax.axis_size("replica").bit_length() - 1
    shards = [
        w[0] for w in (query_weight, key_weight, value_weight, output_weight, inner_weight, outer_weight)
    ]
    vectors = [
        v[0] for v in (query_bias, value_bias, output_bias, first_gain, first_bias, inner_bias,
                       outer_bias, second_gain, second_bias)
    ]
    full = gather_weights(shards, jnp.concatenate(vectors).reshape(48, 128), count)
    weights, shared = full[:6], [split_vectors(full[6][s]) for s in range(2)]
    length = lax.dynamic_slice_in_dim(lengths, 2 * group + core, 1)
    x = lax.dynamic_index_in_dim(inputs, core, 0, keepdims=False)
    grad = own_cotangent(cotangent, permutation, groups)
    lower, lower_stored = layer_forward(length, x, 0, weights, shared[0])
    upper, upper_stored = layer_forward(length, lower, 1, weights, shared[1])
    upper_grad, upper_small, upper_parts = layer_backward(
        length, grad, lower, 1, weights, shared[1], upper_stored
    )
    lower_grad, lower_small, lower_parts = layer_backward(
        length, upper_grad, x, 0, weights, shared[0], lower_stored
    )
    total, small, input_grads, activations = reduce_grads(
        (lower_parts, upper_parts), jnp.stack([lower_small, upper_small]),
        (lower_grad, upper_grad), (lower, upper), permutation, count,
    )
    side = lax.axis_index("shard")
    own = lax.dynamic_index_in_dim(small.reshape(2, -1), side, 0, keepdims=False)
    pieces, at = [], 0
    for width in VECTORS:
        pieces.append(own[None, at : at + 512 * width])
        at += 512 * width
    dq, dk, dv, do, d1, d2 = unpack(total)
    return (
        activations[None], input_grads[None], dq, pieces[0], dk, dv, pieces[1], do, pieces[2], pieces[3],
        pieces[4], d1, pieces[5], d2, pieces[6], pieces[7], pieces[8],
    )


def solution(mesh):
    matrix, vector = P("section", "shard", None), P("section", "shard")
    rows = P(("shard", "replica"), None, None)
    in_specs = (
        rows, rows, P(), P(), matrix, vector, matrix, matrix, vector, matrix, vector, vector,
        vector, matrix, vector, matrix, vector, vector, vector,
    )
    both = P("section", ("shard", "replica"), None, None)
    out_specs = (
        both, both, matrix, vector, matrix, matrix, vector, matrix, vector, vector, vector,
        matrix, vector, matrix, vector, vector, vector,
    )
    return jax.shard_map(
        on_device, mesh=mesh, in_specs=in_specs, out_specs=out_specs, check_vma=False
    )
```

```python
import jax
import jax.numpy as jnp
from jax import lax
from jax.experimental import pallas as pl
from jax.experimental.pallas import tpu as pltpu

ALL = ("section", "shard", "replica")
GROUP = ("shard", "replica")
UNITS = 12
HALF = 256
VMEM_LIMIT = 64000000


def my_bits(count):
    replica = lax.axis_index("replica")
    return tuple((lax.rem(replica // (1 << (count - 1 - p)), 2) for p in range(count)))


def across(p, count, bits):
    replica = lax.axis_index("replica")
    weight = 1 << (count - 1 - p)
    return {"replica": replica + weight * (1 - 2 * bits[p])}


def place(device, replicas):
    groups = 2 * replicas
    return {
        "section": device // groups,
        "shard": lax.rem(device, groups) // replicas,
        "replica": lax.rem(device, replicas),
    }


def greet_all(me, devices, replicas):
    barrier = pltpu.get_barrier_semaphore()

    def hello(step, carry):
        pl.semaphore_signal(
            barrier, inc=1, device_id=place(lax.rem(me + step, devices), replicas),
            device_id_type=pl.DeviceIdType.MESH,
        )
        return carry

    lax.fori_loop(1, devices, hello, 0)
    pl.semaphore_wait(barrier, devices - 1)


def remote(src, dst, send_sem, recv_sem, partner):
    return pltpu.make_async_remote_copy(
        src_ref=src,
        dst_ref=dst,
        send_sem=send_sem,
        recv_sem=recv_sem,
        device_id=partner,
        device_id_type=pl.DeviceIdType.MESH,
    )


HEAD_DIM = 64
EPSILON = 1e-12
MASKED = -1000000000.0
HIDDEN_BLOCK = 512
WIDE = 256
BF = jnp.bfloat16
F32 = jnp.float32


def mm(a, b):
    return lax.dot_general(a, b, (((1,), (0,)), ((), ())), preferred_element_type=F32)


def mm_right(a, b):
    return lax.dot_general(a, b, (((1,), (1,)), ((), ())), preferred_element_type=F32)


def mm_left(a, b):
    return lax.dot_general(a, b, (((0,), (0,)), ((), ())), preferred_element_type=F32)


def normalized(values):
    average = jnp.mean(values, axis=-1, keepdims=True)
    centred = values - average
    variance = jnp.mean(centred * centred, axis=-1, keepdims=True)
    scale = lax.rsqrt(variance + EPSILON)
    return centred * scale, scale


def normalize_back(grad, unit, scale, gain):
    gs = grad * gain
    mean_gs = jnp.mean(gs, axis=-1, keepdims=True)
    mean_gn = jnp.mean(gs * unit, axis=-1, keepdims=True)
    return (gs - mean_gs - unit * mean_gn) * scale


def head_lanes(head):
    lane = lax.broadcasted_iota(jnp.int32, (1, WIDE), 1)
    return lane // HEAD_DIM == head


def row_sum(values):
    return jnp.sum(values, axis=0, keepdims=True)


def attend_body(
    step, steps, length, x, vectors, layer, wq, wk, wv, wo, q_out, k_out, v_out, log_out,
    context_out, unit_out, scale_out, total,
):
    slots = x.shape[0]
    rows = x[...]
    lanes_of = pl.ds(pl.multiple_of(step * WIDE, WIDE), WIDE)
    q = (mm(rows, wq[...]) + vectors[layer, 0:1, lanes_of]).astype(BF)
    k = mm(rows, wk[...]).astype(BF)
    v = (mm(rows, wv[...]) + vectors[layer, 1:2, lanes_of]).astype(BF)
    q_out[...] = q
    k_out[...] = k
    v_out[...] = v
    live = lax.broadcasted_iota(jnp.int32, (1, slots), 1) < length[0]
    scaled = (q.astype(F32) * 0.125).astype(BF)
    zero = jnp.zeros_like(scaled)
    context = jnp.zeros((slots, WIDE), F32)
    logs = jnp.zeros((slots, 128), F32)
    column = lax.broadcasted_iota(jnp.int32, (1, 128), 1)
    for head in range(WIDE // HEAD_DIM):
        lanes = head_lanes(head)
        scores = mm_right(jnp.where(lanes, scaled, zero), k)
        scores = jnp.where(live, scores, MASKED)
        highest = jnp.max(scores, axis=-1, keepdims=True)
        exponent = jnp.exp(scores - highest)
        totals = jnp.sum(exponent, axis=-1, keepdims=True)
        probs = (exponent * (1.0 / totals)).astype(BF)
        context = jnp.where(lanes, mm(probs, v), context)
        logs = jnp.where(column == head, highest + jnp.log(totals), logs)
    log_out[...] = jnp.transpose(logs)[:8]
    low = context.astype(BF)
    context_out[...] = low

    @pl.when(step == 0)
    def _():
        total[...] = rows.astype(F32) + vectors[layer, 2:3]

    total[...] += mm(low, wo[...])

    @pl.when(step == steps - 1)
    def _():
        unit, scale = normalized(total[...])
        unit_out[...] = unit
        scale_out[...] = jnp.broadcast_to(scale, scale_out.shape)


def feed_body(
    step, steps, length, vectors, halves, layer, unit1, w1, w2, act_out, slope_out, unit_out,
    scale_out, result_out, low, total,
):
    @pl.when(step == 0)
    def _():
        middle = unit1[...] * vectors[layer, 3:4] + vectors[layer, 4:5]
        low[...] = middle.astype(BF)
        total[...] = middle + vectors[layer, 9:10]

    per = steps // 2
    bias = halves[layer, step // per, pl.ds(5 + lax.rem(step, per), 1)]
    inner = mm(low[...], w1[...]) + bias
    cdf = 0.5 * (1.0 + lax.erf(inner * 0.7071067811865476))
    act = (inner * cdf).astype(BF)
    act_out[...] = act
    slope_out[...] = (cdf + inner * (jnp.exp(-0.5 * inner * inner) * 0.3989422804014327)).astype(BF)
    total[...] += mm(act, w2[...])

    @pl.when(step == steps - 1)
    def _():
        unit, scale = normalized(total[...])
        unit_out[...] = unit
        scale_out[...] = jnp.broadcast_to(scale, scale_out.shape)
        live = lax.broadcasted_iota(jnp.int32, (unit.shape[0], 1), 0) < length[0]
        result = unit * vectors[layer, 10:11] + vectors[layer, 11:12]
        result_out[...] = jnp.where(live, result, 0.0).astype(BF)


def feed_back_body(
    step, steps, length, grad, unit2, scale2, g2, unit1, scale1, g1, b1, act, slope, w1, w2,
    d1_out, d2_out, first_out, vectors_out, inner_rows, second, outer, low, total,
):
    @pl.when(step == 0)
    def _():
        live = lax.broadcasted_iota(jnp.int32, (grad.shape[0], 1), 0) < length[0]
        g = jnp.where(live, grad[...].astype(F32), 0.0)
        unit = unit2[...]
        d_second = normalize_back(g, unit, scale2[:, :1], g2[...])
        second[...] = d_second
        d_outer = d_second.astype(BF)
        outer[...] = d_outer
        vectors_out[0:1] = row_sum(d_outer.astype(F32))
        vectors_out[1:2] = row_sum(g * unit)
        vectors_out[2:3] = row_sum(g)
        low[...] = (unit1[...] * g1[...] + b1[...]).astype(BF)
        total[...] = jnp.zeros_like(total)

    d_outer = outer[...]
    d_inner = (mm_right(d_outer, w2[...]) * slope[...].astype(F32)).astype(BF)
    inner_rows[step, 0:1] = row_sum(d_inner.astype(F32))
    total[...] += mm_right(d_inner, w1[...])
    d2_out[...] = mm_left(act[...], d_outer).astype(BF).reshape(d2_out.shape)
    d1 = mm_left(low[...], d_inner).astype(BF)
    half = d1.shape[0] // 2
    d1_out[0, 0] = d1[:half]
    d1_out[1, 0] = d1[half:]

    @pl.when(step == steps - 1)
    def _():
        d_middle = second[...] + total[...]
        unit = unit1[...]
        d_first = normalize_back(d_middle, unit, scale1[:, :1], g1[...])
        first_out[...] = d_first
        vectors_out[3:4] = row_sum(d_middle * unit)
        vectors_out[4:5] = row_sum(d_middle)
        vectors_out[5:6] = row_sum(d_first.astype(BF).astype(F32))


def attend_back_body(
    step, steps, length, first, x, q, k, v, log, context, wq, wk, wv, wo, dqkv_out, do_out, x_out,
    sums_out, attended, total,
):
    slots = x.shape[0]

    @pl.when(step == 0)
    def _():
        attended[...] = first[...].astype(BF)
        total[...] = first[...]

    d_att = attended[...]
    d_context = mm_right(d_att, wo[...]).astype(BF)
    queries = q[...]
    keys = k[...]
    values = v[...]
    scaled = (queries.astype(F32) * 0.125).astype(BF)
    zero = jnp.zeros_like(scaled)
    live = lax.broadcasted_iota(jnp.int32, (slots, 1), 0) < length[0]
    d_q = jnp.zeros((slots, WIDE), F32)
    d_k = jnp.zeros((slots, WIDE), F32)
    d_v = jnp.zeros((slots, WIDE), F32)
    for head in range(WIDE // HEAD_DIM):
        lanes = head_lanes(head)
        scores = mm_right(keys, jnp.where(lanes, scaled, zero))
        scores = jnp.where(live, scores, MASKED)
        probs = jnp.exp(scores - log[head : head + 1])
        d_v = jnp.where(lanes, mm(probs.astype(BF), d_context), d_v)
        d_probs = mm_right(values, jnp.where(lanes, d_context, zero))
        dots = row_sum(probs * d_probs)
        d_scores = (probs * (d_probs - dots)).astype(BF)
        d_k = jnp.where(lanes, mm(d_scores, queries), d_k)
        d_q = jnp.where(lanes, mm_left(d_scores, keys), d_q)
    d_q = (d_q * 0.125).astype(BF)
    d_k = (d_k * 0.125).astype(BF)
    d_v = d_v.astype(BF)
    sums_out[step, 0:1] = row_sum(d_q.astype(F32))
    sums_out[step, 1:2] = row_sum(d_v.astype(F32))
    total[...] += mm_right(d_q, wq[...]) + mm_right(d_k, wk[...]) + mm_right(d_v, wv[...])
    rows = x[...]
    for at, value in enumerate((d_q, d_k, d_v)):
        weight = mm_left(rows, value).astype(BF)
        half = weight.shape[0] // 2
        dqkv_out[0, at] = weight[:half]
        dqkv_out[1, at] = weight[half:]
    do_out[...] = mm_left(context[...], d_att).astype(BF).reshape(do_out.shape)

    @pl.when(step == steps - 1)
    def _():
        x_out[...] = total[...].astype(BF)


def struct(shape, dtype):
    return jax.ShapeDtypeStruct(shape, dtype)


UNIT_ORDER = (0, 1, 2, 3, 4, 8, 9, 5, 10, 11, 6, 7)
DIRECT_SETS = ((0, 1, 6, 7), (0, 1, 6, 7))
HOPS = (0.0, 4.0, 8.0, 15.0, 18.0, 21.0, 24.0)
PACE = 5.6
CROSS = 11.3


class Plan:
    def __init__(self):
        self.entries = []
        self.done = set()

    def add(self, when, key, action):
        self.entries.append((when, len(self.entries), key, action))

    def sort(self):
        self.entries.sort(key=lambda entry: entry[:2])

    def run_first(self):
        _, _, key, action = self.entries.pop(0)
        action()
        self.done.add(key)

    def until(self, when):
        while self.entries and self.entries[0][0] <= when:
            self.run_first()

    def pending(self, when):
        return bool(self.entries) and self.entries[0][0] <= when

    def missing(self, keys):
        return any(key not in self.done for key in keys)

    def require(self, keys):
        while self.missing(keys):
            self.run_first()


def front_kernel(count, length, permutation, small, shards, inputs, outs, scratch):
    full, (rows_out, dealt), stored = outs[:6], outs[6:8], (outs[8:20], outs[20:32])
    (stage, spread, ordered, halves, rows, xs, unit1, scale1, unit2, scale2, low, total,
     send_sem, recv_sem, load_sem, store_sem, deal_send, deal_recv, home_send, home_recv,
     small_send, small_recv, keep_sem) = scratch
    core = lax.axis_index("section")
    side = lax.axis_index("shard")
    bits = my_bits(count)
    sibling = {"section": 1 - core}
    facing = {"shard": 1 - side}
    corner = {"section": 1 - core, "shard": 1 - side}
    replicas = 1 << count
    groups = 2 * replicas
    devices = 2 * groups
    group = side * replicas + lax.axis_index("replica")
    me = core * groups + group
    chunk, columns = spread.shape[1:]
    strip = HALF // replicas
    position = sum(bits[p] * (1 << p) for p in range(count))
    greet_all(me, devices, replicas)

    def chip(index):
        return {"shard": index // replicas, "replica": lax.rem(index, replicas)}

    def piece(index):
        where = pl.ds(pl.multiple_of(index * chunk, chunk), chunk)
        return inputs.at[:, where, pl.ds(pl.multiple_of(core * columns, columns), columns)]

    def spread_copy(target):
        return remote(
            piece(target), spread.at[pl.ds(2 * group, 2)], deal_send.at[target],
            deal_recv.at[group], chip(target),
        )

    spread_own = pltpu.make_async_copy(
        piece(group), spread.at[pl.ds(2 * group, 2)], deal_recv.at[group]
    )

    def spread_start(step, carry):
        spread_copy(lax.rem(group + step, groups)).start()
        return carry

    def spread_wait(step, carry):
        source = lax.rem(group + step, groups)
        landed = spread.at[pl.ds(2 * source, 2)]
        remote(
            landed, landed, deal_send.at[source], deal_recv.at[source], chip(source)
        ).wait_recv()
        return carry

    def spot(device):
        where = pl.ds(pl.multiple_of(lax.rem(device, groups) * chunk, chunk), chunk)
        start = pl.multiple_of((device // groups) * columns, columns)
        return xs.at[where, pl.ds(start, columns)]

    def slot_of(device):
        return 2 * lax.rem(device, groups) + device // groups

    def home_copy(target):
        return remote(
            ordered.at[slot_of(target)], spot(me), home_send.at[target], home_recv.at[me],
            place(target, replicas),
        )

    home_own = pltpu.make_async_copy(ordered.at[slot_of(me)], spot(me), home_recv.at[me])

    def home_start(step, carry):
        home_copy(lax.rem(me + step, devices)).start()
        return carry

    def home_wait(step, carry):
        source = lax.rem(me + step, devices)
        remote(
            spot(source), spot(source), home_send.at[source], home_recv.at[source],
            place(source, replicas),
        ).wait_recv()
        return carry

    def spread_done(step, carry):
        spread_copy(lax.rem(group + step, groups)).wait_send()
        return carry

    def home_done(step, carry):
        home_copy(lax.rem(me + step, devices)).wait_send()
        return carry

    def reorder(slot, carry):
        ordered[slot] = spread[permutation[slot]]
        return carry

    def deal_second():
        spread_own.wait()
        lax.fori_loop(1, groups, spread_wait, 0)
        lax.fori_loop(0, devices, reorder, 0)
        home_own.start()
        lax.fori_loop(1, devices, home_start, 0)

    def deal_last():
        home_own.wait()
        lax.fori_loop(1, devices, home_wait, 0)

    def small_copy(index, partner):
        return remote(
            small, halves.at[core, side], small_send.at[index], small_recv.at[index], partner
        )

    small_own = pltpu.make_async_copy(small, halves.at[core, side], small_send.at[3])

    def vectors_here():
        small_own.wait()
        for index, layer, half, partner in (
            (0, 1 - core, side, sibling), (1, core, 1 - side, facing),
            (2, 1 - core, 1 - side, corner),
        ):
            landed = halves.at[layer, half]
            remote(
                landed, landed, small_send.at[index], small_recv.at[index], partner
            ).wait_recv()
        for layer in range(2):
            for half in range(2):
                rows[layer, :, pl.ds(512 * half, 512)] = halves[layer, half]

    def shard_at(unit, start, size):
        where = pl.ds(start, size)
        if unit < 4:
            return shards[unit].at[where]
        if unit < 8:
            return shards[4].at[where, pl.ds(1024 * (unit - 4), 1024)]
        return shards[5].at[pl.ds(512 * (unit - 8) + start, size)]

    def out_at(layer, unit, half, start, size):
        base = 512 * half + start if unit < 8 else 2048 * half + 512 * (unit - 8) + start
        where = pl.ds(pl.multiple_of(base, strip), size)
        if unit < 4:
            return full[unit].at[layer, where]
        if unit < 8:
            return full[4].at[layer, where, pl.ds(1024 * (unit - 4), 1024)]
        return full[5].at[layer, where]

    mine = HALF * core

    def wire(layer, unit, hop, src, dst, partner):
        index = UNITS * layer + unit
        return remote(src, dst, send_sem.at[index, hop], recv_sem.at[index, hop], partner)

    def arrive(layer, unit, hop, landed, partner):
        wire(layer, unit, hop, landed, landed, partner).wait_recv()

    def cross_rows(layer, unit):
        if unit in DIRECT_SETS[layer]:
            return mine, HALF
        return pl.multiple_of(mine + position * strip, strip), strip

    def cross(layer, unit):
        start, size = cross_rows(layer, unit)
        target = out_at(layer, unit, side, start, size)

        @pl.when(core == layer)
        def _():
            wire(layer, unit, 0, shard_at(unit, start, size), target, facing).start()

        @pl.when(core != layer)
        def _():
            arrive(layer, unit, count + 2, out_at(layer, unit, side, 0, 512), sibling)
            wire(layer, unit, 0, target, target, facing).start()

    def block(k):
        return pl.multiple_of(mine + ((position >> k) << k) * strip, strip), strip << k

    def other_block(k):
        start = ((position >> k) ^ 1) << k
        return pl.multiple_of(mine + start * strip, strip), strip << k

    def hop(layer, unit, k):
        there = 1 - side
        if k == 0:
            arrive(layer, unit, 0, out_at(layer, unit, there, *cross_rows(layer, unit)), facing)
        else:
            arrive(
                layer, unit, k, out_at(layer, unit, there, *other_block(k - 1)),
                across(k - 1, count, bits),
            )
        if k < count and unit not in DIRECT_SETS[layer]:
            held = out_at(layer, unit, there, *block(k))
            wire(layer, unit, k + 1, held, held, across(k, count, bits)).start()
        else:
            held = out_at(layer, unit, there, mine, HALF)
            wire(layer, unit, count + 1, held, held, sibling).start()

    def passed(layer, unit):
        landed = out_at(layer, unit, 1 - side, HALF * (1 - core), HALF)
        arrive(layer, unit, count + 1, landed, sibling)

        @pl.when(core == layer)
        def _():
            store(layer, unit).wait()

    def store(layer, unit):
        return pltpu.make_async_copy(
            stage.at[unit], out_at(layer, unit, side, 0, 512), store_sem.at[unit]
        )

    def load(unit):
        return pltpu.make_async_copy(shard_at(unit, 0, 512), stage.at[unit], load_sem.at[unit])

    def own_start(layer):
        for unit in UNIT_ORDER:
            source = shard_at(unit, 0, 512)
            wire(
                layer, unit, count + 2, source, out_at(layer, unit, side, 0, 512), sibling
            ).start()
            load(unit).start()

    def own_store(layer):
        for unit in UNIT_ORDER:
            load(unit).wait()
            store(layer, unit).start()

    plan = Plan()
    number = [0, 0]
    for layer in range(2):
        for unit in UNIT_ORDER:
            key = (layer, unit)
            if unit in DIRECT_SETS[layer]:
                landing = 14.0 + CROSS * (number[0] + 1)
                number[0] += 1
                plan.add(landing - 2.5 * CROSS, ("cross",) + key, lambda l=layer, u=unit: cross(l, u))
                plan.add(landing, ("hop",) + key, lambda l=layer, u=unit: hop(l, u, 0))
                plan.add(landing + 3.0, ("unit",) + key, lambda l=layer, u=unit: passed(l, u))
            else:
                begin = 6.0 + PACE * number[1]
                number[1] += 1
                plan.add(begin - 16.0, ("cross",) + key, lambda l=layer, u=unit: cross(l, u))
                for k in range(count + 1):
                    plan.add(
                        begin + HOPS[k], ("hop", k) + key, lambda l=layer, u=unit, k=k: hop(l, u, k)
                    )
                plan.add(
                    begin + HOPS[count] + 3.0, ("unit",) + key,
                    lambda l=layer, u=unit: passed(l, u),
                )
    plan.add(20.0, "deal", deal_second)
    plan.add(40.0, "inputs", deal_last)
    plan.add(10.0, "vectors", vectors_here)
    plan.sort()

    spread_own.start()
    lax.fori_loop(1, groups, spread_start, 0)
    for index, partner in enumerate((sibling, facing, corner)):
        small_copy(index, partner).start()
    small_own.start()
    for layer in range(2):
        @pl.when(core == layer)
        def _():
            own_start(layer)
    plan.until(1.0)
    for layer in range(2):
        @pl.when(core == layer)
        def _():
            own_store(layer)

    slots, width = xs.shape
    attention_steps = width // WIDE
    hidden = full[4].shape[-1]
    hidden_steps = hidden // HIDDEN_BLOCK
    band = pl.BlockSpec((slots, WIDE), lambda j: (0, j))
    wide = pl.BlockSpec((width, WIDE), lambda j: (0, j))
    hidden_band = pl.BlockSpec((slots, HIDDEN_BLOCK), lambda j: (0, j))

    def during(step, steps, begin, each, needs):
        for at in range(steps):
            when = begin + each * at
            wanted = needs(at)
            if plan.pending(when) or plan.missing(wanted):
                @pl.when(step == at)
                def _():
                    plan.require(wanted)
                    plan.until(when)

    def attend_stage(layer, begin):
        (q, k, v, log, context) = stored[layer][:5]

        def body(*refs):
            step = pl.program_id(0)
            attend_body(step, attention_steps, length, xs, rows, layer, *refs, unit1, scale1, total)
            during(step, attention_steps, begin, 5.0, lambda at: [])

        pltpu.emit_pipeline(
            body,
            grid=(attention_steps,),
            in_specs=[wide, wide, wide, pl.BlockSpec((WIDE, width), lambda j: (j, 0))],
            out_specs=[
                band, band, band, pl.BlockSpec((None, 8, slots), lambda j: (j, 0, 0)), band
            ],
        )(*(full[i].at[layer] for i in range(4)), q, k, v, log, context)

    def feed_needs(layer, step):
        return [
            ("unit", layer, unit)
            for at in range(min(step + 1, hidden_steps))
            for unit in (4 + at * HIDDEN_BLOCK // 1024, 8 + at % 4)
        ]

    def feed_stage(layer, begin):
        act, slope = stored[layer][7:9]

        def body(*refs):
            step = pl.program_id(0)
            feed_body(
                step, hidden_steps, length, rows, halves, layer, unit1, *refs, unit2, scale2, xs,
                low, total,
            )
            during(step, hidden_steps, begin, 2.5, lambda at: feed_needs(layer, at + 2))

        pltpu.emit_pipeline(
            body,
            grid=(hidden_steps,),
            in_specs=[
                pl.BlockSpec((width, HIDDEN_BLOCK), lambda j: (0, j)),
                pl.BlockSpec((HIDDEN_BLOCK, width), lambda j: (j, 0)),
            ],
            out_specs=[hidden_band, hidden_band],
        )(full[4].at[layer], full[5].at[layer], act, slope)

    def keep(source, target, at):
        copy = pltpu.make_async_copy(source, target, keep_sem.at[at])
        copy.start()
        return copy

    begin = (45.0, 95.0)
    keeping = []
    for layer in range(2):
        plan.require(["vectors", "inputs"] + [("unit", layer, unit) for unit in range(4)])
        if layer == 0:
            keeping += [keep(xs, dealt, 0), keep(rows, rows_out, 1)]
        attend_stage(layer, begin[layer])
        for copy in keeping:
            copy.wait()
        keeping = [keep(unit1, stored[layer][5], 2), keep(scale1, stored[layer][6], 3)]
        plan.require(feed_needs(layer, 1))
        feed_stage(layer, begin[layer] + 22.0)
        for copy in keeping:
            copy.wait()
        keeping = [
            keep(unit2, stored[layer][9], 4), keep(scale2, stored[layer][10], 5),
            keep(xs, stored[layer][11], 6),
        ]
    plan.until(1000000.0)
    for copy in keeping:
        copy.wait()
    lax.fori_loop(1, groups, spread_done, 0)
    lax.fori_loop(1, devices, home_done, 0)
    for index, partner in enumerate((sibling, facing, corner)):
        small_copy(index, partner).wait_send()
    for layer in range(2):
        for unit in range(UNITS):
            start, size = cross_rows(layer, unit)
            crossed = out_at(layer, unit, side, start, size)
            wire(layer, unit, 0, crossed, crossed, facing).wait_send()
            if unit not in DIRECT_SETS[layer]:
                for k in range(count):
                    held = out_at(layer, unit, 1 - side, *block(k))
                    wire(layer, unit, k + 1, held, held, across(k, count, bits)).wait_send()
            held = out_at(layer, unit, 1 - side, mine, HALF)
            wire(layer, unit, count + 1, held, held, sibling).wait_send()

        @pl.when(core == layer)
        def _():
            for unit in range(UNITS):
                own = out_at(layer, unit, side, 0, 512)
                wire(layer, unit, count + 2, own, own, sibling).wait_send()


def forward(length, permutation, small, shards, inputs, count):
    groups = 2 << count
    slots, width = inputs.shape[1:]
    hidden = shards[4].shape[-1]
    part = (2 * groups, slots // groups, width // 2)
    dma = pltpu.SemaphoreType.DMA
    square = (slots, width)
    steps = width // WIDE
    layer = [
        struct(square, BF), struct(square, BF), struct(square, BF), struct((steps, 8, slots), F32),
        struct(square, BF), struct(square, F32), struct((slots, 128), F32),
        struct((slots, hidden), BF), struct((slots, hidden), BF), struct(square, F32),
        struct((slots, 128), F32), struct(square, BF),
    ]
    out_shape = (
        [struct((2, width, width), BF)] * 4
        + [struct((2, width, hidden), BF), struct((2, hidden, width), BF)]
        + [struct((2,) + small.shape[:1] + (width,), F32), struct(square, BF)]
        + layer + layer
    )
    smem = pl.BlockSpec(memory_space=pltpu.SMEM)
    anywhere = pl.BlockSpec(memory_space=pl.ANY)

    def kernel(*refs):
        front_kernel(
            count, *refs[:3], refs[3:9], refs[9], refs[10 : 10 + len(out_shape)],
            refs[10 + len(out_shape) :],
        )

    return pl.pallas_call(
        kernel,
        out_shape=out_shape,
        in_specs=[smem, smem] + [anywhere] * 8,
        out_specs=[anywhere] * len(out_shape),
        scratch_shapes=[
            pltpu.VMEM((UNITS, 512, 1024), BF), pltpu.VMEM(part, BF), pltpu.VMEM(part, BF),
            pltpu.VMEM((2, 2) + small.shape, F32),
            pltpu.VMEM((2,) + small.shape[:1] + (width,), F32),
            pltpu.VMEM(square, BF), pltpu.VMEM(square, F32), pltpu.VMEM((slots, 128), F32),
            pltpu.VMEM(square, F32), pltpu.VMEM((slots, 128), F32),
            pltpu.VMEM(square, BF), pltpu.VMEM(square, F32),
            dma((2 * UNITS, count + 3)), dma((2 * UNITS, count + 3)), dma((UNITS,)), dma((UNITS,)),
            dma((groups,)), dma((groups,)), dma((2 * groups,)), dma((2 * groups,)),
            dma((4,)), dma((3,)), dma((7,)),
        ],
        compiler_params=pltpu.CompilerParams(
            collective_id=0, has_side_effects=True, vmem_limit_bytes=VMEM_LIMIT
        ),
        name="forward",
    )(length, permutation, small, *shards, inputs)


SENT_RING = 4
LAND_RING = 5
PIECES = 2 * UNITS
DEAL_STEP = 5
EARLY = ((0, 1, 2, 3), (1, 3, 5, 7), (0, 1, 2, 3))
AHEAD = sum(len(steps) for steps in EARLY)


def device_of(number, groups):
    return lax.rem(number, 2) * groups + number // 2


def back_kernel(count, length, inverse, gains, lower, upper, weights, results, outs, scratch):
    (total, small_total, landing, dealt, acts, d1_low, d2_low, dqkv_low, do_low, up_d1, up_d2,
     dqkv_up, do_up, grad_low, grad_up) = outs
    (xs, first, gradient, unit1, unit2, scale1, scale2, second, outer, middle, running, attended,
     vectors, inner_rows, sums) = scratch[:15]
    (own, came, across_half, kept, from_x), rest = scratch[15:20], scratch[20:]
    halves, rest = rest[:count], rest[count:]
    (spread, ordered, smalls, small_own, small_recv, send0, recv0, send_x, recv_x, send_rs, recv_rs,
     send_ag, recv_ag, load_sem, came_sem, piece_sem, small_send, small_arrive, deal_send,
     deal_recv, home_send, home_recv, act_sem, total_sem, fetch_sem, done_send, done_recv) = rest
    wq, wk, wv, wo, w1, w2 = weights
    (up_unit2, up_scale2, up_unit1, up_scale1, up_act, up_slope, up_x, up_q, up_k, up_v, up_log,
     up_context, cotangent) = upper
    (low_unit2, low_scale2, low_unit1, low_scale1, low_act, low_slope, low_x, low_q, low_k, low_v,
     low_log, low_context) = lower
    core = lax.axis_index("section")
    side = lax.axis_index("shard")
    replica = lax.axis_index("replica")
    bits = my_bits(count)
    sibling = {"section": 1 - core}
    facing = {"shard": 1 - side}
    everything = (slice(None),) * count
    rows = kept.shape[-2]
    keep_ring = kept.shape[0]
    replicas = 1 << count
    groups = 2 * replicas
    group = side * replicas + replica
    me = core * groups + group
    chunk = spread.shape[1]
    greet_all(me, 2 * groups, replicas)

    layers = ((up_d1, up_d2, dqkv_up, do_up), (d1_low, d2_low, dqkv_low, do_low))
    ranges, at = [], 0
    for order in range(2):
        for index in range(4):
            depth = layers[order][index].shape[1]
            ranges.append((order, index, at, at + depth))
            at += depth

    def part_of(order, index, unit, half):
        where = pl.ds(pl.multiple_of(HALF * half, HALF), HALF)
        return layers[order][index].at[:, unit, where]

    def core_copy(unit, source=None):
        source = landing.at[unit] if source is None else source
        return remote(source, landing.at[unit], send0.at[unit], recv0.at[unit], sibling)

    def send_core(order, which):
        for at_order, index, low, high in ranges:
            if at_order == order and index in which:
                for unit in range(low, high):
                    core_copy(unit, part_of(order, index, unit - low, 1 - core)).start()

    def own_load(source, slot):
        return pltpu.make_async_copy(source, own.at[slot], load_sem.at[slot])

    def came_load(unit):
        slot = lax.rem(unit, 2)
        return pltpu.make_async_copy(landing.at[unit], came.at[slot], came_sem.at[slot])

    def start_load(unit):
        for order, index, low, high in ranges:
            @pl.when(jnp.logical_and(unit >= low, unit < high))
            def _():
                own_load(part_of(order, index, unit - low, core), lax.rem(unit, 2)).start()

    def x_copy(unit):
        return remote(
            across_half.at[lax.rem(unit, SENT_RING)], from_x.at[lax.rem(unit, LAND_RING)],
            send_x.at[unit], recv_x.at[unit], facing,
        )

    def rs_copy(unit, p):
        slot = lax.rem(unit, keep_ring)
        return remote(
            kept.at[(slot,) + everything[:p] + (1 - bits[p],) + bits[p + 1 :]],
            halves[p].at[lax.rem(unit, LAND_RING)],
            send_rs.at[p, unit],
            recv_rs.at[p, unit],
            across(p, count, bits),
        )

    def ag_copy(unit, p):
        where = (unit,) + everything[:p] + bits[p:]
        source = kept.at[(lax.rem(unit, keep_ring),) + bits] if p == 0 else total.at[where]
        return remote(
            source, total.at[where], send_ag.at[p, unit], recv_ag.at[p, unit],
            across(p, count, bits),
        )

    def ag_arrive(unit, p):
        where = total.at[(unit,) + everything[:p] + (1 - bits[p],) + bits[p + 1 :]]
        remote(
            where, where, send_ag.at[p, unit], recv_ag.at[p, unit], across(p, count, bits)
        ).wait_recv()

    def piece_copy(unit):
        return pltpu.make_async_copy(
            kept.at[(lax.rem(unit, keep_ring),) + bits], total.at[(unit,) + bits],
            piece_sem.at[unit],
        )

    def done_copy(unit):
        index = lax.rem(unit, UNITS)
        return remote(
            total.at[unit], total.at[PIECES + index], done_send.at[index], done_recv.at[index],
            sibling,
        )

    def small_copy(step):
        partner = [sibling, facing] + [across(p, count, bits) for p in range(count)]
        source = smalls.at[1 - core] if step == 0 else small_own.at[step - 1]
        return remote(
            source, small_recv.at[step], small_send.at[step], small_arrive.at[step], partner[step]
        )

    def chunk_of(layer, target):
        return results[layer].at[pl.ds(pl.multiple_of(target * chunk, chunk), chunk)]

    def spread_copy(layer, target):
        return remote(
            chunk_of(layer, lax.rem(target, groups)), spread.at[me], deal_send.at[target],
            deal_recv.at[me], place(target, replicas),
        )

    def spread_own(layer):
        return pltpu.make_async_copy(chunk_of(layer, group), spread.at[me], deal_recv.at[me])

    def spread_start(step, carry):
        target = lax.rem(me + step, 2 * groups)
        for layer in range(2):
            @pl.when(target // groups == layer)
            def _():
                spread_copy(layer, target).start()
        return carry

    def spread_wait(step, carry):
        source = lax.rem(me + step, 2 * groups)
        remote(
            spread.at[source], spread.at[source], deal_send.at[source], deal_recv.at[source],
            place(source, replicas),
        ).wait_recv()
        return carry

    def chip(index):
        return {"shard": index // replicas, "replica": lax.rem(index, replicas)}

    def home_copy(target):
        return remote(
            ordered.at[pl.ds(2 * target, 2)], dealt.at[:, group], home_send.at[target],
            home_recv.at[group], chip(target),
        )

    def home_own():
        return pltpu.make_async_copy(
            ordered.at[pl.ds(2 * group, 2)], dealt.at[:, group], home_recv.at[group]
        )

    def home_start(step, carry):
        home_copy(lax.rem(group + step, groups)).start()
        return carry

    def home_wait(step, carry):
        source = lax.rem(group + step, groups)
        remote(
            dealt.at[:, source], dealt.at[:, source], home_send.at[source], home_recv.at[source],
            chip(source),
        ).wait_recv()
        return carry

    def reorder(slot, carry):
        ordered[slot] = spread[device_of(inverse[slot], groups)]
        return carry

    def places_of(index, dims):
        return tuple((lax.rem(index // (1 << (dims - 1 - q)), 2) for q in range(dims)))

    def tick(now):
        @pl.when(jnp.logical_and(now >= SENT_RING, now < PIECES + SENT_RING))
        def _():
            x_copy(now - SENT_RING).wait_send()

        @pl.when(jnp.logical_and(now >= keep_ring, now < PIECES + keep_ring))
        def _():
            for p in range(count):
                rs_copy(now - keep_ring, p).wait_send()
            ag_copy(now - keep_ring, 0).wait_send()

        @pl.when(now < PIECES)
        def _():
            unit = now
            slot = lax.rem(unit, 2)

            @pl.when(unit == 0)
            def _():
                start_load(0)
                core_copy(0).wait_recv()
                came_load(0).start()

            own_load(landing.at[unit], slot).wait()
            came_load(unit).wait()

            @pl.when(unit + 1 < PIECES)
            def _():
                start_load(unit + 1)
                core_copy(unit + 1).wait_recv()
                came_load(unit + 1).start()

            out_slot = lax.rem(unit, SENT_RING)
            kept_slot = lax.rem(unit, keep_ring)

            def add(block, c):
                where = pl.ds(pl.multiple_of(block * 32, 32), 32)
                across_half[out_slot, where] = (
                    own[slot, 1 - side, where] + came[slot, 1 - side, where]
                )
                return c

            lax.fori_loop(0, HALF // 32, add, 0)
            x_copy(unit).start()

            def add_kept(index, c):
                where = pl.ds(pl.multiple_of(index * rows, rows), rows)
                mine = (kept_slot,) + places_of(index, count)
                kept[mine] = own[slot, side, where] + came[slot, side, where]
                return c

            lax.fori_loop(0, 1 << count, add_kept, 0)

        @pl.when(jnp.logical_and(now >= 1, now < PIECES + 1))
        def _():
            unit = now - 1
            slot = lax.rem(unit, keep_ring)
            land = lax.rem(unit, LAND_RING)
            x_copy(unit).wait_recv()

            def add(index, c):
                where = pl.ds(pl.multiple_of(index * rows, rows), rows)
                mine = (slot,) + places_of(index, count)
                kept[mine] = kept[mine] + from_x[land, where]
                return c

            lax.fori_loop(0, 1 << count, add, 0)
            rs_copy(unit, count - 1).start()

        for step in range(count):
            p = count - 1 - step

            @pl.when(jnp.logical_and(now >= 2 + step, now < PIECES + 2 + step))
            def _():
                unit = now - (2 + step)
                slot = lax.rem(unit, keep_ring)
                land = lax.rem(unit, LAND_RING)
                rs_copy(unit, p).wait_recv()

                def add(index, c):
                    mine = (slot,) + places_of(index, p) + bits[p:]
                    kept[mine] = kept[mine] + halves[p][(land,) + places_of(index, p)]
                    return c

                if p == 0:
                    add(0, 0)
                    piece_copy(unit).start()
                    ag_copy(unit, 0).start()
                else:
                    lax.fori_loop(0, 1 << p, add, 0)
                    rs_copy(unit, p - 1).start()

        for p in range(count):
            lag = 2 + count + p

            @pl.when(jnp.logical_and(now >= lag, now < PIECES + lag))
            def _():
                unit = now - lag
                ag_arrive(unit, p)
                if p == 0:
                    piece_copy(unit).wait()
                if p + 1 < count:
                    ag_copy(unit, p + 1).start()
                else:
                    @pl.when((unit < UNITS) == (core == 0))
                    def _():
                        done_copy(unit).start()

    def early(step, phase):
        before = sum(len(steps) for steps in EARLY[:phase])
        now = -1
        for at, when in enumerate(EARLY[phase]):
            now = jnp.where(step == when, before + at, now)

        @pl.when(now >= 0)
        def _():
            tick(now)

    def fetch(source, target, at):
        copy = pltpu.make_async_copy(source, target, fetch_sem.at[at])
        copy.start()
        return copy

    waits = [
        fetch(cotangent, gradient, 0), fetch(up_unit1, unit1, 2), fetch(up_unit2, unit2, 3),
        fetch(up_scale1, scale1, 4), fetch(up_scale2, scale2, 5),
    ]
    up_rows = fetch(up_x, xs, 1)
    for layer in range(2):
        @pl.when(core == layer)
        def _():
            spread_own(layer).start()
    lax.fori_loop(1, 2 * groups, spread_start, 0)
    for copy in waits:
        copy.wait()

    slots, width = xs.shape
    attention_steps = width // WIDE
    hidden_steps = w1.shape[-1] // HIDDEN_BLOCK
    per = 512 // WIDE
    wide_per = 1024 // HIDDEN_BLOCK
    pairs = HIDDEN_BLOCK // 512
    band = pl.BlockSpec((slots, WIDE), lambda j: (0, j))
    columns = pl.BlockSpec((width, WIDE), lambda j: (0, j))

    def attention(layer, phase, q, k, v, log, context, dqkv, do):
        def body(*refs):
            step = pl.program_id(0)
            attend_back_body(
                step, attention_steps, length, first, xs, *refs, gradient, sums, attended, running
            )
            early(step, phase)

        pltpu.emit_pipeline(
            body,
            grid=(attention_steps,),
            in_specs=[
                band, band, band, pl.BlockSpec((None, 8, slots), lambda j: (j, 0, 0)), band,
                columns, columns, columns, pl.BlockSpec((WIDE, width), lambda j: (j, 0)),
            ],
            out_specs=[
                pl.BlockSpec((2, 3, 512, WIDE), lambda j: (0, 0, 0, j)),
                pl.BlockSpec((1, 1, WIDE, width), lambda j: (j // per, 0, j % per, 0)),
            ],
        )(q, k, v, log, context, wq.at[layer], wk.at[layer], wv.at[layer], wo.at[layer], dqkv, do)
        for at in range(attention_steps):
            lanes = pl.ds(WIDE * at, WIDE)
            smalls[layer, 0:1, lanes] = sums[at, 0:1]
            smalls[layer, 1:2, lanes] = sums[at, 1:2]

    hidden_band = pl.BlockSpec((slots, HIDDEN_BLOCK), lambda j: (0, j))

    def deal_second():
        spread_own(0).wait()
        lax.fori_loop(1, 2 * groups, spread_wait, 0)
        lax.fori_loop(0, 2 * groups, reorder, 0)
        home_own().start()
        lax.fori_loop(1, groups, home_start, 0)

    def feed_stage(layer, act, slope, d1, d2):
        def body(*refs):
            step = pl.program_id(0)
            feed_back_body(
                step, hidden_steps, length, gradient, unit2, scale2, gains.at[layer, 10:11],
                unit1, scale1, gains.at[layer, 3:4], gains.at[layer, 4:5], *refs, first,
                vectors, inner_rows, second, outer, middle, running,
            )
            if layer == 0:
                early(step, 1)
            else:
                pl.when(step == DEAL_STEP)(deal_second)

        pltpu.emit_pipeline(
            body,
            grid=(hidden_steps,),
            in_specs=[
                hidden_band, hidden_band,
                pl.BlockSpec((width, HIDDEN_BLOCK), lambda j: (0, j)),
                pl.BlockSpec((HIDDEN_BLOCK, width), lambda j: (j, 0)),
            ],
            out_specs=[
                pl.BlockSpec(
                    (2, 1, 512, HIDDEN_BLOCK), lambda j: (0, j // wide_per, 0, j % wide_per)
                ),
                pl.BlockSpec(
                    (1, pairs, 512, width),
                    lambda j: (j // (hidden_steps // 2), j % (hidden_steps // 2), 0, 0),
                ),
            ],
        )(act, slope, w1.at[layer], w2.at[layer], d1, d2)
        for at, source in ((2, 5), (3, 3), (4, 4), (9, 0), (10, 1), (11, 2)):
            smalls[layer, at : at + 1] = vectors[source : source + 1]
        for at in range(hidden_steps):
            line = 5 + at // wide_per
            lanes = pl.ds(HIDDEN_BLOCK * (at % wide_per), HIDDEN_BLOCK)
            smalls[layer, line : line + 1, lanes] = inner_rows[at, 0:1]

    feed_stage(1, up_act, up_slope, up_d1, up_d2)
    send_core(0, (0, 1))
    later = [
        fetch(low_unit1, unit1, 2), fetch(low_unit2, unit2, 3), fetch(low_scale1, scale1, 4),
        fetch(low_scale2, scale2, 5),
    ]
    up_rows.wait()
    attention(1, 0, up_q, up_k, up_v, up_log, up_context, dqkv_up, do_up)
    send_core(0, (2, 3))
    waits = [fetch(gradient, grad_up, 0), fetch(low_x, xs, 1)]
    for copy in later:
        copy.wait()
    feed_stage(0, low_act, low_slope, d1_low, d2_low)
    send_core(1, (0, 1))
    for copy in waits:
        copy.wait()
    attention(0, 2, low_q, low_k, low_v, low_log, low_context, dqkv_low, do_low)
    send_core(1, (2, 3))
    small_copy(0).start()
    held = fetch(gradient, grad_low, 0)
    held.wait()
    small_steps = count + 2
    both = (grad_low, grad_up)

    def exchange(layer):
        return remote(both[1 - layer], acts.at[layer], act_sem.at[0], act_sem.at[1], sibling)

    for layer in range(2):
        @pl.when(core == layer)
        def _():
            exchange(layer).start()
    grad_back = fetch(grad_up, xs, 1)
    grad_back.wait()

    @pl.when(core == 0)
    def _():
        pltpu.make_async_copy(gradient, acts.at[0], act_sem.at[2]).start()

    @pl.when(core == 1)
    def _():
        pltpu.make_async_copy(xs, acts.at[1], act_sem.at[2]).start()

    def late(now, carry):
        for step in range(small_steps):
            @pl.when(now == step + 1)
            def _():
                small_copy(step).wait_recv()
                before = smalls[core] if step == 0 else small_own[step - 1]
                small_own[step] = before + small_recv[step]
                if step + 1 < small_steps:
                    small_copy(step + 1).start()

        tick(now + AHEAD)
        return carry

    lax.fori_loop(0, PIECES + max(keep_ring, 2 + 2 * count) - AHEAD, late, 0)
    out = pltpu.make_async_copy(small_own.at[small_steps - 1], small_total, total_sem)
    out.start()

    def last(unit, carry):
        core_copy(unit).wait_send()
        for p in range(1, count):
            ag_copy(unit, p).wait_send()
        return carry

    lax.fori_loop(0, PIECES, last, 0)

    def swapped(index, carry):
        done_copy(index).wait_send()
        done_copy(index).wait_recv()
        return carry

    lax.fori_loop(0, UNITS, swapped, 0)
    for step in range(small_steps):
        small_copy(step).wait_send()

    def spread_done(step, carry):
        spread_copy(0, lax.rem(me + step, 2 * groups)).wait_send()
        return carry

    def home_done(step, carry):
        home_copy(lax.rem(group + step, groups)).wait_send()
        return carry

    lax.fori_loop(1, 2 * groups, spread_done, 0)
    home_own().wait()
    lax.fori_loop(1, groups, home_wait, 0)
    lax.fori_loop(1, groups, home_done, 0)
    back = remote(both[0], acts.at[1 - core], act_sem.at[0], act_sem.at[1], sibling)
    back.wait_send()
    back.wait_recv()
    pltpu.make_async_copy(xs, acts.at[core], act_sem.at[2]).wait()
    out.wait()


def backward(length, inverse, gains, lower, upper, weights, results, count):
    cut = (2,) * count
    rows = HALF // (1 << count)
    narrow = cut + (rows, 1024)
    dma = pltpu.SemaphoreType.DMA
    groups = 2 << count
    slots, width = results[0].shape
    chunk = slots // groups
    keep_ring = count + 5
    hidden = weights[4].shape[-1]
    sizes = [len(lower), len(upper), len(weights), len(results)]

    def kernel(*refs):
        start, groups_of = 3, []
        for size in sizes:
            groups_of.append(refs[start : start + size])
            start += size
        back_kernel(count, *refs[:3], *groups_of, refs[start : start + 15], refs[start + 15 :])

    anywhere = pl.BlockSpec(memory_space=pl.ANY)
    vmem = pl.BlockSpec(memory_space=pltpu.VMEM)
    smem = pl.BlockSpec(memory_space=pltpu.SMEM)
    vectors = (UNITS, width)
    square = (slots, width)
    feed_shape, head_shape = (2, 4, 512, 1024), (2, 3, 512, 1024)
    out_shape = [
        struct((PIECES + UNITS,) + narrow, BF),
        struct(vectors, F32),
        struct((PIECES, 2, HALF, 1024), BF),
        struct((2, groups, chunk, width), BF),
        struct((2,) + square, BF),
        struct(feed_shape, BF), struct(feed_shape, BF),
        struct(head_shape, BF), struct((2, 1, 512, 1024), BF),
        struct(feed_shape, BF), struct(feed_shape, BF),
        struct(head_shape, BF), struct((2, 1, 512, 1024), BF),
        struct(square, BF), struct(square, BF),
    ]
    result = pl.pallas_call(
        kernel,
        out_shape=out_shape,
        in_specs=[smem, smem, vmem] + [anywhere] * sum(sizes),
        out_specs=[anywhere] * len(out_shape),
        scratch_shapes=[
            pltpu.VMEM(square, BF), pltpu.VMEM(square, F32), pltpu.VMEM(square, BF),
            pltpu.VMEM(square, F32), pltpu.VMEM(square, F32),
            pltpu.VMEM((slots, 128), F32), pltpu.VMEM((slots, 128), F32),
            pltpu.VMEM(square, F32), pltpu.VMEM(square, BF), pltpu.VMEM(square, BF),
            pltpu.VMEM(square, F32), pltpu.VMEM(square, BF),
            pltpu.VMEM((8, width), F32),
            pltpu.VMEM((hidden // HIDDEN_BLOCK, 8, HIDDEN_BLOCK), F32),
            pltpu.VMEM((width // WIDE, 8, WIDE), F32),
            pltpu.VMEM((2, 2, HALF, 1024), BF),
            pltpu.VMEM((2, 2, HALF, 1024), BF),
            pltpu.VMEM((SENT_RING, HALF, 1024), BF),
            pltpu.VMEM((keep_ring,) + narrow, BF),
            pltpu.VMEM((LAND_RING, HALF, 1024), BF),
        ]
        + [pltpu.VMEM((LAND_RING,) + (2,) * p + (rows, 1024), BF) for p in range(count)]
        + [
            pltpu.VMEM((2 * groups, chunk, width), BF),
            pltpu.VMEM((2 * groups, chunk, width), BF),
            pltpu.VMEM((2,) + vectors, F32),
            pltpu.VMEM((count + 2,) + vectors, F32),
            pltpu.VMEM((count + 2,) + vectors, F32),
            dma((PIECES,)), dma((PIECES,)), dma((PIECES,)), dma((PIECES,)),
            dma((count, PIECES)), dma((count, PIECES)), dma((count, PIECES)), dma((count, PIECES)),
            dma((2,)), dma((2,)), dma((PIECES,)), dma((count + 2,)), dma((count + 2,)),
            dma((2 * groups,)), dma((2 * groups,)), dma((groups,)), dma((groups,)),
            dma((3,)), dma, dma((6,)), dma((UNITS,)), dma((UNITS,)),
        ],
        compiler_params=pltpu.CompilerParams(
            collective_id=1, has_side_effects=True, vmem_limit_bytes=VMEM_LIMIT
        ),
        name="backward",
    )(length, inverse, gains, *lower, *upper, *weights, *results)
    total, small_total, _, dealt, acts = result[:5]
    return total.reshape(3, UNITS, HALF, 1024), small_total, dealt.reshape(2, slots, width), acts


from jax.sharding import PartitionSpec as P

VECTORS = (1, 1, 1, 1, 1, 4, 1, 1, 1)


def unpack_kernel(core, narrow, first, second, *outs):
    for at in range(4):
        outs[at][0] = narrow[0, at].astype(F32)
        outs[4][0, :, pl.ds(1024 * at, 1024)] = first[0, at].astype(F32)
        outs[5][0, at] = second[0, at].astype(F32)


def unpack(core, total):
    def band(kind):
        return pl.BlockSpec(
            (1, 4, 128, 1024),
            lambda h, b, core: (jnp.where(h == core[0], 1 - core[0], 2), kind, b, 0),
        )

    square = pl.BlockSpec((1, 128, 1024), lambda h, b, core: (0, 2 * h + b, 0))
    result = pl.pallas_call(
        unpack_kernel,
        grid_spec=pltpu.PrefetchScalarGridSpec(
            num_scalar_prefetch=1,
            grid=(2, 2),
            in_specs=[band(2), band(0), band(1)],
            out_specs=[square] * 4
            + [
                pl.BlockSpec((1, 128, 4096), lambda h, b, core: (0, 2 * h + b, 0)),
                pl.BlockSpec((1, 4, 128, 1024), lambda h, b, core: (0, 0, 2 * h + b, 0)),
            ],
        ),
        out_shape=[struct((1, 512, 1024), F32)] * 4
        + [struct((1, 512, 4096), F32), struct((1, 4, 512, 1024), F32)],
        compiler_params=pltpu.CompilerParams(vmem_limit_bytes=VMEM_LIMIT),
        name="unpack",
    )(core.reshape(1), total, total, total)
    return (*result[:5], result[5].reshape(1, 2048, 1024))


def on_device(
    inputs, cotangent, lengths, permutation, query_weight, query_bias, key_weight, value_weight,
    value_bias, output_weight, output_bias, first_gain, first_bias, inner_weight, inner_bias,
    outer_weight, outer_bias, second_gain, second_bias,
):
    core = lax.axis_index("section")
    group = lax.axis_index(GROUP)
    count = lax.axis_size("replica").bit_length() - 1
    shards = [
        w[0] for w in (query_weight, key_weight, value_weight, output_weight, inner_weight, outer_weight)
    ]
    vectors = [
        v[0] for v in (query_bias, value_bias, output_bias, first_gain, first_bias, inner_bias,
                       outer_bias, second_gain, second_bias)
    ]
    everyone = jnp.arange(permutation.shape[0], dtype=jnp.int32)
    own = lax.dynamic_slice_in_dim(permutation, 2 * group + core, 1)
    length = jnp.sum(jnp.where(everyone == own, lengths, 0), keepdims=True)
    inverse = jnp.sum(
        jnp.where(permutation[None, :] == everyone[:, None], everyone[None, :], 0), axis=1
    )
    short = jnp.concatenate(vectors).astype(F32).reshape(UNITS, -1)
    short = jnp.pad(short, ((0, 16 - UNITS), (0, 0)))
    result = forward(length, permutation, short, shards, inputs, count)
    weights, gains, x, low, up = result[:6], result[6], result[7], result[8:20], result[20:32]
    grad = lax.dynamic_index_in_dim(cotangent, core, 0, keepdims=False)
    lower, upper = low[11], up[11]

    def kept(stored, rows):
        q, k, v, log, context, unit1, scale1, act, slope, unit2, scale2 = stored[:11]
        return (unit2, scale2, unit1, scale1, act, slope, rows, q, k, v, log, context)

    total, small, activations, input_grads = backward(
        length, inverse, gains, kept(low, x), kept(up, lower) + (grad,), weights, (lower, upper),
        count,
    )
    side = lax.axis_index("shard")
    pieces, at = [], 0
    for width in VECTORS:
        whole_vector = small[at : at + width].reshape(2, -1)
        pieces.append(lax.dynamic_slice_in_dim(whole_vector, side, 1, axis=0))
        at += width
    dq, dk, dv, do, d1, d2 = unpack(core, total)
    return (
        activations[None], input_grads[None], dq, pieces[0], dk, dv, pieces[1], do, pieces[2],
        pieces[3], pieces[4], d1, pieces[5], d2, pieces[6], pieces[7], pieces[8],
    )


def solution(mesh):
    matrix, vector = P("section", "shard", None), P("section", "shard")
    rows = P(("shard", "replica"), None, None)
    in_specs = (
        rows, rows, P(), P(), matrix, vector, matrix, matrix, vector, matrix, vector, vector,
        vector, matrix, vector, matrix, vector, vector, vector,
    )
    both = P("section", ("shard", "replica"), None, None)
    out_specs = (
        both, both, matrix, vector, matrix, matrix, vector, matrix, vector, vector, vector,
        matrix, vector, matrix, vector, vector, vector,
    )
    return jax.shard_map(
        on_device, mesh=mesh, in_specs=in_specs, out_specs=out_specs, check_vma=False
    )
```

```python
import jax
import jax.numpy as jnp
from jax import lax
from jax.experimental import pallas as pl
from jax.experimental.pallas import tpu as pltpu

ALL = ("section", "shard", "replica")
GROUP = ("shard", "replica")
UNITS = 12
HALF = 256
VMEM_LIMIT = 64000000


def my_bits(count):
    replica = lax.axis_index("replica")
    return tuple((lax.rem(replica // (1 << (count - 1 - p)), 2) for p in range(count)))


def across(p, count, bits):
    replica = lax.axis_index("replica")
    weight = 1 << (count - 1 - p)
    return {"replica": replica + weight * (1 - 2 * bits[p])}


def place(device, replicas):
    groups = 2 * replicas
    return {
        "section": device // groups,
        "shard": lax.rem(device, groups) // replicas,
        "replica": lax.rem(device, replicas),
    }


def greet_all(me, devices, replicas):
    barrier = pltpu.get_barrier_semaphore()

    def hello(step, carry):
        pl.semaphore_signal(
            barrier, inc=1, device_id=place(lax.rem(me + step, devices), replicas),
            device_id_type=pl.DeviceIdType.MESH,
        )
        return carry

    lax.fori_loop(1, devices, hello, 0)
    pl.semaphore_wait(barrier, devices - 1)


def remote(src, dst, send_sem, recv_sem, partner):
    return pltpu.make_async_remote_copy(
        src_ref=src,
        dst_ref=dst,
        send_sem=send_sem,
        recv_sem=recv_sem,
        device_id=partner,
        device_id_type=pl.DeviceIdType.MESH,
    )


def device_of(number, groups):
    return lax.rem(number, 2) * groups + number // 2


class Deal:
    def __init__(self, layer, source, target, inverse, buffers):
        (self.spread, self.ordered, self.send1, self.recv1, self.send2, self.recv2) = buffers
        self.layer, self.source, self.target, self.inverse = layer, source, target, inverse
        self.groups = self.spread.shape[0] // 2
        self.replicas = self.groups // 2
        self.chunk = self.spread.shape[1]
        self.core = lax.axis_index("section")
        self.group = lax.axis_index("shard") * self.replicas + lax.axis_index("replica")
        self.me = self.core * self.groups + self.group

    def chip(self, index):
        return {
            "section": self.layer, "shard": index // self.replicas,
            "replica": lax.rem(index, self.replicas),
        }

    def rows_of(self, index):
        return self.source.at[pl.ds(pl.multiple_of(index * self.chunk, self.chunk), self.chunk)]

    def first(self, index):
        return remote(
            self.rows_of(index), self.spread.at[self.me], self.send1.at[index],
            self.recv1.at[self.me], self.chip(index),
        )

    def first_own(self):
        return pltpu.make_async_copy(
            self.rows_of(self.group), self.spread.at[self.me], self.recv1.at[self.me]
        )

    def home(self, index):
        return remote(
            self.ordered.at[pl.ds(2 * index, 2)], self.target.at[:, self.group],
            self.send2.at[index], self.recv2.at[self.group], self.chip(index),
        )

    def home_own(self):
        return pltpu.make_async_copy(
            self.ordered.at[pl.ds(2 * self.group, 2)], self.target.at[:, self.group],
            self.recv2.at[self.group],
        )

    def each_first(self, act):
        def body(step, carry):
            @pl.when(jnp.logical_or(step > 0, self.core != self.layer))
            def _():
                act(self.first(lax.rem(self.group + step, self.groups)))
            return carry

        lax.fori_loop(0, self.groups, body, 0)

    def start(self):
        @pl.when(self.core == self.layer)
        def _():
            self.first_own().start()

        self.each_first(lambda copy: copy.start())

    def second(self):
        @pl.when(self.core == self.layer)
        def _():
            self.first_own().wait()

            def landed(step, carry):
                source = lax.rem(self.me + step, 2 * self.groups)
                here = self.spread.at[source]
                remote(
                    here, here, self.send1.at[lax.rem(source, self.groups)],
                    self.recv1.at[source], place(source, self.replicas),
                ).wait_recv()
                return carry

            lax.fori_loop(1, 2 * self.groups, landed, 0)

            def reorder(slot, carry):
                self.ordered[slot] = self.spread[device_of(self.inverse[slot], self.groups)]
                return carry

            lax.fori_loop(0, 2 * self.groups, reorder, 0)
            self.home_own().start()

            def send(step, carry):
                self.home(lax.rem(self.group + step, self.groups)).start()
                return carry

            lax.fori_loop(1, self.groups, send, 0)

    def last(self):
        self.each_first(lambda copy: copy.wait_send())

        @pl.when(self.core == self.layer)
        def _():
            self.home_own().wait()

            def landed(step, carry):
                source = lax.rem(self.group + step, self.groups)
                here = self.target.at[:, source]
                remote(
                    here, here, self.send2.at[source], self.recv2.at[source], self.chip(source)
                ).wait_recv()
                return carry

            lax.fori_loop(1, self.groups, landed, 0)

            def sent(step, carry):
                self.home(lax.rem(self.group + step, self.groups)).wait_send()
                return carry

            lax.fori_loop(1, self.groups, sent, 0)


def deal_buffers(groups, chunk, width):
    dma = pltpu.SemaphoreType.DMA
    return [
        pltpu.VMEM((2 * groups, chunk, width), jnp.bfloat16),
        pltpu.VMEM((2 * groups, chunk, width), jnp.bfloat16),
        dma((groups,)), dma((2 * groups,)), dma((groups,)), dma((groups,)),
    ]


HEAD_DIM = 64
EPSILON = 1e-12
MASKED = -1000000000.0
HIDDEN_BLOCK = 512
WIDE = 256
BF = jnp.bfloat16
F32 = jnp.float32


def mm(a, b):
    return lax.dot_general(a, b, (((1,), (0,)), ((), ())), preferred_element_type=F32)


def mm_right(a, b):
    return lax.dot_general(a, b, (((1,), (1,)), ((), ())), preferred_element_type=F32)


def mm_left(a, b):
    return lax.dot_general(a, b, (((0,), (0,)), ((), ())), preferred_element_type=F32)


def normalized(values):
    average = jnp.mean(values, axis=-1, keepdims=True)
    centred = values - average
    variance = jnp.mean(centred * centred, axis=-1, keepdims=True)
    scale = lax.rsqrt(variance + EPSILON)
    return centred * scale, scale


def normalize_back(grad, unit, scale, gain):
    gs = grad * gain
    mean_gs = jnp.mean(gs, axis=-1, keepdims=True)
    mean_gn = jnp.mean(gs * unit, axis=-1, keepdims=True)
    return (gs - mean_gs - unit * mean_gn) * scale


def head_lanes(head):
    lane = lax.broadcasted_iota(jnp.int32, (1, WIDE), 1)
    return lane // HEAD_DIM == head


def row_sum(values):
    return jnp.sum(values, axis=0, keepdims=True)


def attend_body(
    step, steps, length, x, vectors, layer, wq, wk, wv, wo, q_out, k_out, v_out, log_out,
    context_out, unit_out, scale_out, total,
):
    slots = x.shape[0]
    rows = x[...]
    lanes_of = pl.ds(pl.multiple_of(step * WIDE, WIDE), WIDE)
    q = (mm(rows, wq[...]) + vectors[layer, 0:1, lanes_of]).astype(BF)
    k = mm(rows, wk[...]).astype(BF)
    v = (mm(rows, wv[...]) + vectors[layer, 1:2, lanes_of]).astype(BF)
    q_out[...] = q
    k_out[...] = k
    v_out[...] = v
    live = lax.broadcasted_iota(jnp.int32, (1, slots), 1) < length[0]
    scaled = (q.astype(F32) * 0.125).astype(BF)
    zero = jnp.zeros_like(scaled)
    context = jnp.zeros((slots, WIDE), F32)
    logs = jnp.zeros((slots, 128), F32)
    column = lax.broadcasted_iota(jnp.int32, (1, 128), 1)
    for head in range(WIDE // HEAD_DIM):
        lanes = head_lanes(head)
        scores = mm_right(jnp.where(lanes, scaled, zero), k)
        scores = jnp.where(live, scores, MASKED)
        highest = jnp.max(scores, axis=-1, keepdims=True)
        exponent = jnp.exp(scores - highest)
        totals = jnp.sum(exponent, axis=-1, keepdims=True)
        probs = (exponent * (1.0 / totals)).astype(BF)
        context = jnp.where(lanes, mm(probs, v), context)
        logs = jnp.where(column == head, highest + jnp.log(totals), logs)
    log_out[...] = jnp.transpose(logs)[:8]
    low = context.astype(BF)
    context_out[...] = low

    @pl.when(step == 0)
    def _():
        total[...] = rows.astype(F32) + vectors[layer, 2:3]

    total[...] += mm(low, wo[...])

    @pl.when(step == steps - 1)
    def _():
        unit, scale = normalized(total[...])
        unit_out[...] = unit
        scale_out[...] = jnp.broadcast_to(scale, scale_out.shape)


def feed_body(
    step, steps, length, vectors, halves, layer, unit1, w1, w2, act_out, slope_out, unit_out,
    scale_out, result_out, low, total,
):
    @pl.when(step == 0)
    def _():
        middle = unit1[...] * vectors[layer, 3:4] + vectors[layer, 4:5]
        low[...] = middle.astype(BF)
        total[...] = middle + vectors[layer, 9:10]

    per = steps // 2
    bias = halves[layer, step // per, pl.ds(5 + lax.rem(step, per), 1)]
    inner = mm(low[...], w1[...]) + bias
    cdf = 0.5 * (1.0 + lax.erf(inner * 0.7071067811865476))
    act = (inner * cdf).astype(BF)
    act_out[...] = act
    slope_out[...] = (cdf + inner * (jnp.exp(-0.5 * inner * inner) * 0.3989422804014327)).astype(BF)
    total[...] += mm(act, w2[...])

    @pl.when(step == steps - 1)
    def _():
        unit, scale = normalized(total[...])
        unit_out[...] = unit
        scale_out[...] = jnp.broadcast_to(scale, scale_out.shape)
        live = lax.broadcasted_iota(jnp.int32, (unit.shape[0], 1), 0) < length[0]
        result = unit * vectors[layer, 10:11] + vectors[layer, 11:12]
        result_out[...] = jnp.where(live, result, 0.0).astype(BF)


def feed_back_body(
    step, steps, length, grad, unit2, scale2, g2, unit1, scale1, g1, b1, act, slope, w1, w2,
    d1_out, d2_out, first_out, vectors_out, inner_rows, second, outer, low, total,
):
    @pl.when(step == 0)
    def _():
        live = lax.broadcasted_iota(jnp.int32, (grad.shape[0], 1), 0) < length[0]
        g = jnp.where(live, grad[...].astype(F32), 0.0)
        unit = unit2[...]
        d_second = normalize_back(g, unit, scale2[:, :1], g2[...])
        second[...] = d_second
        d_outer = d_second.astype(BF)
        outer[...] = d_outer
        vectors_out[0:1] = row_sum(d_outer.astype(F32))
        vectors_out[1:2] = row_sum(g * unit)
        vectors_out[2:3] = row_sum(g)
        low[...] = (unit1[...] * g1[...] + b1[...]).astype(BF)
        total[...] = jnp.zeros_like(total)

    d_outer = outer[...]
    d_inner = (mm_right(d_outer, w2[...]) * slope[...].astype(F32)).astype(BF)
    inner_rows[step, 0:1] = row_sum(d_inner.astype(F32))
    total[...] += mm_right(d_inner, w1[...])
    d2_out[...] = mm_left(act[...], d_outer).astype(BF).reshape(d2_out.shape)
    d1 = mm_left(low[...], d_inner).astype(BF)
    half = d1.shape[0] // 2
    d1_out[0, 0] = d1[:half]
    d1_out[1, 0] = d1[half:]

    @pl.when(step == steps - 1)
    def _():
        d_middle = second[...] + total[...]
        unit = unit1[...]
        d_first = normalize_back(d_middle, unit, scale1[:, :1], g1[...])
        first_out[...] = d_first
        vectors_out[3:4] = row_sum(d_middle * unit)
        vectors_out[4:5] = row_sum(d_middle)
        vectors_out[5:6] = row_sum(d_first.astype(BF).astype(F32))


def attend_back_body(
    step, steps, length, first, x, q, k, v, log, context, wq, wk, wv, wo, dqkv_out, do_out, x_out,
    sums_out, attended, total,
):
    slots = x.shape[0]

    @pl.when(step == 0)
    def _():
        attended[...] = first[...].astype(BF)
        total[...] = first[...]

    d_att = attended[...]
    d_context = mm_right(d_att, wo[...]).astype(BF)
    queries = q[...]
    keys = k[...]
    values = v[...]
    scaled = (queries.astype(F32) * 0.125).astype(BF)
    zero = jnp.zeros_like(scaled)
    live = lax.broadcasted_iota(jnp.int32, (slots, 1), 0) < length[0]
    d_q = jnp.zeros((slots, WIDE), F32)
    d_k = jnp.zeros((slots, WIDE), F32)
    d_v = jnp.zeros((slots, WIDE), F32)
    for head in range(WIDE // HEAD_DIM):
        lanes = head_lanes(head)
        scores = mm_right(keys, jnp.where(lanes, scaled, zero))
        scores = jnp.where(live, scores, MASKED)
        probs = jnp.exp(scores - log[head : head + 1])
        d_v = jnp.where(lanes, mm(probs.astype(BF), d_context), d_v)
        d_probs = mm_right(values, jnp.where(lanes, d_context, zero))
        dots = row_sum(probs * d_probs)
        d_scores = (probs * (d_probs - dots)).astype(BF)
        d_k = jnp.where(lanes, mm(d_scores, queries), d_k)
        d_q = jnp.where(lanes, mm_left(d_scores, keys), d_q)
    d_q = (d_q * 0.125).astype(BF)
    d_k = (d_k * 0.125).astype(BF)
    d_v = d_v.astype(BF)
    sums_out[step, 0:1] = row_sum(d_q.astype(F32))
    sums_out[step, 1:2] = row_sum(d_v.astype(F32))
    total[...] += mm_right(d_q, wq[...]) + mm_right(d_k, wk[...]) + mm_right(d_v, wv[...])
    rows = x[...]
    for at, value in enumerate((d_q, d_k, d_v)):
        weight = mm_left(rows, value).astype(BF)
        half = weight.shape[0] // 2
        dqkv_out[0, at] = weight[:half]
        dqkv_out[1, at] = weight[half:]
    do_out[...] = mm_left(context[...], d_att).astype(BF).reshape(do_out.shape)

    @pl.when(step == steps - 1)
    def _():
        x_out[...] = total[...].astype(BF)


def struct(shape, dtype):
    return jax.ShapeDtypeStruct(shape, dtype)


UNIT_ORDER = (0, 1, 2, 3, 4, 8, 9, 5, 10, 11, 6, 7)
DIRECT_SETS = ((0, 1, 6, 7), (0, 1, 6, 7))
HOPS = (0.0, 10.0, 20.0, 34.0, 36.0, 40.0, 44.0)
PACE = 7.0
CROSS = 17.0
OUT_STEP = 1


class Plan:
    def __init__(self):
        self.entries = []
        self.done = set()

    def add(self, when, key, action):
        self.entries.append((when, len(self.entries), key, action))

    def sort(self):
        self.entries.sort(key=lambda entry: entry[:2])

    def run_first(self):
        _, _, key, action = self.entries.pop(0)
        action()
        self.done.add(key)

    def until(self, when):
        while self.entries and self.entries[0][0] <= when:
            self.run_first()

    def pending(self, when):
        return bool(self.entries) and self.entries[0][0] <= when

    def missing(self, keys):
        return any(key not in self.done for key in keys)

    def require(self, keys):
        while self.missing(keys):
            self.run_first()


def front_kernel(count, length, permutation, inverse, small, shards, inputs, outs, scratch):
    full, (rows_out, dealt), stored = outs[:6], outs[6:8], (outs[8:20], outs[20:32])
    deal = Deal(0, outs[19], outs[32], inverse, scratch[:6])
    scratch = scratch[6:]
    (stage, spread, ordered, halves, rows, xs, unit1, scale1, unit2, scale2, low, total,
     send_sem, recv_sem, load_sem, store_sem, deal_send, deal_recv, home_send, home_recv,
     small_send, small_recv, keep_sem) = scratch
    core = lax.axis_index("section")
    side = lax.axis_index("shard")
    bits = my_bits(count)
    sibling = {"section": 1 - core}
    facing = {"shard": 1 - side}
    corner = {"section": 1 - core, "shard": 1 - side}
    replicas = 1 << count
    groups = 2 * replicas
    devices = 2 * groups
    group = side * replicas + lax.axis_index("replica")
    me = core * groups + group
    chunk, columns = spread.shape[1:]
    strip = HALF // replicas
    position = sum(bits[p] * (1 << p) for p in range(count))
    greet_all(me, devices, replicas)

    def chip(index):
        return {"shard": index // replicas, "replica": lax.rem(index, replicas)}

    def piece(index):
        where = pl.ds(pl.multiple_of(index * chunk, chunk), chunk)
        return inputs.at[:, where, pl.ds(pl.multiple_of(core * columns, columns), columns)]

    def spread_copy(target):
        return remote(
            piece(target), spread.at[pl.ds(2 * group, 2)], deal_send.at[target],
            deal_recv.at[group], chip(target),
        )

    spread_own = pltpu.make_async_copy(
        piece(group), spread.at[pl.ds(2 * group, 2)], deal_recv.at[group]
    )

    def spread_start(step, carry):
        spread_copy(lax.rem(group + step, groups)).start()
        return carry

    def spread_wait(step, carry):
        source = lax.rem(group + step, groups)
        landed = spread.at[pl.ds(2 * source, 2)]
        remote(
            landed, landed, deal_send.at[source], deal_recv.at[source], chip(source)
        ).wait_recv()
        return carry

    def spot(device):
        where = pl.ds(pl.multiple_of(lax.rem(device, groups) * chunk, chunk), chunk)
        start = pl.multiple_of((device // groups) * columns, columns)
        return xs.at[where, pl.ds(start, columns)]

    def slot_of(device):
        return 2 * lax.rem(device, groups) + device // groups

    def home_copy(target):
        return remote(
            ordered.at[slot_of(target)], spot(me), home_send.at[target], home_recv.at[me],
            place(target, replicas),
        )

    home_own = pltpu.make_async_copy(ordered.at[slot_of(me)], spot(me), home_recv.at[me])

    def home_start(step, carry):
        home_copy(lax.rem(me + step, devices)).start()
        return carry

    def home_wait(step, carry):
        source = lax.rem(me + step, devices)
        remote(
            spot(source), spot(source), home_send.at[source], home_recv.at[source],
            place(source, replicas),
        ).wait_recv()
        return carry

    def spread_done(step, carry):
        spread_copy(lax.rem(group + step, groups)).wait_send()
        return carry

    def home_done(step, carry):
        home_copy(lax.rem(me + step, devices)).wait_send()
        return carry

    def reorder(slot, carry):
        ordered[slot] = spread[permutation[slot]]
        return carry

    def deal_second():
        spread_own.wait()
        lax.fori_loop(1, groups, spread_wait, 0)
        lax.fori_loop(0, devices, reorder, 0)
        home_own.start()
        lax.fori_loop(1, devices, home_start, 0)

    def deal_last():
        home_own.wait()
        lax.fori_loop(1, devices, home_wait, 0)

    def small_copy(index, partner):
        return remote(
            small, halves.at[core, side], small_send.at[index], small_recv.at[index], partner
        )

    small_own = pltpu.make_async_copy(small, halves.at[core, side], small_send.at[3])

    def vectors_here():
        small_own.wait()
        for index, layer, half, partner in (
            (0, 1 - core, side, sibling), (1, core, 1 - side, facing),
            (2, 1 - core, 1 - side, corner),
        ):
            landed = halves.at[layer, half]
            remote(
                landed, landed, small_send.at[index], small_recv.at[index], partner
            ).wait_recv()
        for layer in range(2):
            for half in range(2):
                rows[layer, :, pl.ds(512 * half, 512)] = halves[layer, half]

    def shard_at(unit, start, size):
        where = pl.ds(start, size)
        if unit < 4:
            return shards[unit].at[where]
        if unit < 8:
            return shards[4].at[where, pl.ds(1024 * (unit - 4), 1024)]
        return shards[5].at[pl.ds(512 * (unit - 8) + start, size)]

    def out_at(layer, unit, half, start, size):
        base = 512 * half + start if unit < 8 else 2048 * half + 512 * (unit - 8) + start
        where = pl.ds(pl.multiple_of(base, strip), size)
        if unit < 4:
            return full[unit].at[layer, where]
        if unit < 8:
            return full[4].at[layer, where, pl.ds(1024 * (unit - 4), 1024)]
        return full[5].at[layer, where]

    mine = HALF * core

    def wire(layer, unit, hop, src, dst, partner):
        index = UNITS * layer + unit
        return remote(src, dst, send_sem.at[index, hop], recv_sem.at[index, hop], partner)

    def arrive(layer, unit, hop, landed, partner):
        wire(layer, unit, hop, landed, landed, partner).wait_recv()

    def cross_rows(layer, unit):
        if unit in DIRECT_SETS[layer]:
            return mine, HALF
        return pl.multiple_of(mine + position * strip, strip), strip

    def cross(layer, unit):
        start, size = cross_rows(layer, unit)
        target = out_at(layer, unit, side, start, size)

        @pl.when(core == layer)
        def _():
            wire(layer, unit, 0, shard_at(unit, start, size), target, facing).start()

        @pl.when(core != layer)
        def _():
            arrive(layer, unit, count + 2, out_at(layer, unit, side, 0, 512), sibling)
            wire(layer, unit, 0, target, target, facing).start()

    def block(k):
        return pl.multiple_of(mine + ((position >> k) << k) * strip, strip), strip << k

    def other_block(k):
        start = ((position >> k) ^ 1) << k
        return pl.multiple_of(mine + start * strip, strip), strip << k

    def hop(layer, unit, k):
        there = 1 - side
        if k == 0:
            arrive(layer, unit, 0, out_at(layer, unit, there, *cross_rows(layer, unit)), facing)
        else:
            arrive(
                layer, unit, k, out_at(layer, unit, there, *other_block(k - 1)),
                across(k - 1, count, bits),
            )
        if k < count and unit not in DIRECT_SETS[layer]:
            held = out_at(layer, unit, there, *block(k))
            wire(layer, unit, k + 1, held, held, across(k, count, bits)).start()
        else:
            held = out_at(layer, unit, there, mine, HALF)
            wire(layer, unit, count + 1, held, held, sibling).start()

    def passed(layer, unit):
        landed = out_at(layer, unit, 1 - side, HALF * (1 - core), HALF)
        arrive(layer, unit, count + 1, landed, sibling)

        @pl.when(core == layer)
        def _():
            store(layer, unit).wait()

    def store(layer, unit):
        return pltpu.make_async_copy(
            stage.at[unit], out_at(layer, unit, side, 0, 512), store_sem.at[unit]
        )

    def load(unit):
        return pltpu.make_async_copy(shard_at(unit, 0, 512), stage.at[unit], load_sem.at[unit])

    def own_start(layer):
        for unit in UNIT_ORDER:
            source = shard_at(unit, 0, 512)
            wire(
                layer, unit, count + 2, source, out_at(layer, unit, side, 0, 512), sibling
            ).start()
            load(unit).start()

    def own_store(layer):
        for unit in UNIT_ORDER:
            load(unit).wait()
            store(layer, unit).start()

    plan = Plan()
    number = [0, 0]
    for layer in range(2):
        for unit in UNIT_ORDER:
            key = (layer, unit)
            if unit in DIRECT_SETS[layer]:
                landing = 14.0 + CROSS * (number[0] + 1)
                number[0] += 1
                plan.add(landing - 1.7 * CROSS, ("cross",) + key, lambda l=layer, u=unit: cross(l, u))
                plan.add(landing, ("hop",) + key, lambda l=layer, u=unit: hop(l, u, 0))
                plan.add(landing + 3.0, ("unit",) + key, lambda l=layer, u=unit: passed(l, u))
            else:
                begin = 6.0 + PACE * number[1]
                number[1] += 1
                plan.add(begin - 60.0, ("cross",) + key, lambda l=layer, u=unit: cross(l, u))
                for k in range(count + 1):
                    plan.add(
                        begin + HOPS[k], ("hop", k) + key, lambda l=layer, u=unit, k=k: hop(l, u, k)
                    )
                plan.add(
                    begin + HOPS[count] + 3.0, ("unit",) + key,
                    lambda l=layer, u=unit: passed(l, u),
                )
    plan.add(30.0, "deal", deal_second)
    plan.add(50.0, "inputs", deal_last)
    plan.add(10.0, "vectors", vectors_here)
    plan.sort()

    spread_own.start()
    lax.fori_loop(1, groups, spread_start, 0)
    for index, partner in enumerate((sibling, facing, corner)):
        small_copy(index, partner).start()
    small_own.start()
    for layer in range(2):
        @pl.when(core == layer)
        def _():
            own_start(layer)
    plan.until(1.0)
    for layer in range(2):
        @pl.when(core == layer)
        def _():
            own_store(layer)

    slots, width = xs.shape
    attention_steps = width // WIDE
    hidden = full[4].shape[-1]
    hidden_steps = hidden // HIDDEN_BLOCK
    band = pl.BlockSpec((slots, WIDE), lambda j: (0, j))
    wide = pl.BlockSpec((width, WIDE), lambda j: (0, j))
    hidden_band = pl.BlockSpec((slots, HIDDEN_BLOCK), lambda j: (0, j))

    def during(step, steps, begin, each, needs):
        for at in range(steps):
            when = begin + each * at
            wanted = needs(at)
            if plan.pending(when) or plan.missing(wanted):
                @pl.when(step == at)
                def _():
                    plan.require(wanted)
                    plan.until(when)

    def attend_stage(layer, begin):
        (q, k, v, log, context) = stored[layer][:5]

        def body(*refs):
            step = pl.program_id(0)
            attend_body(step, attention_steps, length, xs, rows, layer, *refs, unit1, scale1, total)
            during(step, attention_steps, begin, 5.0, lambda at: [])

        pltpu.emit_pipeline(
            body,
            grid=(attention_steps,),
            in_specs=[wide, wide, wide, pl.BlockSpec((WIDE, width), lambda j: (j, 0))],
            out_specs=[
                band, band, band, pl.BlockSpec((None, 8, slots), lambda j: (j, 0, 0)), band
            ],
        )(*(full[i].at[layer] for i in range(4)), q, k, v, log, context)

    def feed_needs(layer, step):
        return [
            ("unit", layer, unit)
            for at in range(min(step + 1, hidden_steps))
            for unit in (4 + at * HIDDEN_BLOCK // 1024, 8 + at % 4)
        ]

    def feed_stage(layer, begin):
        act, slope = stored[layer][7:9]

        def body(*refs):
            step = pl.program_id(0)
            feed_body(
                step, hidden_steps, length, rows, halves, layer, unit1, *refs, unit2, scale2, xs,
                low, total,
            )
            during(step, hidden_steps, begin, 2.5, lambda at: feed_needs(layer, at + 2))
            if layer == 1:
                pl.when(step == OUT_STEP)(deal.second)

        pltpu.emit_pipeline(
            body,
            grid=(hidden_steps,),
            in_specs=[
                pl.BlockSpec((width, HIDDEN_BLOCK), lambda j: (0, j)),
                pl.BlockSpec((HIDDEN_BLOCK, width), lambda j: (j, 0)),
            ],
            out_specs=[hidden_band, hidden_band],
        )(full[4].at[layer], full[5].at[layer], act, slope)

    def keep(source, target, at):
        copy = pltpu.make_async_copy(source, target, keep_sem.at[at])
        copy.start()
        return copy

    begin = (75.0, 125.0)
    keeping = []
    for layer in range(2):
        plan.require(["vectors", "inputs"] + [("unit", layer, unit) for unit in range(4)])
        if layer == 0:
            keeping += [keep(xs, dealt, 0), keep(rows, rows_out, 1)]
        attend_stage(layer, begin[layer])
        for copy in keeping:
            copy.wait()
        keeping = [keep(unit1, stored[layer][5], 2), keep(scale1, stored[layer][6], 3)]
        plan.require(feed_needs(layer, 1))
        feed_stage(layer, begin[layer] + 22.0)
        for copy in keeping:
            copy.wait()
        keeping = [
            keep(unit2, stored[layer][9], 4), keep(scale2, stored[layer][10], 5),
            keep(xs, stored[layer][11], 6),
        ]
        if layer == 0:
            keeping.pop().wait()
            deal.start()
    plan.until(1000000.0)
    for copy in keeping:
        copy.wait()
    deal.last()
    lax.fori_loop(1, groups, spread_done, 0)
    lax.fori_loop(1, devices, home_done, 0)
    for index, partner in enumerate((sibling, facing, corner)):
        small_copy(index, partner).wait_send()
    for layer in range(2):
        for unit in range(UNITS):
            start, size = cross_rows(layer, unit)
            crossed = out_at(layer, unit, side, start, size)
            wire(layer, unit, 0, crossed, crossed, facing).wait_send()
            if unit not in DIRECT_SETS[layer]:
                for k in range(count):
                    held = out_at(layer, unit, 1 - side, *block(k))
                    wire(layer, unit, k + 1, held, held, across(k, count, bits)).wait_send()
            held = out_at(layer, unit, 1 - side, mine, HALF)
            wire(layer, unit, count + 1, held, held, sibling).wait_send()

        @pl.when(core == layer)
        def _():
            for unit in range(UNITS):
                own = out_at(layer, unit, side, 0, 512)
                wire(layer, unit, count + 2, own, own, sibling).wait_send()


def forward(length, permutation, inverse, small, shards, inputs, count):
    groups = 2 << count
    slots, width = inputs.shape[1:]
    hidden = shards[4].shape[-1]
    part = (2 * groups, slots // groups, width // 2)
    dma = pltpu.SemaphoreType.DMA
    square = (slots, width)
    steps = width // WIDE
    layer = [
        struct(square, BF), struct(square, BF), struct(square, BF), struct((steps, 8, slots), F32),
        struct(square, BF), struct(square, F32), struct((slots, 128), F32),
        struct((slots, hidden), BF), struct((slots, hidden), BF), struct(square, F32),
        struct((slots, 128), F32), struct(square, BF),
    ]
    out_shape = (
        [struct((2, width, width), BF)] * 4
        + [struct((2, width, hidden), BF), struct((2, hidden, width), BF)]
        + [struct((2,) + small.shape[:1] + (width,), F32), struct(square, BF)]
        + layer + layer + [struct((2, groups, slots // groups, width), BF)]
    )
    smem = pl.BlockSpec(memory_space=pltpu.SMEM)
    anywhere = pl.BlockSpec(memory_space=pl.ANY)

    def kernel(*refs):
        front_kernel(
            count, *refs[:4], refs[4:10], refs[10], refs[11 : 11 + len(out_shape)],
            refs[11 + len(out_shape) :],
        )

    return pl.pallas_call(
        kernel,
        out_shape=out_shape,
        in_specs=[smem] * 3 + [anywhere] * 8,
        out_specs=[anywhere] * len(out_shape),
        scratch_shapes=deal_buffers(groups, slots // groups, width)
        + [
            pltpu.VMEM((UNITS, 512, 1024), BF), pltpu.VMEM(part, BF), pltpu.VMEM(part, BF),
            pltpu.VMEM((2, 2) + small.shape, F32),
            pltpu.VMEM((2,) + small.shape[:1] + (width,), F32),
            pltpu.VMEM(square, BF), pltpu.VMEM(square, F32), pltpu.VMEM((slots, 128), F32),
            pltpu.VMEM(square, F32), pltpu.VMEM((slots, 128), F32),
            pltpu.VMEM(square, BF), pltpu.VMEM(square, F32),
            dma((2 * UNITS, count + 3)), dma((2 * UNITS, count + 3)), dma((UNITS,)), dma((UNITS,)),
            dma((groups,)), dma((groups,)), dma((2 * groups,)), dma((2 * groups,)),
            dma((4,)), dma((3,)), dma((7,)),
        ],
        compiler_params=pltpu.CompilerParams(
            collective_id=0, has_side_effects=True, vmem_limit_bytes=VMEM_LIMIT
        ),
        name="forward",
    )(length, permutation, inverse, small, *shards, inputs)


SENT_RING = 4
LAND_RING = 5
PIECES = 2 * UNITS
DEAL_STEP = 5
EARLY = ((0, 1, 2, 3), (1, 3, 5, 7), (0, 1, 2, 3), (6,))
AHEAD = sum(len(steps) for steps in EARLY)


def back_kernel(count, length, inverse, gains, lower, upper, weights, result, outs, scratch):
    (total, small_total, landing, _, acts, d1_low, d2_low, dqkv_low, do_low, up_d1, up_d2,
     dqkv_up, do_up, grad_low, grad_up) = outs
    (xs, first, gradient, unit1, unit2, scale1, scale2, second, outer, middle, running, attended,
     vectors, inner_rows, sums) = scratch[:15]
    (own, came, across_half, kept, from_x), rest = scratch[15:20], scratch[20:]
    halves, rest = rest[:count], rest[count:]
    deal = Deal(1, result, outs[3], inverse, rest[:6])
    (smalls, small_own, small_recv, send0, recv0, send_x, recv_x, send_rs, recv_rs,
     send_ag, recv_ag, load_sem, came_sem, piece_sem, small_send, small_arrive,
     act_sem, total_sem, fetch_sem, done_send, done_recv) = rest[6:]
    wq, wk, wv, wo, w1, w2 = weights
    (up_unit2, up_scale2, up_unit1, up_scale1, up_act, up_slope, up_x, up_q, up_k, up_v, up_log,
     up_context, cotangent) = upper
    (low_unit2, low_scale2, low_unit1, low_scale1, low_act, low_slope, low_x, low_q, low_k, low_v,
     low_log, low_context) = lower
    core = lax.axis_index("section")
    side = lax.axis_index("shard")
    replica = lax.axis_index("replica")
    bits = my_bits(count)
    sibling = {"section": 1 - core}
    facing = {"shard": 1 - side}
    everything = (slice(None),) * count
    rows = kept.shape[-2]
    keep_ring = kept.shape[0]
    replicas = 1 << count
    groups = 2 * replicas
    group = side * replicas + replica
    me = core * groups + group
    greet_all(me, 2 * groups, replicas)

    layers = ((up_d1, up_d2, dqkv_up, do_up), (d1_low, d2_low, dqkv_low, do_low))
    ranges, at = [], 0
    for order in range(2):
        for index in range(4):
            depth = layers[order][index].shape[1]
            ranges.append((order, index, at, at + depth))
            at += depth

    def part_of(order, index, unit, half):
        where = pl.ds(pl.multiple_of(HALF * half, HALF), HALF)
        return layers[order][index].at[:, unit, where]

    def core_copy(unit, source=None):
        source = landing.at[unit] if source is None else source
        return remote(source, landing.at[unit], send0.at[unit], recv0.at[unit], sibling)

    def send_core(order, which, only=range(PIECES)):
        for at_order, index, low, high in ranges:
            if at_order == order and index in which:
                for unit in [u for u in range(low, high) if u in only]:
                    core_copy(unit, part_of(order, index, unit - low, 1 - core)).start()

    def own_load(source, slot):
        return pltpu.make_async_copy(source, own.at[slot], load_sem.at[slot])

    def came_load(unit):
        slot = lax.rem(unit, 2)
        return pltpu.make_async_copy(landing.at[unit], came.at[slot], came_sem.at[slot])

    def start_load(unit):
        for order, index, low, high in ranges:
            @pl.when(jnp.logical_and(unit >= low, unit < high))
            def _():
                own_load(part_of(order, index, unit - low, core), lax.rem(unit, 2)).start()

    def x_copy(unit):
        return remote(
            across_half.at[lax.rem(unit, SENT_RING)], from_x.at[lax.rem(unit, LAND_RING)],
            send_x.at[unit], recv_x.at[unit], facing,
        )

    def rs_copy(unit, p):
        slot = lax.rem(unit, keep_ring)
        return remote(
            kept.at[(slot,) + everything[:p] + (1 - bits[p],) + bits[p + 1 :]],
            halves[p].at[lax.rem(unit, LAND_RING)],
            send_rs.at[p, unit],
            recv_rs.at[p, unit],
            across(p, count, bits),
        )

    def ag_copy(unit, p):
        where = (unit,) + everything[:p] + bits[p:]
        source = kept.at[(lax.rem(unit, keep_ring),) + bits] if p == 0 else total.at[where]
        return remote(
            source, total.at[where], send_ag.at[p, unit], recv_ag.at[p, unit],
            across(p, count, bits),
        )

    def ag_arrive(unit, p):
        where = total.at[(unit,) + everything[:p] + (1 - bits[p],) + bits[p + 1 :]]
        remote(
            where, where, send_ag.at[p, unit], recv_ag.at[p, unit], across(p, count, bits)
        ).wait_recv()

    def piece_copy(unit):
        return pltpu.make_async_copy(
            kept.at[(lax.rem(unit, keep_ring),) + bits], total.at[(unit,) + bits],
            piece_sem.at[unit],
        )

    def done_copy(unit):
        index = lax.rem(unit, UNITS)
        return remote(
            total.at[unit], total.at[PIECES + index], done_send.at[index], done_recv.at[index],
            sibling,
        )

    def small_copy(step):
        partner = [sibling, facing] + [across(p, count, bits) for p in range(count)]
        source = smalls.at[1 - core] if step == 0 else small_own.at[step - 1]
        return remote(
            source, small_recv.at[step], small_send.at[step], small_arrive.at[step], partner[step]
        )

    def places_of(index, dims):
        return tuple((lax.rem(index // (1 << (dims - 1 - q)), 2) for q in range(dims)))

    def tick(now):
        @pl.when(jnp.logical_and(now >= SENT_RING, now < PIECES + SENT_RING))
        def _():
            x_copy(now - SENT_RING).wait_send()

        @pl.when(jnp.logical_and(now >= keep_ring, now < PIECES + keep_ring))
        def _():
            for p in range(count):
                rs_copy(now - keep_ring, p).wait_send()
            ag_copy(now - keep_ring, 0).wait_send()

        @pl.when(now < PIECES)
        def _():
            unit = now
            slot = lax.rem(unit, 2)

            @pl.when(unit == 0)
            def _():
                start_load(0)
                core_copy(0).wait_recv()
                came_load(0).start()

            own_load(landing.at[unit], slot).wait()
            came_load(unit).wait()

            @pl.when(unit + 1 < PIECES)
            def _():
                start_load(unit + 1)
                core_copy(unit + 1).wait_recv()
                came_load(unit + 1).start()

            out_slot = lax.rem(unit, SENT_RING)
            kept_slot = lax.rem(unit, keep_ring)

            def add(block, c):
                where = pl.ds(pl.multiple_of(block * 32, 32), 32)
                across_half[out_slot, where] = (
                    own[slot, 1 - side, where] + came[slot, 1 - side, where]
                )
                return c

            lax.fori_loop(0, HALF // 32, add, 0)
            x_copy(unit).start()

            def add_kept(index, c):
                where = pl.ds(pl.multiple_of(index * rows, rows), rows)
                mine = (kept_slot,) + places_of(index, count)
                kept[mine] = own[slot, side, where] + came[slot, side, where]
                return c

            lax.fori_loop(0, 1 << count, add_kept, 0)

        @pl.when(jnp.logical_and(now >= 1, now < PIECES + 1))
        def _():
            unit = now - 1
            slot = lax.rem(unit, keep_ring)
            land = lax.rem(unit, LAND_RING)
            x_copy(unit).wait_recv()

            def add(index, c):
                where = pl.ds(pl.multiple_of(index * rows, rows), rows)
                mine = (slot,) + places_of(index, count)
                kept[mine] = kept[mine] + from_x[land, where]
                return c

            lax.fori_loop(0, 1 << count, add, 0)
            rs_copy(unit, count - 1).start()

        for step in range(count):
            p = count - 1 - step

            @pl.when(jnp.logical_and(now >= 2 + step, now < PIECES + 2 + step))
            def _():
                unit = now - (2 + step)
                slot = lax.rem(unit, keep_ring)
                land = lax.rem(unit, LAND_RING)
                rs_copy(unit, p).wait_recv()

                def add(index, c):
                    mine = (slot,) + places_of(index, p) + bits[p:]
                    kept[mine] = kept[mine] + halves[p][(land,) + places_of(index, p)]
                    return c

                if p == 0:
                    add(0, 0)
                    piece_copy(unit).start()
                    ag_copy(unit, 0).start()
                else:
                    lax.fori_loop(0, 1 << p, add, 0)
                    rs_copy(unit, p - 1).start()

        for p in range(count):
            lag = 2 + count + p

            @pl.when(jnp.logical_and(now >= lag, now < PIECES + lag))
            def _():
                unit = now - lag
                ag_arrive(unit, p)
                if p == 0:
                    piece_copy(unit).wait()
                if p + 1 < count:
                    ag_copy(unit, p + 1).start()
                else:
                    @pl.when((unit < UNITS) == (core == 0))
                    def _():
                        done_copy(unit).start()

    def early(step, phase):
        before = 0 if phase == 3 else len(EARLY[3]) + sum(len(steps) for steps in EARLY[:phase])
        now = -1
        for at, when in enumerate(EARLY[phase]):
            now = jnp.where(step == when, before + at, now)

        @pl.when(now >= 0)
        def _():
            tick(now)

    def fetch(source, target, at):
        copy = pltpu.make_async_copy(source, target, fetch_sem.at[at])
        copy.start()
        return copy

    waits = [
        fetch(cotangent, gradient, 0), fetch(up_unit1, unit1, 2), fetch(up_unit2, unit2, 3),
        fetch(up_scale1, scale1, 4), fetch(up_scale2, scale2, 5),
    ]
    up_rows = fetch(up_x, xs, 1)
    deal.start()
    for copy in waits:
        copy.wait()

    slots, width = xs.shape
    attention_steps = width // WIDE
    hidden_steps = w1.shape[-1] // HIDDEN_BLOCK
    per = 512 // WIDE
    wide_per = 1024 // HIDDEN_BLOCK
    pairs = HIDDEN_BLOCK // 512
    band = pl.BlockSpec((slots, WIDE), lambda j: (0, j))
    columns = pl.BlockSpec((width, WIDE), lambda j: (0, j))

    def attention(layer, phase, q, k, v, log, context, dqkv, do):
        def body(*refs):
            step = pl.program_id(0)
            attend_back_body(
                step, attention_steps, length, first, xs, *refs, gradient, sums, attended, running
            )
            early(step, phase)

        pltpu.emit_pipeline(
            body,
            grid=(attention_steps,),
            in_specs=[
                band, band, band, pl.BlockSpec((None, 8, slots), lambda j: (j, 0, 0)), band,
                columns, columns, columns, pl.BlockSpec((WIDE, width), lambda j: (j, 0)),
            ],
            out_specs=[
                pl.BlockSpec((2, 3, 512, WIDE), lambda j: (0, 0, 0, j)),
                pl.BlockSpec((1, 1, WIDE, width), lambda j: (j // per, 0, j % per, 0)),
            ],
        )(q, k, v, log, context, wq.at[layer], wk.at[layer], wv.at[layer], wo.at[layer], dqkv, do)
        for at in range(attention_steps):
            lanes = pl.ds(WIDE * at, WIDE)
            smalls[layer, 0:1, lanes] = sums[at, 0:1]
            smalls[layer, 1:2, lanes] = sums[at, 1:2]

    def feed_stage(layer, act, slope, d1, d2, begin, steps):
        def body(*refs):
            step = pl.program_id(0) + begin
            feed_back_body(
                step, hidden_steps, length, gradient, unit2, scale2, gains.at[layer, 10:11],
                unit1, scale1, gains.at[layer, 3:4], gains.at[layer, 4:5], *refs, first,
                vectors, inner_rows, second, outer, middle, running,
            )
            if layer == 0:
                early(step, 1)
            elif begin > 0:
                pl.when(step == DEAL_STEP)(deal.second)
                early(step, 3)

        half = hidden_steps // 2
        hidden_band = pl.BlockSpec((slots, HIDDEN_BLOCK), lambda j: (0, j + begin))
        pltpu.emit_pipeline(
            body,
            grid=(steps,),
            in_specs=[
                hidden_band, hidden_band,
                pl.BlockSpec((width, HIDDEN_BLOCK), lambda j: (0, j + begin)),
                pl.BlockSpec((HIDDEN_BLOCK, width), lambda j: (j + begin, 0)),
            ],
            out_specs=[
                pl.BlockSpec(
                    (2, 1, 512, HIDDEN_BLOCK),
                    lambda j: (0, (j + begin) // wide_per, 0, (j + begin) % wide_per),
                ),
                pl.BlockSpec(
                    (1, pairs, 512, width),
                    lambda j: ((j + begin) // half, (j + begin) % half, 0, 0),
                ),
            ],
        )(act, slope, w1.at[layer], w2.at[layer], d1, d2)

    def feed_sums(layer):
        for at, source in ((2, 5), (3, 3), (4, 4), (9, 0), (10, 1), (11, 2)):
            smalls[layer, at : at + 1] = vectors[source : source + 1]
        for at in range(hidden_steps):
            line = 5 + at // wide_per
            lanes = pl.ds(HIDDEN_BLOCK * (at % wide_per), HIDDEN_BLOCK)
            smalls[layer, line : line + 1, lanes] = inner_rows[at, 0:1]

    start_units = UNITS // 6
    feed_stage(1, up_act, up_slope, up_d1, up_d2, 0, hidden_steps // 2)
    send_core(0, (0, 1), range(start_units))
    feed_stage(1, up_act, up_slope, up_d1, up_d2, hidden_steps // 2, hidden_steps // 2)
    feed_sums(1)
    send_core(0, (0, 1), range(start_units, 2 * UNITS))
    later = [
        fetch(low_unit1, unit1, 2), fetch(low_unit2, unit2, 3), fetch(low_scale1, scale1, 4),
        fetch(low_scale2, scale2, 5),
    ]
    up_rows.wait()
    attention(1, 0, up_q, up_k, up_v, up_log, up_context, dqkv_up, do_up)
    send_core(0, (2, 3))
    waits = [fetch(gradient, grad_up, 0), fetch(low_x, xs, 1)]
    for copy in later:
        copy.wait()
    feed_stage(0, low_act, low_slope, d1_low, d2_low, 0, hidden_steps)
    feed_sums(0)
    send_core(1, (0, 1))
    for copy in waits:
        copy.wait()
    attention(0, 2, low_q, low_k, low_v, low_log, low_context, dqkv_low, do_low)
    send_core(1, (2, 3))
    small_copy(0).start()
    held = fetch(gradient, grad_low, 0)
    held.wait()
    small_steps = count + 2
    both = (grad_low, grad_up)

    def exchange(layer):
        return remote(both[1 - layer], acts.at[layer], act_sem.at[0], act_sem.at[1], sibling)

    for layer in range(2):
        @pl.when(core == layer)
        def _():
            exchange(layer).start()
    grad_back = fetch(grad_up, xs, 1)
    grad_back.wait()

    @pl.when(core == 0)
    def _():
        pltpu.make_async_copy(gradient, acts.at[0], act_sem.at[2]).start()

    @pl.when(core == 1)
    def _():
        pltpu.make_async_copy(xs, acts.at[1], act_sem.at[2]).start()

    def late(now, carry):
        for step in range(small_steps):
            @pl.when(now == step + 1)
            def _():
                small_copy(step).wait_recv()
                before = smalls[core] if step == 0 else small_own[step - 1]
                small_own[step] = before + small_recv[step]
                if step + 1 < small_steps:
                    small_copy(step + 1).start()

        tick(now + AHEAD)
        return carry

    lax.fori_loop(0, PIECES + max(keep_ring, 2 + 2 * count) - AHEAD, late, 0)
    out = pltpu.make_async_copy(small_own.at[small_steps - 1], small_total, total_sem)
    out.start()

    def last(unit, carry):
        core_copy(unit).wait_send()
        for p in range(1, count):
            ag_copy(unit, p).wait_send()
        return carry

    lax.fori_loop(0, PIECES, last, 0)

    def swapped(index, carry):
        done_copy(index).wait_send()
        done_copy(index).wait_recv()
        return carry

    lax.fori_loop(0, UNITS, swapped, 0)
    for step in range(small_steps):
        small_copy(step).wait_send()

    deal.last()
    back = remote(both[0], acts.at[1 - core], act_sem.at[0], act_sem.at[1], sibling)
    back.wait_send()
    back.wait_recv()
    pltpu.make_async_copy(xs, acts.at[core], act_sem.at[2]).wait()
    out.wait()


def backward(length, inverse, gains, lower, upper, weights, result, count):
    cut = (2,) * count
    rows = HALF // (1 << count)
    narrow = cut + (rows, 1024)
    dma = pltpu.SemaphoreType.DMA
    groups = 2 << count
    slots, width = result.shape
    chunk = slots // groups
    keep_ring = count + 5
    hidden = weights[4].shape[-1]
    sizes = [len(lower), len(upper), len(weights)]

    def kernel(*refs):
        start, groups_of = 3, []
        for size in sizes:
            groups_of.append(refs[start : start + size])
            start += size
        back_kernel(
            count, *refs[:3], *groups_of, refs[start], refs[start + 1 : start + 16],
            refs[start + 16 :],
        )

    anywhere = pl.BlockSpec(memory_space=pl.ANY)
    vmem = pl.BlockSpec(memory_space=pltpu.VMEM)
    smem = pl.BlockSpec(memory_space=pltpu.SMEM)
    vectors = (UNITS, width)
    square = (slots, width)
    feed_shape, head_shape = (2, 4, 512, 1024), (2, 3, 512, 1024)
    out_shape = [
        struct((PIECES + UNITS,) + narrow, BF),
        struct(vectors, F32),
        struct((PIECES, 2, HALF, 1024), BF),
        struct((2, groups, chunk, width), BF),
        struct((2,) + square, BF),
        struct(feed_shape, BF), struct(feed_shape, BF),
        struct(head_shape, BF), struct((2, 1, 512, 1024), BF),
        struct(feed_shape, BF), struct(feed_shape, BF),
        struct(head_shape, BF), struct((2, 1, 512, 1024), BF),
        struct(square, BF), struct(square, BF),
    ]
    result = pl.pallas_call(
        kernel,
        out_shape=out_shape,
        in_specs=[smem, smem, vmem] + [anywhere] * (sum(sizes) + 1),
        out_specs=[anywhere] * len(out_shape),
        scratch_shapes=[
            pltpu.VMEM(square, BF), pltpu.VMEM(square, F32), pltpu.VMEM(square, BF),
            pltpu.VMEM(square, F32), pltpu.VMEM(square, F32),
            pltpu.VMEM((slots, 128), F32), pltpu.VMEM((slots, 128), F32),
            pltpu.VMEM(square, F32), pltpu.VMEM(square, BF), pltpu.VMEM(square, BF),
            pltpu.VMEM(square, F32), pltpu.VMEM(square, BF),
            pltpu.VMEM((8, width), F32),
            pltpu.VMEM((hidden // HIDDEN_BLOCK, 8, HIDDEN_BLOCK), F32),
            pltpu.VMEM((width // WIDE, 8, WIDE), F32),
            pltpu.VMEM((2, 2, HALF, 1024), BF),
            pltpu.VMEM((2, 2, HALF, 1024), BF),
            pltpu.VMEM((SENT_RING, HALF, 1024), BF),
            pltpu.VMEM((keep_ring,) + narrow, BF),
            pltpu.VMEM((LAND_RING, HALF, 1024), BF),
        ]
        + [pltpu.VMEM((LAND_RING,) + (2,) * p + (rows, 1024), BF) for p in range(count)]
        + deal_buffers(groups, chunk, width)
        + [
            pltpu.VMEM((2,) + vectors, F32),
            pltpu.VMEM((count + 2,) + vectors, F32),
            pltpu.VMEM((count + 2,) + vectors, F32),
            dma((PIECES,)), dma((PIECES,)), dma((PIECES,)), dma((PIECES,)),
            dma((count, PIECES)), dma((count, PIECES)), dma((count, PIECES)), dma((count, PIECES)),
            dma((2,)), dma((2,)), dma((PIECES,)), dma((count + 2,)), dma((count + 2,)),
            dma((3,)), dma, dma((6,)), dma((UNITS,)), dma((UNITS,)),
        ],
        compiler_params=pltpu.CompilerParams(
            collective_id=1, has_side_effects=True, vmem_limit_bytes=VMEM_LIMIT
        ),
        name="backward",
    )(length, inverse, gains, *lower, *upper, *weights, result)
    total, small_total, _, dealt, acts = result[:5]
    return total.reshape(3, UNITS, HALF, 1024), small_total, dealt.reshape(2, slots, width), acts


from jax.sharding import PartitionSpec as P

VECTORS = (1, 1, 1, 1, 1, 4, 1, 1, 1)


def unpack_kernel(core, narrow, first, second, *outs):
    for at in range(4):
        outs[at][0] = narrow[0, at].astype(F32)
        outs[4][0, :, pl.ds(1024 * at, 1024)] = first[0, at].astype(F32)
        outs[5][0, at] = second[0, at].astype(F32)


def unpack(core, total):
    def band(kind):
        return pl.BlockSpec(
            (1, 4, 128, 1024),
            lambda h, b, core: (jnp.where(h == core[0], 1 - core[0], 2), kind, b, 0),
        )

    square = pl.BlockSpec((1, 128, 1024), lambda h, b, core: (0, 2 * h + b, 0))
    result = pl.pallas_call(
        unpack_kernel,
        grid_spec=pltpu.PrefetchScalarGridSpec(
            num_scalar_prefetch=1,
            grid=(2, 2),
            in_specs=[band(2), band(0), band(1)],
            out_specs=[square] * 4
            + [
                pl.BlockSpec((1, 128, 4096), lambda h, b, core: (0, 2 * h + b, 0)),
                pl.BlockSpec((1, 4, 128, 1024), lambda h, b, core: (0, 0, 2 * h + b, 0)),
            ],
        ),
        out_shape=[struct((1, 512, 1024), F32)] * 4
        + [struct((1, 512, 4096), F32), struct((1, 4, 512, 1024), F32)],
        compiler_params=pltpu.CompilerParams(vmem_limit_bytes=VMEM_LIMIT),
        name="unpack",
    )(core.reshape(1), total, total, total)
    return (*result[:5], result[5].reshape(1, 2048, 1024))


def on_device(
    inputs, cotangent, lengths, permutation, query_weight, query_bias, key_weight, value_weight,
    value_bias, output_weight, output_bias, first_gain, first_bias, inner_weight, inner_bias,
    outer_weight, outer_bias, second_gain, second_bias,
):
    core = lax.axis_index("section")
    group = lax.axis_index(GROUP)
    count = lax.axis_size("replica").bit_length() - 1
    shards = [
        w[0] for w in (query_weight, key_weight, value_weight, output_weight, inner_weight, outer_weight)
    ]
    vectors = [
        v[0] for v in (query_bias, value_bias, output_bias, first_gain, first_bias, inner_bias,
                       outer_bias, second_gain, second_bias)
    ]
    everyone = jnp.arange(permutation.shape[0], dtype=jnp.int32)
    own = lax.dynamic_slice_in_dim(permutation, 2 * group + core, 1)
    length = jnp.sum(jnp.where(everyone == own, lengths, 0), keepdims=True)
    inverse = jnp.sum(
        jnp.where(permutation[None, :] == everyone[:, None], everyone[None, :], 0), axis=1
    )
    short = jnp.concatenate(vectors).astype(F32).reshape(UNITS, -1)
    short = jnp.pad(short, ((0, 16 - UNITS), (0, 0)))
    result = forward(length, permutation, inverse, short, shards, inputs, count)
    weights, gains, x, low, up = result[:6], result[6], result[7], result[8:20], result[20:32]
    grad = lax.dynamic_index_in_dim(cotangent, core, 0, keepdims=False)
    lower, upper = low[11], up[11]
    lower_home = result[32].reshape(2, *lower.shape)

    def kept(stored, rows):
        q, k, v, log, context, unit1, scale1, act, slope, unit2, scale2 = stored[:11]
        return (unit2, scale2, unit1, scale1, act, slope, rows, q, k, v, log, context)

    total, small, upper_home, input_grads = backward(
        length, inverse, gains, kept(low, x), kept(up, lower) + (grad,), weights, upper,
        count,
    )
    activations = jnp.where(core == 0, lower_home, upper_home)
    side = lax.axis_index("shard")
    pieces, at = [], 0
    for width in VECTORS:
        whole_vector = small[at : at + width].reshape(2, -1)
        pieces.append(lax.dynamic_slice_in_dim(whole_vector, side, 1, axis=0))
        at += width
    dq, dk, dv, do, d1, d2 = unpack(core, total)
    return (
        activations[None], input_grads[None], dq, pieces[0], dk, dv, pieces[1], do, pieces[2],
        pieces[3], pieces[4], d1, pieces[5], d2, pieces[6], pieces[7], pieces[8],
    )


def solution(mesh):
    matrix, vector = P("section", "shard", None), P("section", "shard")
    rows = P(("shard", "replica"), None, None)
    in_specs = (
        rows, rows, P(), P(), matrix, vector, matrix, matrix, vector, matrix, vector, vector,
        vector, matrix, vector, matrix, vector, vector, vector,
    )
    both = P("section", ("shard", "replica"), None, None)
    out_specs = (
        both, both, matrix, vector, matrix, matrix, vector, matrix, vector, vector, vector,
        matrix, vector, matrix, vector, vector, vector,
    )
    return jax.shard_map(
        on_device, mesh=mesh, in_specs=in_specs, out_specs=out_specs, check_vma=False
    )
```

```python
import jax
import jax.numpy as jnp
from jax import lax
from jax.experimental import pallas as pl
from jax.experimental.pallas import tpu as pltpu

ALL = ("section", "shard", "replica")
GROUP = ("shard", "replica")
UNITS = 12
HALF = 256
VMEM_LIMIT = 64000000


def my_bits(count):
    replica = lax.axis_index("replica")
    return tuple((lax.rem(replica // (1 << (count - 1 - p)), 2) for p in range(count)))


def across(p, count, bits):
    replica = lax.axis_index("replica")
    weight = 1 << (count - 1 - p)
    return {"replica": replica + weight * (1 - 2 * bits[p])}


def place(device, replicas):
    groups = 2 * replicas
    return {
        "section": device // groups,
        "shard": lax.rem(device, groups) // replicas,
        "replica": lax.rem(device, replicas),
    }


def greet_all(me, devices, replicas):
    barrier = pltpu.get_barrier_semaphore()

    def hello(step, carry):
        pl.semaphore_signal(
            barrier, inc=1, device_id=place(lax.rem(me + step, devices), replicas),
            device_id_type=pl.DeviceIdType.MESH,
        )
        return carry

    lax.fori_loop(1, devices, hello, 0)
    pl.semaphore_wait(barrier, devices - 1)


def remote(src, dst, send_sem, recv_sem, partner):
    return pltpu.make_async_remote_copy(
        src_ref=src,
        dst_ref=dst,
        send_sem=send_sem,
        recv_sem=recv_sem,
        device_id=partner,
        device_id_type=pl.DeviceIdType.MESH,
    )


def device_of(number, groups):
    return lax.rem(number, 2) * groups + number // 2


class Deal:
    def __init__(self, layer, source, target, inverse, buffers):
        (self.spread, self.ordered, self.send1, self.recv1, self.send2, self.recv2) = buffers
        self.layer, self.source, self.target, self.inverse = layer, source, target, inverse
        self.groups = self.spread.shape[0] // 2
        self.replicas = self.groups // 2
        self.chunk = self.spread.shape[1]
        self.core = lax.axis_index("section")
        self.group = lax.axis_index("shard") * self.replicas + lax.axis_index("replica")
        self.me = self.core * self.groups + self.group

    def chip(self, index):
        return {
            "section": self.layer, "shard": index // self.replicas,
            "replica": lax.rem(index, self.replicas),
        }

    def rows_of(self, index):
        return self.source.at[pl.ds(pl.multiple_of(index * self.chunk, self.chunk), self.chunk)]

    def first(self, index):
        return remote(
            self.rows_of(index), self.spread.at[self.me], self.send1.at[index],
            self.recv1.at[self.me], self.chip(index),
        )

    def first_own(self):
        return pltpu.make_async_copy(
            self.rows_of(self.group), self.spread.at[self.me], self.recv1.at[self.me]
        )

    def home(self, index):
        return remote(
            self.ordered.at[pl.ds(2 * index, 2)], self.target.at[:, self.group],
            self.send2.at[index], self.recv2.at[self.group], self.chip(index),
        )

    def home_own(self):
        return pltpu.make_async_copy(
            self.ordered.at[pl.ds(2 * self.group, 2)], self.target.at[:, self.group],
            self.recv2.at[self.group],
        )

    def each_first(self, act):
        def body(step, carry):
            @pl.when(jnp.logical_or(step > 0, self.core != self.layer))
            def _():
                act(self.first(lax.rem(self.group + step, self.groups)))
            return carry

        lax.fori_loop(0, self.groups, body, 0)

    def start(self):
        @pl.when(self.core == self.layer)
        def _():
            self.first_own().start()

        self.each_first(lambda copy: copy.start())

    def second(self):
        @pl.when(self.core == self.layer)
        def _():
            self.first_own().wait()

            def landed(step, carry):
                source = lax.rem(self.me + step, 2 * self.groups)
                here = self.spread.at[source]
                remote(
                    here, here, self.send1.at[lax.rem(source, self.groups)],
                    self.recv1.at[source], place(source, self.replicas),
                ).wait_recv()
                return carry

            lax.fori_loop(1, 2 * self.groups, landed, 0)

            def reorder(slot, carry):
                self.ordered[slot] = self.spread[device_of(self.inverse[slot], self.groups)]
                return carry

            lax.fori_loop(0, 2 * self.groups, reorder, 0)
            self.home_own().start()

            def send(step, carry):
                self.home(lax.rem(self.group + step, self.groups)).start()
                return carry

            lax.fori_loop(1, self.groups, send, 0)

    def last(self):
        self.each_first(lambda copy: copy.wait_send())

        @pl.when(self.core == self.layer)
        def _():
            self.home_own().wait()

            def landed(step, carry):
                source = lax.rem(self.group + step, self.groups)
                here = self.target.at[:, source]
                remote(
                    here, here, self.send2.at[source], self.recv2.at[source], self.chip(source)
                ).wait_recv()
                return carry

            lax.fori_loop(1, self.groups, landed, 0)

            def sent(step, carry):
                self.home(lax.rem(self.group + step, self.groups)).wait_send()
                return carry

            lax.fori_loop(1, self.groups, sent, 0)


def deal_buffers(groups, chunk, width):
    dma = pltpu.SemaphoreType.DMA
    return [
        pltpu.VMEM((2 * groups, chunk, width), jnp.bfloat16),
        pltpu.VMEM((2 * groups, chunk, width), jnp.bfloat16),
        dma((groups,)), dma((2 * groups,)), dma((groups,)), dma((groups,)),
    ]


HEAD_DIM = 64
EPSILON = 1e-12
MASKED = -1000000000.0
HIDDEN_BLOCK = 512
WIDE = 256
BF = jnp.bfloat16
F32 = jnp.float32


def mm(a, b):
    return lax.dot_general(a, b, (((1,), (0,)), ((), ())), preferred_element_type=F32)


def mm_right(a, b):
    return lax.dot_general(a, b, (((1,), (1,)), ((), ())), preferred_element_type=F32)


def mm_left(a, b):
    return lax.dot_general(a, b, (((0,), (0,)), ((), ())), preferred_element_type=F32)


def normalized(values):
    average = jnp.mean(values, axis=-1, keepdims=True)
    centred = values - average
    variance = jnp.mean(centred * centred, axis=-1, keepdims=True)
    scale = lax.rsqrt(variance + EPSILON)
    return centred * scale, scale


def normalize_back(grad, unit, scale, gain):
    gs = grad * gain
    mean_gs = jnp.mean(gs, axis=-1, keepdims=True)
    mean_gn = jnp.mean(gs * unit, axis=-1, keepdims=True)
    return (gs - mean_gs - unit * mean_gn) * scale


def head_lanes(head):
    lane = lax.broadcasted_iota(jnp.int32, (1, WIDE), 1)
    return lane // HEAD_DIM == head


def row_sum(values):
    return jnp.sum(values, axis=0, keepdims=True)


def attend_body(
    step, steps, length, x, vectors, layer, wq, wk, wv, wo, q_out, k_out, v_out, log_out,
    context_out, unit_out, scale_out, total,
):
    slots = x.shape[0]
    rows = x[...]
    lanes_of = pl.ds(pl.multiple_of(step * WIDE, WIDE), WIDE)
    q = (mm(rows, wq[...]) + vectors[layer, 0:1, lanes_of]).astype(BF)
    k = mm(rows, wk[...]).astype(BF)
    v = (mm(rows, wv[...]) + vectors[layer, 1:2, lanes_of]).astype(BF)
    q_out[...] = q
    k_out[...] = k
    v_out[...] = v
    live = lax.broadcasted_iota(jnp.int32, (1, slots), 1) < length[0]
    scaled = (q.astype(F32) * 0.125).astype(BF)
    zero = jnp.zeros_like(scaled)
    context = jnp.zeros((slots, WIDE), F32)
    logs = jnp.zeros((slots, 128), F32)
    column = lax.broadcasted_iota(jnp.int32, (1, 128), 1)
    for head in range(WIDE // HEAD_DIM):
        lanes = head_lanes(head)
        scores = mm_right(jnp.where(lanes, scaled, zero), k)
        scores = jnp.where(live, scores, MASKED)
        highest = jnp.max(scores, axis=-1, keepdims=True)
        exponent = jnp.exp(scores - highest)
        totals = jnp.sum(exponent, axis=-1, keepdims=True)
        probs = (exponent * (1.0 / totals)).astype(BF)
        context = jnp.where(lanes, mm(probs, v), context)
        logs = jnp.where(column == head, highest + jnp.log(totals), logs)
    log_out[...] = jnp.transpose(logs)[:8]
    low = context.astype(BF)
    context_out[...] = low

    @pl.when(step == 0)
    def _():
        total[...] = rows.astype(F32) + vectors[layer, 2:3]

    total[...] += mm(low, wo[...])

    @pl.when(step == steps - 1)
    def _():
        unit, scale = normalized(total[...])
        unit_out[...] = unit
        scale_out[...] = jnp.broadcast_to(scale, scale_out.shape)


def feed_body(
    step, steps, length, vectors, halves, layer, unit1, w1, w2, act_out, slope_out, unit_out,
    scale_out, result_out, low, total,
):
    @pl.when(step == 0)
    def _():
        middle = unit1[...] * vectors[layer, 3:4] + vectors[layer, 4:5]
        low[...] = middle.astype(BF)
        total[...] = middle + vectors[layer, 9:10]

    per = steps // 2
    bias = halves[layer, step // per, pl.ds(5 + lax.rem(step, per), 1)]
    inner = mm(low[...], w1[...]) + bias
    cdf = 0.5 * (1.0 + lax.erf(inner * 0.7071067811865476))
    act = (inner * cdf).astype(BF)
    act_out[...] = act
    slope_out[...] = (cdf + inner * (jnp.exp(-0.5 * inner * inner) * 0.3989422804014327)).astype(BF)
    total[...] += mm(act, w2[...])

    @pl.when(step == steps - 1)
    def _():
        unit, scale = normalized(total[...])
        unit_out[...] = unit
        scale_out[...] = jnp.broadcast_to(scale, scale_out.shape)
        live = lax.broadcasted_iota(jnp.int32, (unit.shape[0], 1), 0) < length[0]
        result = unit * vectors[layer, 10:11] + vectors[layer, 11:12]
        result_out[...] = jnp.where(live, result, 0.0).astype(BF)


def feed_back_body(
    step, steps, length, grad, unit2, scale2, g2, unit1, scale1, g1, b1, act, slope, w1, w2,
    d1_out, d2_out, first_out, vectors_out, inner_rows, second, outer, low, total,
):
    @pl.when(step == 0)
    def _():
        live = lax.broadcasted_iota(jnp.int32, (grad.shape[0], 1), 0) < length[0]
        g = jnp.where(live, grad[...].astype(F32), 0.0)
        unit = unit2[...]
        d_second = normalize_back(g, unit, scale2[:, :1], g2[...])
        second[...] = d_second
        d_outer = d_second.astype(BF)
        outer[...] = d_outer
        vectors_out[0:1] = row_sum(d_outer.astype(F32))
        vectors_out[1:2] = row_sum(g * unit)
        vectors_out[2:3] = row_sum(g)
        low[...] = (unit1[...] * g1[...] + b1[...]).astype(BF)
        total[...] = jnp.zeros_like(total)

    d_outer = outer[...]
    d_inner = (mm_right(d_outer, w2[...]) * slope[...].astype(F32)).astype(BF)
    inner_rows[step, 0:1] = row_sum(d_inner.astype(F32))
    total[...] += mm_right(d_inner, w1[...])
    d2_out[...] = mm_left(act[...], d_outer).astype(BF).reshape(d2_out.shape)
    d1 = mm_left(low[...], d_inner).astype(BF)
    half = d1.shape[0] // 2
    d1_out[0, 0] = d1[:half]
    d1_out[1, 0] = d1[half:]

    @pl.when(step == steps - 1)
    def _():
        d_middle = second[...] + total[...]
        unit = unit1[...]
        d_first = normalize_back(d_middle, unit, scale1[:, :1], g1[...])
        first_out[...] = d_first
        vectors_out[3:4] = row_sum(d_middle * unit)
        vectors_out[4:5] = row_sum(d_middle)
        vectors_out[5:6] = row_sum(d_first.astype(BF).astype(F32))


def attend_back_body(
    step, steps, length, first, x, q, k, v, log, context, wq, wk, wv, wo, dqkv_out, do_out, x_out,
    sums_out, attended, total,
):
    slots = x.shape[0]

    @pl.when(step == 0)
    def _():
        attended[...] = first[...].astype(BF)
        total[...] = first[...]

    d_att = attended[...]
    d_context = mm_right(d_att, wo[...]).astype(BF)
    queries = q[...]
    keys = k[...]
    values = v[...]
    scaled = (queries.astype(F32) * 0.125).astype(BF)
    zero = jnp.zeros_like(scaled)
    live = lax.broadcasted_iota(jnp.int32, (slots, 1), 0) < length[0]
    d_q = jnp.zeros((slots, WIDE), F32)
    d_k = jnp.zeros((slots, WIDE), F32)
    d_v = jnp.zeros((slots, WIDE), F32)
    for head in range(WIDE // HEAD_DIM):
        lanes = head_lanes(head)
        scores = mm_right(keys, jnp.where(lanes, scaled, zero))
        scores = jnp.where(live, scores, MASKED)
        probs = jnp.exp(scores - log[head : head + 1])
        d_v = jnp.where(lanes, mm(probs.astype(BF), d_context), d_v)
        d_probs = mm_right(values, jnp.where(lanes, d_context, zero))
        dots = row_sum(probs * d_probs)
        d_scores = (probs * (d_probs - dots)).astype(BF)
        d_k = jnp.where(lanes, mm(d_scores, queries), d_k)
        d_q = jnp.where(lanes, mm_left(d_scores, keys), d_q)
    d_q = (d_q * 0.125).astype(BF)
    d_k = (d_k * 0.125).astype(BF)
    d_v = d_v.astype(BF)
    sums_out[step, 0:1] = row_sum(d_q.astype(F32))
    sums_out[step, 1:2] = row_sum(d_v.astype(F32))
    total[...] += mm_right(d_q, wq[...]) + mm_right(d_k, wk[...]) + mm_right(d_v, wv[...])
    rows = x[...]
    for at, value in enumerate((d_q, d_k, d_v)):
        weight = mm_left(rows, value).astype(BF)
        half = weight.shape[0] // 2
        dqkv_out[0, at] = weight[:half]
        dqkv_out[1, at] = weight[half:]
    do_out[...] = mm_left(context[...], d_att).astype(BF).reshape(do_out.shape)

    @pl.when(step == steps - 1)
    def _():
        x_out[...] = total[...].astype(BF)


def struct(shape, dtype):
    return jax.ShapeDtypeStruct(shape, dtype)


UNIT_ORDER = (0, 1, 2, 3, 4, 8, 9, 5, 10, 11, 6, 7)
DIRECT_SETS = ((0, 1, 6, 7), (0, 1, 6, 7))
HOPS = (0.0, 10.0, 20.0, 34.0, 36.0, 40.0, 44.0)
PACE = 7.0
CROSS = 17.0
OUT_STEP = 3


class Plan:
    def __init__(self):
        self.entries = []
        self.done = set()

    def add(self, when, key, action):
        self.entries.append((when, len(self.entries), key, action))

    def sort(self):
        self.entries.sort(key=lambda entry: entry[:2])

    def run_first(self):
        _, _, key, action = self.entries.pop(0)
        action()
        self.done.add(key)

    def until(self, when):
        while self.entries and self.entries[0][0] <= when:
            self.run_first()

    def pending(self, when):
        return bool(self.entries) and self.entries[0][0] <= when

    def missing(self, keys):
        return any(key not in self.done for key in keys)

    def require(self, keys):
        while self.missing(keys):
            self.run_first()


def front_kernel(count, length, permutation, inverse, small, shards, inputs, outs, scratch):
    full, (rows_out, dealt), stored = outs[:6], outs[6:8], (outs[8:20], outs[20:32])
    deal = Deal(0, outs[19], outs[32], inverse, scratch[:6])
    scratch = scratch[6:]
    (stage, spread, ordered, halves, rows, xs, unit1, scale1, unit2, scale2, low, total,
     send_sem, recv_sem, load_sem, store_sem, deal_send, deal_recv, home_send, home_recv,
     small_send, small_recv, keep_sem) = scratch
    core = lax.axis_index("section")
    side = lax.axis_index("shard")
    bits = my_bits(count)
    sibling = {"section": 1 - core}
    facing = {"shard": 1 - side}
    corner = {"section": 1 - core, "shard": 1 - side}
    replicas = 1 << count
    groups = 2 * replicas
    devices = 2 * groups
    group = side * replicas + lax.axis_index("replica")
    me = core * groups + group
    chunk, columns = spread.shape[1:]
    strip = HALF // replicas
    position = sum(bits[p] * (1 << p) for p in range(count))
    greet_all(me, devices, replicas)

    def chip(index):
        return {"shard": index // replicas, "replica": lax.rem(index, replicas)}

    def piece(index):
        where = pl.ds(pl.multiple_of(index * chunk, chunk), chunk)
        return inputs.at[:, where, pl.ds(pl.multiple_of(core * columns, columns), columns)]

    def spread_copy(target):
        return remote(
            piece(target), spread.at[pl.ds(2 * group, 2)], deal_send.at[target],
            deal_recv.at[group], chip(target),
        )

    spread_own = pltpu.make_async_copy(
        piece(group), spread.at[pl.ds(2 * group, 2)], deal_recv.at[group]
    )

    def spread_start(step, carry):
        spread_copy(lax.rem(group + step, groups)).start()
        return carry

    def spread_wait(step, carry):
        source = lax.rem(group + step, groups)
        landed = spread.at[pl.ds(2 * source, 2)]
        remote(
            landed, landed, deal_send.at[source], deal_recv.at[source], chip(source)
        ).wait_recv()
        return carry

    def spot(device):
        where = pl.ds(pl.multiple_of(lax.rem(device, groups) * chunk, chunk), chunk)
        start = pl.multiple_of((device // groups) * columns, columns)
        return xs.at[where, pl.ds(start, columns)]

    def slot_of(device):
        return 2 * lax.rem(device, groups) + device // groups

    def home_copy(target):
        return remote(
            ordered.at[slot_of(target)], spot(me), home_send.at[target], home_recv.at[me],
            place(target, replicas),
        )

    home_own = pltpu.make_async_copy(ordered.at[slot_of(me)], spot(me), home_recv.at[me])

    def home_start(step, carry):
        home_copy(lax.rem(me + step, devices)).start()
        return carry

    def home_wait(step, carry):
        source = lax.rem(me + step, devices)
        remote(
            spot(source), spot(source), home_send.at[source], home_recv.at[source],
            place(source, replicas),
        ).wait_recv()
        return carry

    def spread_done(step, carry):
        spread_copy(lax.rem(group + step, groups)).wait_send()
        return carry

    def home_done(step, carry):
        home_copy(lax.rem(me + step, devices)).wait_send()
        return carry

    def reorder(slot, carry):
        ordered[slot] = spread[permutation[slot]]
        return carry

    def deal_second():
        spread_own.wait()
        lax.fori_loop(1, groups, spread_wait, 0)
        lax.fori_loop(0, devices, reorder, 0)
        home_own.start()
        lax.fori_loop(1, devices, home_start, 0)

    def deal_last():
        home_own.wait()
        lax.fori_loop(1, devices, home_wait, 0)

    def small_copy(index, partner):
        return remote(
            small, halves.at[core, side], small_send.at[index], small_recv.at[index], partner
        )

    small_own = pltpu.make_async_copy(small, halves.at[core, side], small_send.at[3])

    def vectors_here():
        small_own.wait()
        for index, layer, half, partner in (
            (0, 1 - core, side, sibling), (1, core, 1 - side, facing),
            (2, 1 - core, 1 - side, corner),
        ):
            landed = halves.at[layer, half]
            remote(
                landed, landed, small_send.at[index], small_recv.at[index], partner
            ).wait_recv()
        for layer in range(2):
            for half in range(2):
                rows[layer, :, pl.ds(512 * half, 512)] = halves[layer, half]

    def shard_at(unit, start, size):
        where = pl.ds(start, size)
        if unit < 4:
            return shards[unit].at[where]
        if unit < 8:
            return shards[4].at[where, pl.ds(1024 * (unit - 4), 1024)]
        return shards[5].at[pl.ds(512 * (unit - 8) + start, size)]

    def out_at(layer, unit, half, start, size):
        base = 512 * half + start if unit < 8 else 2048 * half + 512 * (unit - 8) + start
        where = pl.ds(pl.multiple_of(base, strip), size)
        if unit < 4:
            return full[unit].at[layer, where]
        if unit < 8:
            return full[4].at[layer, where, pl.ds(1024 * (unit - 4), 1024)]
        return full[5].at[layer, where]

    mine = HALF * core

    def wire(layer, unit, hop, src, dst, partner):
        index = UNITS * layer + unit
        return remote(src, dst, send_sem.at[index, hop], recv_sem.at[index, hop], partner)

    def arrive(layer, unit, hop, landed, partner):
        wire(layer, unit, hop, landed, landed, partner).wait_recv()

    def cross_rows(layer, unit):
        if unit in DIRECT_SETS[layer]:
            return mine, HALF
        return pl.multiple_of(mine + position * strip, strip), strip

    def cross(layer, unit):
        start, size = cross_rows(layer, unit)
        target = out_at(layer, unit, side, start, size)

        @pl.when(core == layer)
        def _():
            wire(layer, unit, 0, shard_at(unit, start, size), target, facing).start()

        @pl.when(core != layer)
        def _():
            arrive(layer, unit, count + 2, out_at(layer, unit, side, 0, 512), sibling)
            wire(layer, unit, 0, target, target, facing).start()

    def block(k):
        return pl.multiple_of(mine + ((position >> k) << k) * strip, strip), strip << k

    def other_block(k):
        start = ((position >> k) ^ 1) << k
        return pl.multiple_of(mine + start * strip, strip), strip << k

    def hop(layer, unit, k):
        there = 1 - side
        if k == 0:
            arrive(layer, unit, 0, out_at(layer, unit, there, *cross_rows(layer, unit)), facing)
        else:
            arrive(
                layer, unit, k, out_at(layer, unit, there, *other_block(k - 1)),
                across(k - 1, count, bits),
            )
        if k < count and unit not in DIRECT_SETS[layer]:
            held = out_at(layer, unit, there, *block(k))
            wire(layer, unit, k + 1, held, held, across(k, count, bits)).start()
        else:
            held = out_at(layer, unit, there, mine, HALF)
            wire(layer, unit, count + 1, held, held, sibling).start()

    def passed(layer, unit):
        landed = out_at(layer, unit, 1 - side, HALF * (1 - core), HALF)
        arrive(layer, unit, count + 1, landed, sibling)

        @pl.when(core == layer)
        def _():
            store(layer, unit).wait()

    def store(layer, unit):
        return pltpu.make_async_copy(
            stage.at[unit], out_at(layer, unit, side, 0, 512), store_sem.at[unit]
        )

    def load(unit):
        return pltpu.make_async_copy(shard_at(unit, 0, 512), stage.at[unit], load_sem.at[unit])

    def own_start(layer):
        for unit in UNIT_ORDER:
            source = shard_at(unit, 0, 512)
            wire(
                layer, unit, count + 2, source, out_at(layer, unit, side, 0, 512), sibling
            ).start()
            load(unit).start()

    def own_store(layer):
        for unit in UNIT_ORDER:
            load(unit).wait()
            store(layer, unit).start()

    plan = Plan()
    number = [0, 0]
    for layer in range(2):
        for unit in UNIT_ORDER:
            key = (layer, unit)
            if unit in DIRECT_SETS[layer]:
                landing = 14.0 + CROSS * (number[0] + 1)
                number[0] += 1
                plan.add(landing - 1.7 * CROSS, ("cross",) + key, lambda l=layer, u=unit: cross(l, u))
                plan.add(landing, ("hop",) + key, lambda l=layer, u=unit: hop(l, u, 0))
                plan.add(landing + 3.0, ("unit",) + key, lambda l=layer, u=unit: passed(l, u))
            else:
                begin = 6.0 + PACE * number[1]
                number[1] += 1
                plan.add(begin - 60.0, ("cross",) + key, lambda l=layer, u=unit: cross(l, u))
                for k in range(count + 1):
                    plan.add(
                        begin + HOPS[k], ("hop", k) + key, lambda l=layer, u=unit, k=k: hop(l, u, k)
                    )
                plan.add(
                    begin + HOPS[count] + 3.0, ("unit",) + key,
                    lambda l=layer, u=unit: passed(l, u),
                )
    plan.add(30.0, "deal", deal_second)
    plan.add(50.0, "inputs", deal_last)
    plan.add(10.0, "vectors", vectors_here)
    plan.sort()

    spread_own.start()
    lax.fori_loop(1, groups, spread_start, 0)
    for index, partner in enumerate((sibling, facing, corner)):
        small_copy(index, partner).start()
    small_own.start()
    for layer in range(2):
        @pl.when(core == layer)
        def _():
            own_start(layer)
    plan.until(1.0)
    for layer in range(2):
        @pl.when(core == layer)
        def _():
            own_store(layer)

    slots, width = xs.shape
    attention_steps = width // WIDE
    hidden = full[4].shape[-1]
    hidden_steps = hidden // HIDDEN_BLOCK
    band = pl.BlockSpec((slots, WIDE), lambda j: (0, j))
    wide = pl.BlockSpec((width, WIDE), lambda j: (0, j))
    hidden_band = pl.BlockSpec((slots, HIDDEN_BLOCK), lambda j: (0, j))

    def during(step, steps, begin, each, needs):
        for at in range(steps):
            when = begin + each * at
            wanted = needs(at)
            if plan.pending(when) or plan.missing(wanted):
                @pl.when(step == at)
                def _():
                    plan.require(wanted)
                    plan.until(when)

    def attend_stage(layer, begin):
        (q, k, v, log, context) = stored[layer][:5]

        def body(*refs):
            step = pl.program_id(0)
            attend_body(step, attention_steps, length, xs, rows, layer, *refs, unit1, scale1, total)
            during(step, attention_steps, begin, 5.0, lambda at: [])
            if layer == 1:
                pl.when(step == OUT_STEP)(deal.second)

        pltpu.emit_pipeline(
            body,
            grid=(attention_steps,),
            in_specs=[wide, wide, wide, pl.BlockSpec((WIDE, width), lambda j: (j, 0))],
            out_specs=[
                band, band, band, pl.BlockSpec((None, 8, slots), lambda j: (j, 0, 0)), band
            ],
        )(*(full[i].at[layer] for i in range(4)), q, k, v, log, context)

    def feed_needs(layer, step):
        return [
            ("unit", layer, unit)
            for at in range(min(step + 1, hidden_steps))
            for unit in (4 + at * HIDDEN_BLOCK // 1024, 8 + at % 4)
        ]

    def feed_stage(layer, begin):
        act, slope = stored[layer][7:9]

        def body(*refs):
            step = pl.program_id(0)
            feed_body(
                step, hidden_steps, length, rows, halves, layer, unit1, *refs, unit2, scale2, xs,
                low, total,
            )
            during(step, hidden_steps, begin, 2.5, lambda at: feed_needs(layer, at + 2))

        pltpu.emit_pipeline(
            body,
            grid=(hidden_steps,),
            in_specs=[
                pl.BlockSpec((width, HIDDEN_BLOCK), lambda j: (0, j)),
                pl.BlockSpec((HIDDEN_BLOCK, width), lambda j: (j, 0)),
            ],
            out_specs=[hidden_band, hidden_band],
        )(full[4].at[layer], full[5].at[layer], act, slope)

    def keep(source, target, at):
        copy = pltpu.make_async_copy(source, target, keep_sem.at[at])
        copy.start()
        return copy

    begin = (75.0, 125.0)
    keeping = []
    for layer in range(2):
        plan.require(["vectors", "inputs"] + [("unit", layer, unit) for unit in range(4)])
        if layer == 0:
            keeping += [keep(xs, dealt, 0), keep(rows, rows_out, 1)]
        attend_stage(layer, begin[layer])
        for copy in keeping:
            copy.wait()
        keeping = [keep(unit1, stored[layer][5], 2), keep(scale1, stored[layer][6], 3)]
        plan.require(feed_needs(layer, 1))
        feed_stage(layer, begin[layer] + 22.0)
        for copy in keeping:
            copy.wait()
        keeping = [
            keep(unit2, stored[layer][9], 4), keep(scale2, stored[layer][10], 5),
            keep(xs, stored[layer][11], 6),
        ]
        if layer == 0:
            keeping.pop().wait()
            deal.start()
    plan.until(1000000.0)
    for copy in keeping:
        copy.wait()
    deal.last()
    lax.fori_loop(1, groups, spread_done, 0)
    lax.fori_loop(1, devices, home_done, 0)
    for index, partner in enumerate((sibling, facing, corner)):
        small_copy(index, partner).wait_send()
    for layer in range(2):
        for unit in range(UNITS):
            start, size = cross_rows(layer, unit)
            crossed = out_at(layer, unit, side, start, size)
            wire(layer, unit, 0, crossed, crossed, facing).wait_send()
            if unit not in DIRECT_SETS[layer]:
                for k in range(count):
                    held = out_at(layer, unit, 1 - side, *block(k))
                    wire(layer, unit, k + 1, held, held, across(k, count, bits)).wait_send()
            held = out_at(layer, unit, 1 - side, mine, HALF)
            wire(layer, unit, count + 1, held, held, sibling).wait_send()

        @pl.when(core == layer)
        def _():
            for unit in range(UNITS):
                own = out_at(layer, unit, side, 0, 512)
                wire(layer, unit, count + 2, own, own, sibling).wait_send()


def forward(length, permutation, inverse, small, shards, inputs, count):
    groups = 2 << count
    slots, width = inputs.shape[1:]
    hidden = shards[4].shape[-1]
    part = (2 * groups, slots // groups, width // 2)
    dma = pltpu.SemaphoreType.DMA
    square = (slots, width)
    steps = width // WIDE
    layer = [
        struct(square, BF), struct(square, BF), struct(square, BF), struct((steps, 8, slots), F32),
        struct(square, BF), struct(square, F32), struct((slots, 128), F32),
        struct((slots, hidden), BF), struct((slots, hidden), BF), struct(square, F32),
        struct((slots, 128), F32), struct(square, BF),
    ]
    out_shape = (
        [struct((2, width, width), BF)] * 4
        + [struct((2, width, hidden), BF), struct((2, hidden, width), BF)]
        + [struct((2,) + small.shape[:1] + (width,), F32), struct(square, BF)]
        + layer + layer + [struct((2, groups, slots // groups, width), BF)]
    )
    smem = pl.BlockSpec(memory_space=pltpu.SMEM)
    anywhere = pl.BlockSpec(memory_space=pl.ANY)

    def kernel(*refs):
        front_kernel(
            count, *refs[:4], refs[4:10], refs[10], refs[11 : 11 + len(out_shape)],
            refs[11 + len(out_shape) :],
        )

    return pl.pallas_call(
        kernel,
        out_shape=out_shape,
        in_specs=[smem] * 3 + [anywhere] * 8,
        out_specs=[anywhere] * len(out_shape),
        scratch_shapes=deal_buffers(groups, slots // groups, width)
        + [
            pltpu.VMEM((UNITS, 512, 1024), BF), pltpu.VMEM(part, BF), pltpu.VMEM(part, BF),
            pltpu.VMEM((2, 2) + small.shape, F32),
            pltpu.VMEM((2,) + small.shape[:1] + (width,), F32),
            pltpu.VMEM(square, BF), pltpu.VMEM(square, F32), pltpu.VMEM((slots, 128), F32),
            pltpu.VMEM(square, F32), pltpu.VMEM((slots, 128), F32),
            pltpu.VMEM(square, BF), pltpu.VMEM(square, F32),
            dma((2 * UNITS, count + 3)), dma((2 * UNITS, count + 3)), dma((UNITS,)), dma((UNITS,)),
            dma((groups,)), dma((groups,)), dma((2 * groups,)), dma((2 * groups,)),
            dma((4,)), dma((3,)), dma((7,)),
        ],
        compiler_params=pltpu.CompilerParams(
            collective_id=0, has_side_effects=True, vmem_limit_bytes=VMEM_LIMIT
        ),
        name="forward",
    )(length, permutation, inverse, small, *shards, inputs)


SENT_RING = 4
LAND_RING = 5
PIECES = 2 * UNITS
DEAL_STEP = 5
EARLY = ((0, 1, 2, 3), (1, 3, 5, 7), (0, 1, 2, 3), (6,))
AHEAD = sum(len(steps) for steps in EARLY)


def back_kernel(count, length, inverse, gains, lower, upper, weights, result, outs, scratch):
    (total, small_total, landing, _, acts, d1_low, d2_low, dqkv_low, do_low, up_d1, up_d2,
     dqkv_up, do_up, grad_low, grad_up) = outs
    (xs, first, gradient, unit1, unit2, scale1, scale2, second, outer, middle, running, attended,
     vectors, inner_rows, sums) = scratch[:15]
    (own, came, across_half, kept, from_x), rest = scratch[15:20], scratch[20:]
    halves, rest = rest[:count], rest[count:]
    deal = Deal(1, result, outs[3], inverse, rest[:6])
    (smalls, small_own, small_recv, send0, recv0, send_x, recv_x, send_rs, recv_rs,
     send_ag, recv_ag, load_sem, came_sem, piece_sem, small_send, small_arrive,
     act_sem, total_sem, fetch_sem, done_send, done_recv) = rest[6:]
    wq, wk, wv, wo, w1, w2 = weights
    (up_unit2, up_scale2, up_unit1, up_scale1, up_act, up_slope, up_x, up_q, up_k, up_v, up_log,
     up_context, cotangent) = upper
    (low_unit2, low_scale2, low_unit1, low_scale1, low_act, low_slope, low_x, low_q, low_k, low_v,
     low_log, low_context) = lower
    core = lax.axis_index("section")
    side = lax.axis_index("shard")
    replica = lax.axis_index("replica")
    bits = my_bits(count)
    sibling = {"section": 1 - core}
    facing = {"shard": 1 - side}
    everything = (slice(None),) * count
    rows = kept.shape[-2]
    keep_ring = kept.shape[0]
    replicas = 1 << count
    groups = 2 * replicas
    group = side * replicas + replica
    me = core * groups + group
    greet_all(me, 2 * groups, replicas)

    layers = ((up_d1, up_d2, dqkv_up, do_up), (d1_low, d2_low, dqkv_low, do_low))
    ranges, at = [], 0
    for order in range(2):
        for index in range(4):
            depth = layers[order][index].shape[1]
            ranges.append((order, index, at, at + depth))
            at += depth

    def part_of(order, index, unit, half):
        where = pl.ds(pl.multiple_of(HALF * half, HALF), HALF)
        return layers[order][index].at[:, unit, where]

    def core_copy(unit, source=None):
        source = landing.at[unit] if source is None else source
        return remote(source, landing.at[unit], send0.at[unit], recv0.at[unit], sibling)

    def send_core(order, which, only=range(PIECES)):
        for at_order, index, low, high in ranges:
            if at_order == order and index in which:
                for unit in [u for u in range(low, high) if u in only]:
                    core_copy(unit, part_of(order, index, unit - low, 1 - core)).start()

    def own_load(source, slot):
        return pltpu.make_async_copy(source, own.at[slot], load_sem.at[slot])

    def came_load(unit):
        slot = lax.rem(unit, 2)
        return pltpu.make_async_copy(landing.at[unit], came.at[slot], came_sem.at[slot])

    def start_load(unit):
        for order, index, low, high in ranges:
            @pl.when(jnp.logical_and(unit >= low, unit < high))
            def _():
                own_load(part_of(order, index, unit - low, core), lax.rem(unit, 2)).start()

    def x_copy(unit):
        return remote(
            across_half.at[lax.rem(unit, SENT_RING)], from_x.at[lax.rem(unit, LAND_RING)],
            send_x.at[unit], recv_x.at[unit], facing,
        )

    def rs_copy(unit, p):
        slot = lax.rem(unit, keep_ring)
        return remote(
            kept.at[(slot,) + everything[:p] + (1 - bits[p],) + bits[p + 1 :]],
            halves[p].at[lax.rem(unit, LAND_RING)],
            send_rs.at[p, unit],
            recv_rs.at[p, unit],
            across(p, count, bits),
        )

    def ag_copy(unit, p):
        where = (unit,) + everything[:p] + bits[p:]
        source = kept.at[(lax.rem(unit, keep_ring),) + bits] if p == 0 else total.at[where]
        return remote(
            source, total.at[where], send_ag.at[p, unit], recv_ag.at[p, unit],
            across(p, count, bits),
        )

    def ag_arrive(unit, p):
        where = total.at[(unit,) + everything[:p] + (1 - bits[p],) + bits[p + 1 :]]
        remote(
            where, where, send_ag.at[p, unit], recv_ag.at[p, unit], across(p, count, bits)
        ).wait_recv()

    def piece_copy(unit):
        return pltpu.make_async_copy(
            kept.at[(lax.rem(unit, keep_ring),) + bits], total.at[(unit,) + bits],
            piece_sem.at[unit],
        )

    def done_copy(unit):
        index = lax.rem(unit, UNITS)
        return remote(
            total.at[unit], total.at[PIECES + index], done_send.at[index], done_recv.at[index],
            sibling,
        )

    def small_copy(step):
        partner = [sibling, facing] + [across(p, count, bits) for p in range(count)]
        source = smalls.at[1 - core] if step == 0 else small_own.at[step - 1]
        return remote(
            source, small_recv.at[step], small_send.at[step], small_arrive.at[step], partner[step]
        )

    def places_of(index, dims):
        return tuple((lax.rem(index // (1 << (dims - 1 - q)), 2) for q in range(dims)))

    def tick(now):
        @pl.when(jnp.logical_and(now >= SENT_RING, now < PIECES + SENT_RING))
        def _():
            x_copy(now - SENT_RING).wait_send()

        @pl.when(jnp.logical_and(now >= keep_ring, now < PIECES + keep_ring))
        def _():
            for p in range(count):
                rs_copy(now - keep_ring, p).wait_send()
            ag_copy(now - keep_ring, 0).wait_send()

        @pl.when(now < PIECES)
        def _():
            unit = now
            slot = lax.rem(unit, 2)

            @pl.when(unit == 0)
            def _():
                start_load(0)
                core_copy(0).wait_recv()
                came_load(0).start()

            own_load(landing.at[unit], slot).wait()
            came_load(unit).wait()

            @pl.when(unit + 1 < PIECES)
            def _():
                start_load(unit + 1)
                core_copy(unit + 1).wait_recv()
                came_load(unit + 1).start()

            out_slot = lax.rem(unit, SENT_RING)
            kept_slot = lax.rem(unit, keep_ring)

            def add(block, c):
                where = pl.ds(pl.multiple_of(block * 32, 32), 32)
                across_half[out_slot, where] = (
                    own[slot, 1 - side, where] + came[slot, 1 - side, where]
                )
                return c

            lax.fori_loop(0, HALF // 32, add, 0)
            x_copy(unit).start()

            def add_kept(index, c):
                where = pl.ds(pl.multiple_of(index * rows, rows), rows)
                mine = (kept_slot,) + places_of(index, count)
                kept[mine] = own[slot, side, where] + came[slot, side, where]
                return c

            lax.fori_loop(0, 1 << count, add_kept, 0)

        @pl.when(jnp.logical_and(now >= 1, now < PIECES + 1))
        def _():
            unit = now - 1
            slot = lax.rem(unit, keep_ring)
            land = lax.rem(unit, LAND_RING)
            x_copy(unit).wait_recv()

            def add(index, c):
                where = pl.ds(pl.multiple_of(index * rows, rows), rows)
                mine = (slot,) + places_of(index, count)
                kept[mine] = kept[mine] + from_x[land, where]
                return c

            lax.fori_loop(0, 1 << count, add, 0)
            rs_copy(unit, count - 1).start()

        for step in range(count):
            p = count - 1 - step

            @pl.when(jnp.logical_and(now >= 2 + step, now < PIECES + 2 + step))
            def _():
                unit = now - (2 + step)
                slot = lax.rem(unit, keep_ring)
                land = lax.rem(unit, LAND_RING)
                rs_copy(unit, p).wait_recv()

                def add(index, c):
                    mine = (slot,) + places_of(index, p) + bits[p:]
                    kept[mine] = kept[mine] + halves[p][(land,) + places_of(index, p)]
                    return c

                if p == 0:
                    add(0, 0)
                    piece_copy(unit).start()
                    ag_copy(unit, 0).start()
                else:
                    lax.fori_loop(0, 1 << p, add, 0)
                    rs_copy(unit, p - 1).start()

        for p in range(count):
            lag = 2 + count + p

            @pl.when(jnp.logical_and(now >= lag, now < PIECES + lag))
            def _():
                unit = now - lag
                ag_arrive(unit, p)
                if p == 0:
                    piece_copy(unit).wait()
                if p + 1 < count:
                    ag_copy(unit, p + 1).start()
                else:
                    @pl.when((unit < UNITS) == (core == 0))
                    def _():
                        done_copy(unit).start()

    def early(step, phase):
        before = 0 if phase == 3 else len(EARLY[3]) + sum(len(steps) for steps in EARLY[:phase])
        now = -1
        for at, when in enumerate(EARLY[phase]):
            now = jnp.where(step == when, before + at, now)

        @pl.when(now >= 0)
        def _():
            tick(now)

    def fetch(source, target, at):
        copy = pltpu.make_async_copy(source, target, fetch_sem.at[at])
        copy.start()
        return copy

    waits = [
        fetch(cotangent, gradient, 0), fetch(up_unit1, unit1, 2), fetch(up_unit2, unit2, 3),
        fetch(up_scale1, scale1, 4), fetch(up_scale2, scale2, 5),
    ]
    up_rows = fetch(up_x, xs, 1)
    deal.start()
    for copy in waits:
        copy.wait()

    slots, width = xs.shape
    attention_steps = width // WIDE
    hidden_steps = w1.shape[-1] // HIDDEN_BLOCK
    per = 512 // WIDE
    wide_per = 1024 // HIDDEN_BLOCK
    pairs = HIDDEN_BLOCK // 512
    band = pl.BlockSpec((slots, WIDE), lambda j: (0, j))
    columns = pl.BlockSpec((width, WIDE), lambda j: (0, j))

    def attention(layer, phase, q, k, v, log, context, dqkv, do):
        def body(*refs):
            step = pl.program_id(0)
            attend_back_body(
                step, attention_steps, length, first, xs, *refs, gradient, sums, attended, running
            )
            early(step, phase)

        pltpu.emit_pipeline(
            body,
            grid=(attention_steps,),
            in_specs=[
                band, band, band, pl.BlockSpec((None, 8, slots), lambda j: (j, 0, 0)), band,
                columns, columns, columns, pl.BlockSpec((WIDE, width), lambda j: (j, 0)),
            ],
            out_specs=[
                pl.BlockSpec((2, 3, 512, WIDE), lambda j: (0, 0, 0, j)),
                pl.BlockSpec((1, 1, WIDE, width), lambda j: (j // per, 0, j % per, 0)),
            ],
        )(q, k, v, log, context, wq.at[layer], wk.at[layer], wv.at[layer], wo.at[layer], dqkv, do)
        for at in range(attention_steps):
            lanes = pl.ds(WIDE * at, WIDE)
            smalls[layer, 0:1, lanes] = sums[at, 0:1]
            smalls[layer, 1:2, lanes] = sums[at, 1:2]

    def feed_stage(layer, act, slope, d1, d2, begin, steps):
        def body(*refs):
            step = pl.program_id(0) + begin
            feed_back_body(
                step, hidden_steps, length, gradient, unit2, scale2, gains.at[layer, 10:11],
                unit1, scale1, gains.at[layer, 3:4], gains.at[layer, 4:5], *refs, first,
                vectors, inner_rows, second, outer, middle, running,
            )
            if layer == 0:
                early(step, 1)
            elif begin > 0:
                pl.when(step == DEAL_STEP)(deal.second)
                early(step, 3)

        half = hidden_steps // 2
        hidden_band = pl.BlockSpec((slots, HIDDEN_BLOCK), lambda j: (0, j + begin))
        pltpu.emit_pipeline(
            body,
            grid=(steps,),
            in_specs=[
                hidden_band, hidden_band,
                pl.BlockSpec((width, HIDDEN_BLOCK), lambda j: (0, j + begin)),
                pl.BlockSpec((HIDDEN_BLOCK, width), lambda j: (j + begin, 0)),
            ],
            out_specs=[
                pl.BlockSpec(
                    (2, 1, 512, HIDDEN_BLOCK),
                    lambda j: (0, (j + begin) // wide_per, 0, (j + begin) % wide_per),
                ),
                pl.BlockSpec(
                    (1, pairs, 512, width),
                    lambda j: ((j + begin) // half, (j + begin) % half, 0, 0),
                ),
            ],
        )(act, slope, w1.at[layer], w2.at[layer], d1, d2)

    def feed_sums(layer):
        for at, source in ((2, 5), (3, 3), (4, 4), (9, 0), (10, 1), (11, 2)):
            smalls[layer, at : at + 1] = vectors[source : source + 1]
        for at in range(hidden_steps):
            line = 5 + at // wide_per
            lanes = pl.ds(HIDDEN_BLOCK * (at % wide_per), HIDDEN_BLOCK)
            smalls[layer, line : line + 1, lanes] = inner_rows[at, 0:1]

    start_units = UNITS // 6
    feed_stage(1, up_act, up_slope, up_d1, up_d2, 0, hidden_steps // 2)
    send_core(0, (0, 1), range(start_units))
    feed_stage(1, up_act, up_slope, up_d1, up_d2, hidden_steps // 2, hidden_steps // 2)
    feed_sums(1)
    send_core(0, (0, 1), range(start_units, 2 * UNITS))
    later = [
        fetch(low_unit1, unit1, 2), fetch(low_unit2, unit2, 3), fetch(low_scale1, scale1, 4),
        fetch(low_scale2, scale2, 5),
    ]
    up_rows.wait()
    attention(1, 0, up_q, up_k, up_v, up_log, up_context, dqkv_up, do_up)
    send_core(0, (2, 3))
    waits = [fetch(gradient, grad_up, 0), fetch(low_x, xs, 1)]
    for copy in later:
        copy.wait()
    feed_stage(0, low_act, low_slope, d1_low, d2_low, 0, hidden_steps)
    feed_sums(0)
    send_core(1, (0, 1))
    for copy in waits:
        copy.wait()
    attention(0, 2, low_q, low_k, low_v, low_log, low_context, dqkv_low, do_low)
    send_core(1, (2, 3))
    small_copy(0).start()
    held = fetch(gradient, grad_low, 0)
    held.wait()
    small_steps = count + 2
    both = (grad_low, grad_up)

    def exchange(layer):
        return remote(both[1 - layer], acts.at[layer], act_sem.at[0], act_sem.at[1], sibling)

    for layer in range(2):
        @pl.when(core == layer)
        def _():
            exchange(layer).start()
    grad_back = fetch(grad_up, xs, 1)
    grad_back.wait()

    @pl.when(core == 0)
    def _():
        pltpu.make_async_copy(gradient, acts.at[0], act_sem.at[2]).start()

    @pl.when(core == 1)
    def _():
        pltpu.make_async_copy(xs, acts.at[1], act_sem.at[2]).start()

    def late(now, carry):
        for step in range(small_steps):
            @pl.when(now == step + 1)
            def _():
                small_copy(step).wait_recv()
                before = smalls[core] if step == 0 else small_own[step - 1]
                small_own[step] = before + small_recv[step]
                if step + 1 < small_steps:
                    small_copy(step + 1).start()

        tick(now + AHEAD)
        return carry

    lax.fori_loop(0, PIECES + max(keep_ring, 2 + 2 * count) - AHEAD, late, 0)
    out = pltpu.make_async_copy(small_own.at[small_steps - 1], small_total, total_sem)
    out.start()

    def last(unit, carry):
        core_copy(unit).wait_send()
        for p in range(1, count):
            ag_copy(unit, p).wait_send()
        return carry

    lax.fori_loop(0, PIECES, last, 0)

    def swapped(index, carry):
        done_copy(index).wait_send()
        done_copy(index).wait_recv()
        return carry

    lax.fori_loop(0, UNITS, swapped, 0)
    for step in range(small_steps):
        small_copy(step).wait_send()

    deal.last()
    back = remote(both[0], acts.at[1 - core], act_sem.at[0], act_sem.at[1], sibling)
    back.wait_send()
    back.wait_recv()
    pltpu.make_async_copy(xs, acts.at[core], act_sem.at[2]).wait()
    out.wait()


def backward(length, inverse, gains, lower, upper, weights, result, count):
    cut = (2,) * count
    rows = HALF // (1 << count)
    narrow = cut + (rows, 1024)
    dma = pltpu.SemaphoreType.DMA
    groups = 2 << count
    slots, width = result.shape
    chunk = slots // groups
    keep_ring = count + 5
    hidden = weights[4].shape[-1]
    sizes = [len(lower), len(upper), len(weights)]

    def kernel(*refs):
        start, groups_of = 3, []
        for size in sizes:
            groups_of.append(refs[start : start + size])
            start += size
        back_kernel(
            count, *refs[:3], *groups_of, refs[start], refs[start + 1 : start + 16],
            refs[start + 16 :],
        )

    anywhere = pl.BlockSpec(memory_space=pl.ANY)
    vmem = pl.BlockSpec(memory_space=pltpu.VMEM)
    smem = pl.BlockSpec(memory_space=pltpu.SMEM)
    vectors = (UNITS, width)
    square = (slots, width)
    feed_shape, head_shape = (2, 4, 512, 1024), (2, 3, 512, 1024)
    out_shape = [
        struct((PIECES + UNITS,) + narrow, BF),
        struct(vectors, F32),
        struct((PIECES, 2, HALF, 1024), BF),
        struct((2, groups, chunk, width), BF),
        struct((2,) + square, BF),
        struct(feed_shape, BF), struct(feed_shape, BF),
        struct(head_shape, BF), struct((2, 1, 512, 1024), BF),
        struct(feed_shape, BF), struct(feed_shape, BF),
        struct(head_shape, BF), struct((2, 1, 512, 1024), BF),
        struct(square, BF), struct(square, BF),
    ]
    result = pl.pallas_call(
        kernel,
        out_shape=out_shape,
        in_specs=[smem, smem, vmem] + [anywhere] * (sum(sizes) + 1),
        out_specs=[anywhere] * len(out_shape),
        scratch_shapes=[
            pltpu.VMEM(square, BF), pltpu.VMEM(square, F32), pltpu.VMEM(square, BF),
            pltpu.VMEM(square, F32), pltpu.VMEM(square, F32),
            pltpu.VMEM((slots, 128), F32), pltpu.VMEM((slots, 128), F32),
            pltpu.VMEM(square, F32), pltpu.VMEM(square, BF), pltpu.VMEM(square, BF),
            pltpu.VMEM(square, F32), pltpu.VMEM(square, BF),
            pltpu.VMEM((8, width), F32),
            pltpu.VMEM((hidden // HIDDEN_BLOCK, 8, HIDDEN_BLOCK), F32),
            pltpu.VMEM((width // WIDE, 8, WIDE), F32),
            pltpu.VMEM((2, 2, HALF, 1024), BF),
            pltpu.VMEM((2, 2, HALF, 1024), BF),
            pltpu.VMEM((SENT_RING, HALF, 1024), BF),
            pltpu.VMEM((keep_ring,) + narrow, BF),
            pltpu.VMEM((LAND_RING, HALF, 1024), BF),
        ]
        + [pltpu.VMEM((LAND_RING,) + (2,) * p + (rows, 1024), BF) for p in range(count)]
        + deal_buffers(groups, chunk, width)
        + [
            pltpu.VMEM((2,) + vectors, F32),
            pltpu.VMEM((count + 2,) + vectors, F32),
            pltpu.VMEM((count + 2,) + vectors, F32),
            dma((PIECES,)), dma((PIECES,)), dma((PIECES,)), dma((PIECES,)),
            dma((count, PIECES)), dma((count, PIECES)), dma((count, PIECES)), dma((count, PIECES)),
            dma((2,)), dma((2,)), dma((PIECES,)), dma((count + 2,)), dma((count + 2,)),
            dma((3,)), dma, dma((6,)), dma((UNITS,)), dma((UNITS,)),
        ],
        compiler_params=pltpu.CompilerParams(
            collective_id=1, has_side_effects=True, vmem_limit_bytes=VMEM_LIMIT
        ),
        name="backward",
    )(length, inverse, gains, *lower, *upper, *weights, result)
    total, small_total, _, dealt, acts = result[:5]
    return total.reshape(3, UNITS, HALF, 1024), small_total, dealt.reshape(2, slots, width), acts


from jax.sharding import PartitionSpec as P

VECTORS = (1, 1, 1, 1, 1, 4, 1, 1, 1)


def unpack_kernel(core, narrow, first, second, *outs):
    for at in range(4):
        outs[at][0] = narrow[0, at].astype(F32)
        outs[4][0, :, pl.ds(1024 * at, 1024)] = first[0, at].astype(F32)
        outs[5][0, at] = second[0, at].astype(F32)


def unpack(core, total):
    def band(kind):
        return pl.BlockSpec(
            (1, 4, 128, 1024),
            lambda h, b, core: (jnp.where(h == core[0], 1 - core[0], 2), kind, b, 0),
        )

    square = pl.BlockSpec((1, 128, 1024), lambda h, b, core: (0, 2 * h + b, 0))
    result = pl.pallas_call(
        unpack_kernel,
        grid_spec=pltpu.PrefetchScalarGridSpec(
            num_scalar_prefetch=1,
            grid=(2, 2),
            in_specs=[band(2), band(0), band(1)],
            out_specs=[square] * 4
            + [
                pl.BlockSpec((1, 128, 4096), lambda h, b, core: (0, 2 * h + b, 0)),
                pl.BlockSpec((1, 4, 128, 1024), lambda h, b, core: (0, 0, 2 * h + b, 0)),
            ],
        ),
        out_shape=[struct((1, 512, 1024), F32)] * 4
        + [struct((1, 512, 4096), F32), struct((1, 4, 512, 1024), F32)],
        compiler_params=pltpu.CompilerParams(vmem_limit_bytes=VMEM_LIMIT),
        name="unpack",
    )(core.reshape(1), total, total, total)
    return (*result[:5], result[5].reshape(1, 2048, 1024))


def on_device(
    inputs, cotangent, lengths, permutation, query_weight, query_bias, key_weight, value_weight,
    value_bias, output_weight, output_bias, first_gain, first_bias, inner_weight, inner_bias,
    outer_weight, outer_bias, second_gain, second_bias,
):
    core = lax.axis_index("section")
    group = lax.axis_index(GROUP)
    count = lax.axis_size("replica").bit_length() - 1
    shards = [
        w[0] for w in (query_weight, key_weight, value_weight, output_weight, inner_weight, outer_weight)
    ]
    vectors = [
        v[0] for v in (query_bias, value_bias, output_bias, first_gain, first_bias, inner_bias,
                       outer_bias, second_gain, second_bias)
    ]
    everyone = jnp.arange(permutation.shape[0], dtype=jnp.int32)
    own = lax.dynamic_slice_in_dim(permutation, 2 * group + core, 1)
    length = jnp.sum(jnp.where(everyone == own, lengths, 0), keepdims=True)
    inverse = jnp.sum(
        jnp.where(permutation[None, :] == everyone[:, None], everyone[None, :], 0), axis=1
    )
    short = jnp.concatenate(vectors).astype(F32).reshape(UNITS, -1)
    short = jnp.pad(short, ((0, 16 - UNITS), (0, 0)))
    result = forward(length, permutation, inverse, short, shards, inputs, count)
    weights, gains, x, low, up = result[:6], result[6], result[7], result[8:20], result[20:32]
    grad = lax.dynamic_index_in_dim(cotangent, core, 0, keepdims=False)
    lower, upper = low[11], up[11]
    lower_home = result[32].reshape(2, *lower.shape)

    def kept(stored, rows):
        q, k, v, log, context, unit1, scale1, act, slope, unit2, scale2 = stored[:11]
        return (unit2, scale2, unit1, scale1, act, slope, rows, q, k, v, log, context)

    total, small, upper_home, input_grads = backward(
        length, inverse, gains, kept(low, x), kept(up, lower) + (grad,), weights, upper,
        count,
    )
    activations = jnp.where(core == 0, lower_home, upper_home)
    side = lax.axis_index("shard")
    pieces, at = [], 0
    for width in VECTORS:
        whole_vector = small[at : at + width].reshape(2, -1)
        pieces.append(lax.dynamic_slice_in_dim(whole_vector, side, 1, axis=0))
        at += width
    dq, dk, dv, do, d1, d2 = unpack(core, total)
    return (
        activations[None], input_grads[None], dq, pieces[0], dk, dv, pieces[1], do, pieces[2],
        pieces[3], pieces[4], d1, pieces[5], d2, pieces[6], pieces[7], pieces[8],
    )


def solution(mesh):
    matrix, vector = P("section", "shard", None), P("section", "shard")
    rows = P(("shard", "replica"), None, None)
    in_specs = (
        rows, rows, P(), P(), matrix, vector, matrix, matrix, vector, matrix, vector, vector,
        vector, matrix, vector, matrix, vector, vector, vector,
    )
    both = P("section", ("shard", "replica"), None, None)
    out_specs = (
        both, both, matrix, vector, matrix, matrix, vector, matrix, vector, vector, vector,
        matrix, vector, matrix, vector, vector, vector,
    )
    return jax.shard_map(
        on_device, mesh=mesh, in_specs=in_specs, out_specs=out_specs, check_vma=False
    )
```
